32 devices in a mesh: ctx: 8 (over y, x, core), fsdp: 4 (over z).
Axes of the slice: x: 2, y: 2, z: 4, core: 2. Of those that a mesh axis runs over, the one named last changes fastest.
Arguments:
- block_input: bfloat16 [4, 1024, 2048], P('fsdp', 'ctx'), may hold values from -6 to 6
- output_grad: bfloat16 [4, 1024, 2048], P('fsdp', 'ctx'), may hold values from -6 to 6
- segment: int32 [4, 1024], P('fsdp'), may hold values from 0 to 3, never falling along the last dimension, each value on 1 to 512 neighbouring positions
- slots: int32 [16], replicated, may hold values from 0 to 15, each once
- ln_gain: bfloat16 [2048], P(('ctx', 'fsdp')), may hold values from 0.5 to 1.5
- ln_bias: bfloat16 [2048], P(('ctx', 'fsdp')), may hold values from -2 to 2
- qkv_w: bfloat16 [2048, 6144], P(('ctx', 'fsdp')), may hold values from -1 to 1
- qkv_b: bfloat16 [6144], P(('ctx', 'fsdp')), may hold values from -0.59765625 to 0.59765625
- dense_w: bfloat16 [2048, 2048], P(('ctx', 'fsdp')), may hold values from -0.5 to 0.5
- dense_b: bfloat16 [2048], P(('ctx', 'fsdp')), may hold values from -2 to 2
- fc1_w: bfloat16 [2048, 8192], P(('ctx', 'fsdp')), may hold values from -0.125 to 0.125
- fc1_b: bfloat16 [8192], P(('ctx', 'fsdp')), may hold values from -2 to 2
- fc2_w: bfloat16 [8192, 2048], P(('ctx', 'fsdp')), may hold values from -0.0625 to 0.0625
- fc2_b: bfloat16 [2048], P(('ctx', 'fsdp')), may hold values from -2 to 2
Outputs:
- block_output: bfloat16 [4, 1024, 2048], P('fsdp', 'ctx')
- input_grad: float32 [4, 1024, 2048], P('fsdp', 'ctx')
- d_ln_gain: float32 [2048], P(('ctx', 'fsdp'))
- d_ln_bias: float32 [2048], P(('ctx', 'fsdp'))
- d_qkv_w: float32 [2048, 6144], P(('ctx', 'fsdp'))
- d_qkv_b: float32 [6144], P(('ctx', 'fsdp'))
- d_dense_w: float32 [2048, 2048], P(('ctx', 'fsdp'))
- d_dense_b: float32 [2048], P(('ctx', 'fsdp'))
- d_fc1_w: float32 [2048, 8192], P(('ctx', 'fsdp'))
- d_fc1_b: float32 [8192], P(('ctx', 'fsdp'))
- d_fc2_w: float32 [8192, 2048], P(('ctx', 'fsdp'))
- d_fc2_b: float32 [2048], P(('ctx', 'fsdp'))
The draws below stay inside these ranges and needn't reach their ends.
Inputs may be any that keep to these rules, and one draw needn't show every extreme that they name: `segment`: ids never fall along positions; each of the 4 documents of a sequence spans 1 to 512 positions, one exactly that many. `slots`: every stretch number appears exactly once.
All inputs are finite; a program needn't handle non-finite values.
Results may differ from the reference program's by a relative error of at most 0.014.
Values may be sent and summed in bfloat16 or wider, within the bound.
A program may use at most 384 MiB of HBM per device.

```python
import math
import jax
import jax.numpy as jnp
import numpy as np
from jax import lax

D = 2048
HEADS = 32
HEAD = 64
ROT = 32
FF = 8192
DOCS = 4
STRETCH = 64
SEQ_LEN = 1024
SEQS = 4
N_CTX = 8


def draw_qkv_w(key, part):
    width = D
    whole = jax.random.normal(key, (width, 3 * width), jnp.float32) * width ** (-0.5)
    return jnp.clip(whole, -1.0, 1.0).astype(jnp.bfloat16)


def steps_of(rng, shape, pieces, smallest, high):
    gain, own = 1.0, jax.random.fold_in(rng, 6)
    for position, parts in pieces:
        draws = jnp.exp(jax.random.uniform(jax.random.fold_in(own, position), (parts,), jnp.float32, smallest / len(pieces), high / len(pieces)))
        gain = gain * jnp.repeat(draws, shape[position] // parts).reshape([-1 if axis == position else 1 for axis in range(len(shape))])
    return gain


def length_profile(number_of, total, bound, skew):
    weights = [(1 << 20) // math.isqrt(standing ** skew) + 1 for standing in range(2, number_of + 1)]
    surplus, holding = total - bound - (number_of - 1), [1] * (number_of - 1)
    while surplus > 0:
        candidates = [i for i in range(number_of - 1) if holding[i] < bound]
        pool, remaining = sum([weights[i] for i in candidates]), surplus
        for i in candidates:
            addition = min(bound - holding[i], max(1, remaining * weights[i] // pool), surplus)
            holding[i] = holding[i] + addition
            surplus = surplus - addition
    return np.array([bound] + holding)


def ragged(key, number_of, total, most, lean):
    if number_of == 2:
        one = jax.random.randint(key, (), max(1, total - most), min(most, total - 1) + 1)
        return jnp.stack([one, total - one])
    sizes = jnp.asarray(length_profile(number_of, total, most, lean), jnp.int32)
    couples = (number_of - 1) // 2
    giver, receiver = sizes[1:1 + 2 * couples:2], sizes[2:2 + 2 * couples:2]
    margin = jnp.minimum(giver - 1, most - receiver)
    moved = jax.random.randint(jax.random.fold_in(key, 1), (couples,), 0, 1 << 20) % (margin + 1)
    sizes = sizes.at[1:1 + 2 * couples:2].set(giver - moved).at[2:2 + 2 * couples:2].set(receiver + moved)
    return sizes[jax.random.permutation(jax.random.fold_in(key, 2), number_of)]


def bell_draw(rng, shape, scale, reach, shards=(), held_as=jnp.bfloat16):
    factor_of = steps_of(rng, shape, shards, -0.22, 0.18) if shards else 1.0
    drawn = jax.random.normal(rng, shape, jnp.float32) * scale * factor_of
    return jnp.minimum(jnp.maximum(drawn, -reach), reach).astype(held_as)


def setup_inputs(seed: int = 0) -> dict:
    streams_of = jax.random.split(jax.random.key(seed), 15)
    return {
        "block_input": bell_draw(streams_of[0], (SEQS, SEQ_LEN, D), 1.0, 6.0, ((0, 4), (1, 8))),
        "output_grad": bell_draw(streams_of[1], (SEQS, SEQ_LEN, D), 1.0, 6.0, ((0, 4), (1, 8))),
        "segment": jax.vmap(lambda own: jnp.searchsorted(jnp.cumsum(ragged(own, DOCS, SEQ_LEN, SEQ_LEN // 2, 0)), jnp.arange(SEQ_LEN), side="right"))(jax.random.split(streams_of[2], SEQS)).reshape((SEQS, SEQ_LEN)).astype(jnp.int32),
        "slots": jax.random.permutation(streams_of[3], 2 * N_CTX).astype(jnp.int32),
        "ln_gain": jnp.clip(1.0 + 0.1 * jax.random.normal(streams_of[4], (D,), jnp.float32), 0.5, 1.5).astype(jnp.bfloat16),
        "ln_bias": bell_draw(streams_of[5], (D,), 0.3, 2.0, ((0, 32),)),
        "qkv_w": draw_qkv_w(jax.random.fold_in(streams_of[14], 71), 0),
        "qkv_b": bell_draw(streams_of[7], (3 * D,), 0.1, 0.59765625, ((0, 32),)),
        "dense_w": bell_draw(streams_of[8], (D, D), (max(1, 64 * D // SEQ_LEN)) ** -0.5, 0.5, ((0, 32),)),
        "dense_b": bell_draw(streams_of[9], (D,), 0.3, 2.0, ((0, 32),)),
        "fc1_w": bell_draw(streams_of[10], (D, FF), D ** -0.5, 0.125, ((0, 32),)),
        "fc1_b": bell_draw(streams_of[11], (FF,), 0.3, 2.0, ((0, 32),)),
        "fc2_w": bell_draw(streams_of[12], (FF, D), FF ** -0.5, 0.0625, ((0, 32),)),
        "fc2_b": bell_draw(streams_of[13], (D,), 0.3, 2.0, ((0, 32),)),
    }


EPS = 1e-05
GELU_C = math.sqrt(2.0 / math.pi)
NEG = -1e+30

def gelu_pair(upper):
    inner = GELU_C * (upper + 0.044715 * upper * upper * upper)
    tanh_val = jnp.tanh(inner)
    value = 0.5 * upper * (1.0 + tanh_val)
    slope = 0.5 * (1.0 + tanh_val) + 0.5 * upper * (1.0 - tanh_val * tanh_val) * GELU_C * (1.0 + 3.0 * 0.044715 * upper * upper)
    return (value, slope)

def rotary_tables(positions):
    half = ROT // 2
    freqs = jnp.exp(-(2.0 * jnp.arange(half, dtype=jnp.float32) / ROT) * math.log(10000.0))
    angles = positions.astype(jnp.float32)[:, None] * freqs[None, :]
    return (jnp.cos(angles)[:, None, :], jnp.sin(angles)[:, None, :])

def rotate(tensor, cosine, sine, sign):
    half = ROT // 2
    first = tensor[..., :half]
    second = tensor[..., half:ROT]
    new_first = first * cosine - sign * second * sine
    new_second = second * cosine + sign * first * sine
    return jnp.concatenate([new_first, new_second, tensor[..., ROT:]], axis=-1)

def to_bf16(value):
    return lax.optimization_barrier(value.astype(jnp.bfloat16)).astype(jnp.float32)

def reference(block_input, output_grad, segment, slots, ln_gain, ln_bias, qkv_w, qkv_b, dense_w, dense_b, fc1_w, fc1_b, fc2_w, fc2_b):
    length = SEQ_LEN
    block = math.gcd(length, 256)
    nblocks = length // block
    scale = HEAD ** (-0.5)
    rows = jnp.arange(length, dtype=jnp.int32)
    positions = slots[rows // STRETCH] * STRETCH + rows % STRETCH
    cosine, sine = rotary_tables(positions)
    gain_float = ln_gain.astype(jnp.float32)
    norm_bias_float = ln_bias.astype(jnp.float32)
    starts = jnp.arange(nblocks, dtype=jnp.int32) * block

    def one_sequence(accum, inputs):
        x_seq, dy_seq, seg_seq = inputs
        docs = jnp.take(seg_seq, positions)
        xf = x_seq.astype(jnp.float32)
        row_mean = lax.optimization_barrier(jnp.mean(xf, axis=-1, keepdims=True))
        centered_input = xf - row_mean
        inverse_deviation = lax.rsqrt(lax.optimization_barrier(jnp.mean(centered_input * centered_input, axis=-1, keepdims=True)) + EPS)
        standardized_input = centered_input * inverse_deviation
        normed_rows = (standardized_input * gain_float + norm_bias_float).astype(jnp.bfloat16)
        proj = jnp.dot(normed_rows, qkv_w, preferred_element_type=jnp.float32) + qkv_b.astype(jnp.float32)
        query = rotate(proj[:, :D].reshape(length, HEADS, HEAD), cosine, sine, 1.0).astype(jnp.bfloat16)
        keys = rotate(proj[:, D:2 * D].reshape(length, HEADS, HEAD), cosine, sine, 1.0).astype(jnp.bfloat16)
        values = proj[:, 2 * D:].reshape(length, HEADS, HEAD).astype(jnp.bfloat16)
        query_f = query.astype(jnp.float32)
        keys_f = keys.astype(jnp.float32)
        values_f = values.astype(jnp.float32)

        def block_mask(start):
            qpos = lax.dynamic_slice_in_dim(positions, start, block, 0)
            qdoc = lax.dynamic_slice_in_dim(docs, start, block, 0)
            return (positions[None, :] <= qpos[:, None]) & (docs[None, :] == qdoc[:, None])

        def attend_block(start):
            qblk = lax.dynamic_slice_in_dim(query_f, start, block, 0)
            mask = block_mask(start)[None]
            scores = jnp.einsum('qhd,khd->hqk', qblk, keys_f) * scale
            scores = jnp.where(mask, scores, NEG)
            top = lax.optimization_barrier(jnp.max(scores, axis=-1))
            expo = jnp.where(mask, jnp.exp(scores - top[..., None]), 0.0)
            total = lax.optimization_barrier(jnp.sum(expo, axis=-1))
            out = jnp.einsum('hqk,khd->qhd', to_bf16(expo), values_f) / total.T[:, :, None]
            return (out, top + jnp.log(total))
        outs, lses = lax.map(attend_block, starts)
        attn = outs.reshape(length, D).astype(jnp.bfloat16)
        upper = jnp.dot(normed_rows, fc1_w, preferred_element_type=jnp.float32) + fc1_b.astype(jnp.float32)
        act_f, slope = gelu_pair(upper)
        act = act_f.astype(jnp.bfloat16)
        y_seq = xf + jnp.dot(attn, dense_w, preferred_element_type=jnp.float32) + dense_b.astype(jnp.float32)
        y_seq = y_seq + jnp.dot(act, fc2_w, preferred_element_type=jnp.float32) + fc2_b.astype(jnp.float32)
        y_seq = y_seq.astype(jnp.bfloat16)
        gradient_float = dy_seq.astype(jnp.float32)
        g_out_b = lax.optimization_barrier(jnp.sum(gradient_float, axis=0))
        g_dense_w = jnp.dot(attn.T, dy_seq, preferred_element_type=jnp.float32)
        g_fc2_w = jnp.dot(act.T, dy_seq, preferred_element_type=jnp.float32)
        dup = jnp.dot(dy_seq, fc2_w.T, preferred_element_type=jnp.float32) * slope
        g_fc1_b = lax.optimization_barrier(jnp.sum(dup, axis=0))
        dup_b = dup.astype(jnp.bfloat16)
        g_fc1_w = jnp.dot(normed_rows.T, dup_b, preferred_element_type=jnp.float32)
        dattn = jnp.dot(dy_seq, dense_w.T, preferred_element_type=jnp.float32).astype(jnp.bfloat16).reshape(length, HEADS, HEAD)
        dattn_f = dattn.astype(jnp.float32)
        delta = lax.optimization_barrier(jnp.sum(dattn_f * attn.reshape(length, HEADS, HEAD).astype(jnp.float32), axis=-1)).T

        def back_block(carry, item):
            dk_acc, dv_acc = carry
            start, lse_blk = item
            qblk = lax.dynamic_slice_in_dim(query_f, start, block, 0)
            dblk = lax.dynamic_slice_in_dim(dattn_f, start, block, 0)
            delta_blk = lax.dynamic_slice_in_dim(delta, start, block, 1)
            mask = block_mask(start)[None]
            scores = jnp.einsum('qhd,khd->hqk', qblk, keys_f) * scale
            probs = jnp.where(mask, jnp.exp(jnp.where(mask, scores, NEG) - lse_blk[..., None]), 0.0)
            dv_acc = dv_acc + jnp.einsum('hqk,qhd->khd', to_bf16(probs), dblk)
            dprob = jnp.einsum('qhd,khd->hqk', dblk, values_f)
            dscore = to_bf16(probs * (dprob - delta_blk[..., None]) * scale)
            dq_blk = jnp.einsum('hqk,khd->qhd', dscore, keys_f)
            dk_acc = dk_acc + jnp.einsum('hqk,qhd->khd', dscore, qblk)
            return ((dk_acc, dv_acc), dq_blk)
        zeros = jnp.zeros((length, HEADS, HEAD), jnp.float32)
        (dkey, dvalue), dq_blocks = lax.scan(back_block, (zeros, zeros), (starts, lses))
        dquery = rotate(dq_blocks.reshape(length, HEADS, HEAD), cosine, sine, -1.0)
        dkey = rotate(dkey, cosine, sine, -1.0)
        dproj = jnp.concatenate([dquery.reshape(length, D), dkey.reshape(length, D), dvalue.reshape(length, D)], axis=1)
        g_qkv_b = lax.optimization_barrier(jnp.sum(dproj, axis=0))
        dproj_b = dproj.astype(jnp.bfloat16)
        g_qkv_w = jnp.dot(normed_rows.T, dproj_b, preferred_element_type=jnp.float32)
        normed_input_grad = jnp.dot(dproj_b, qkv_w.T, preferred_element_type=jnp.float32) + jnp.dot(dup_b, fc1_w.T, preferred_element_type=jnp.float32)
        layer_gain_grad = lax.optimization_barrier(jnp.sum(normed_input_grad * standardized_input, axis=0))
        g_lnb = lax.optimization_barrier(jnp.sum(normed_input_grad, axis=0))
        scaled_rows = normed_input_grad * gain_float
        sequence_input_grad = gradient_float + inverse_deviation * (scaled_rows - lax.optimization_barrier(jnp.mean(scaled_rows, axis=-1, keepdims=True)) - standardized_input * lax.optimization_barrier(jnp.mean(scaled_rows * standardized_input, axis=-1, keepdims=True)))
        grads = (layer_gain_grad, g_lnb, g_qkv_w, g_qkv_b, g_dense_w, g_out_b, g_fc1_w, g_fc1_b, g_fc2_w, g_out_b)
        accum = jax.tree.map(lambda total, new: total + new, accum, grads)
        return (accum, (y_seq, sequence_input_grad))
    init = (jnp.zeros((D,), jnp.float32), jnp.zeros((D,), jnp.float32), jnp.zeros((D, 3 * D), jnp.float32), jnp.zeros((3 * D,), jnp.float32), jnp.zeros((D, D), jnp.float32), jnp.zeros((D,), jnp.float32), jnp.zeros((D, FF), jnp.float32), jnp.zeros((FF,), jnp.float32), jnp.zeros((FF, D), jnp.float32), jnp.zeros((D,), jnp.float32))
    grads, (block_output, input_grad) = lax.scan(one_sequence, init, (block_input, output_grad, segment))
    return (block_output, input_grad, grads[0], grads[1], grads[2], grads[3], grads[4], grads[5], grads[6], grads[7], grads[8], grads[9])
```

```python
import math

import jax
import jax.numpy as jnp
from jax import lax
from jax.experimental import pallas as pl
from jax.experimental.pallas import tpu as pltpu
from jax.sharding import PartitionSpec as P

HEADS = 32
ROT = 32


EPS = 1e-05
GELU_C = math.sqrt(2.0 / math.pi)
NEG = -1e30


def shifted(block, axis, distance):
    devices = range(lax.axis_size(axis))
    route = [((i - distance) % len(devices), i) for i in devices]
    return lax.ppermute(block, axis, route)


def gelu_pair(upper):
    inner = GELU_C * (upper + 0.044715 * upper * upper * upper)
    tanh_val = jnp.tanh(inner)
    value = 0.5 * upper * (1.0 + tanh_val)
    slope = 0.5 * (1.0 + tanh_val) + 0.5 * upper * (1.0 - tanh_val * tanh_val) * GELU_C * (
        1.0 + 3.0 * 0.044715 * upper * upper
    )
    return (value, slope)


def rotary_tables(positions):
    half = ROT // 2
    freqs = jnp.exp(-(2.0 * jnp.arange(half, dtype=jnp.float32) / ROT) * math.log(10000.0))
    angles = positions.astype(jnp.float32)[:, None] * freqs[None, :]
    return (jnp.cos(angles)[:, None, :], jnp.sin(angles)[:, None, :])


def rotate(tensor, cosine, sine, sign):
    half = ROT // 2
    first = tensor[..., :half]
    second = tensor[..., half:ROT]
    new_first = first * cosine - sign * second * sine
    new_second = second * cosine + sign * first * sine
    return jnp.concatenate([new_first, new_second, tensor[..., ROT:]], axis=-1)


def contract_rows(left, right):
    return lax.dot_general(
        left, right, (((0,), (0,)), ((), ())), preferred_element_type=jnp.float32
    )


def contract_cols(left, right):
    return lax.dot_general(
        left, right, (((1,), (1,)), ((), ())), preferred_element_type=jnp.float32
    )


def own_columns(matrix, cycle_size, shard_count, member):
    count = matrix.shape[0]
    piece_width = matrix.shape[1] // (cycle_size * shard_count)
    parted = matrix.reshape(count, cycle_size, shard_count, piece_width)
    return lax.dynamic_slice_in_dim(parted, member, 1, 2).reshape(count, cycle_size * piece_width)


def per_device(
    block_input,
    output_grad,
    segment,
    slots,
    ln_gain,
    ln_bias,
    qkv_w,
    qkv_b,
    dense_w,
    dense_b,
    fc1_w,
    fc1_b,
    fc2_w,
    fc2_b,
):
    cycle_size = lax.axis_size("ctx")
    index = lax.axis_index("ctx")
    shard_count = lax.axis_size("fsdp")
    member = lax.axis_index("fsdp")
    tokens = block_input.shape[1]
    width = block_input.shape[2]
    stretch = tokens // 2
    heads = HEADS
    head_dim = width // heads
    scale = head_dim ** (-0.5)
    seg_row = segment[0]
    slot_ids = jnp.arange(2 * cycle_size, dtype=jnp.int32)

    def positions(start, count):
        rows = start + jnp.arange(count, dtype=jnp.int32)
        slot = rows // stretch
        owner = jnp.sum(jnp.where(slot[:, None] == slot_ids[None, :], slots[None, :], 0), axis=1)
        return owner * stretch + rows % stretch

    qpos = positions(index * tokens, tokens)
    qdoc = jnp.take(seg_row, qpos)
    cosine, sine = rotary_tables(qpos)
    gain_all, norm_bias_every, w_qkv, b_qkv, w_up, b_up = (
        lax.all_gather(ln_gain, ("ctx", "fsdp"), axis=0, tiled=True),
        lax.all_gather(ln_bias, ("ctx", "fsdp"), axis=0, tiled=True),
        lax.all_gather(qkv_w, ("ctx", "fsdp"), axis=0, tiled=True),
        lax.all_gather(qkv_b, ("ctx", "fsdp"), axis=0, tiled=True),
        lax.all_gather(fc1_w, ("ctx", "fsdp"), axis=0, tiled=True),
        lax.all_gather(fc1_b, ("ctx", "fsdp"), axis=0, tiled=True),
    )
    xf = block_input[0].astype(jnp.float32)
    row_mean = jnp.mean(xf, axis=-1, keepdims=True)
    centered_input = xf - row_mean
    inverse_deviation = lax.rsqrt(
        jnp.mean(centered_input * centered_input, axis=-1, keepdims=True) + EPS
    )
    standardized_input = centered_input * inverse_deviation
    gain_float = gain_all.astype(jnp.float32)
    normed_rows = (standardized_input * gain_float + norm_bias_every.astype(jnp.float32)).astype(
        jnp.bfloat16
    )
    proj = jnp.dot(normed_rows, w_qkv, preferred_element_type=jnp.float32) + b_qkv.astype(
        jnp.float32
    )
    query = rotate(proj[:, :width].reshape(tokens, heads, head_dim), cosine, sine, 1.0).astype(
        jnp.bfloat16
    )
    keys = rotate(
        proj[:, width : 2 * width].reshape(tokens, heads, head_dim), cosine, sine, 1.0
    ).astype(jnp.bfloat16)
    keys_flat = keys.reshape(tokens, width)
    values = proj[:, 2 * width :].astype(jnp.bfloat16)
    acc = jnp.zeros((tokens, heads, head_dim), jnp.float32)
    top = jnp.full((heads, tokens), NEG, jnp.float32)
    key_piece = lax.all_gather(keys_flat, "ctx", axis=0, tiled=True)
    value_piece = lax.all_gather(values, "ctx", axis=0, tiled=True)
    count = key_piece.shape[0]
    kpos = positions(jnp.int32(0), count)
    kdoc = jnp.take(seg_row, kpos)
    mask = ((kpos[None, :] <= qpos[:, None]) & (kdoc[None, :] == qdoc[:, None]))[None]
    scores = (
        jnp.einsum(
            "qhd,khd->hqk",
            query,
            key_piece.reshape(count, heads, head_dim),
            preferred_element_type=jnp.float32,
        )
        * scale
    )
    scores = jnp.where(mask, scores, NEG)
    new_top = jnp.maximum(top, jnp.max(scores, axis=-1))
    factor = jnp.exp(top - new_top)
    expo = jnp.where(mask, jnp.exp(scores - new_top[..., None]), 0.0)
    total = jnp.sum(expo, axis=-1)
    part_sum = jnp.einsum(
        "hqk,khd->qhd",
        expo.astype(jnp.bfloat16),
        value_piece.reshape(count, heads, head_dim),
        preferred_element_type=jnp.float32,
    )
    acc = acc * factor.T[:, :, None] + part_sum
    acc, top, total = (acc, new_top, total)
    attn_heads = (acc / total.T[:, :, None]).astype(jnp.bfloat16)
    lse = top + jnp.log(total)
    attn = attn_heads.reshape(tokens, width)
    w_dense, b_dense, w_down, b_down = (
        lax.all_gather(dense_w, ("ctx", "fsdp"), axis=0, tiled=True),
        lax.all_gather(dense_b, ("ctx", "fsdp"), axis=0, tiled=True),
        lax.all_gather(fc2_w, ("ctx", "fsdp"), axis=0, tiled=True),
        lax.all_gather(fc2_b, ("ctx", "fsdp"), axis=0, tiled=True),
    )
    upper = jnp.dot(normed_rows, w_up, preferred_element_type=jnp.float32) + b_up.astype(
        jnp.float32
    )
    act_f, slope = gelu_pair(upper)
    act = act_f.astype(jnp.bfloat16)
    y_rows = (
        xf
        + jnp.dot(attn, w_dense, preferred_element_type=jnp.float32)
        + b_dense.astype(jnp.float32)
    )
    y_rows = (
        y_rows
        + jnp.dot(act, w_down, preferred_element_type=jnp.float32)
        + b_down.astype(jnp.float32)
    )
    grad_rows = output_grad[0]
    gradient_float = grad_rows.astype(jnp.float32)
    group_attn, group_act, group_grad = (
        lax.all_gather(attn, "fsdp", axis=0, tiled=True),
        lax.all_gather(act, "fsdp", axis=0, tiled=True),
        lax.all_gather(grad_rows, "fsdp", axis=0, tiled=True),
    )
    group_bias = jnp.sum(group_grad.astype(jnp.float32), axis=0)
    own_bias = own_columns(group_bias[None], cycle_size, shard_count, member)[0]
    dense_part = contract_rows(own_columns(group_attn, cycle_size, shard_count, member), group_grad)
    down_part = contract_rows(own_columns(group_act, cycle_size, shard_count, member), group_grad)
    g_dense_w, g_dense_b, g_fc2_w, g_fc2_b = (
        lax.psum_scatter(
            dense_part.astype(jnp.bfloat16), "ctx", scatter_dimension=0, tiled=True
        ).astype(jnp.float32),
        lax.psum_scatter(
            own_bias.astype(jnp.bfloat16), "ctx", scatter_dimension=0, tiled=True
        ).astype(jnp.float32),
        lax.psum_scatter(
            down_part.astype(jnp.bfloat16), "ctx", scatter_dimension=0, tiled=True
        ).astype(jnp.float32),
        lax.psum_scatter(
            own_bias.astype(jnp.bfloat16), "ctx", scatter_dimension=0, tiled=True
        ).astype(jnp.float32),
    )
    dup = contract_cols(grad_rows, w_down) * slope
    up_bias_grad = jnp.sum(dup, axis=0)
    dup_b = dup.astype(jnp.bfloat16)
    dattn = contract_cols(grad_rows, w_dense).astype(jnp.bfloat16).reshape(tokens, heads, head_dim)
    delta = jnp.sum(dattn.astype(jnp.float32) * attn_heads.astype(jnp.float32), axis=-1).T

    def cycle_step(step, carry):
        key_cur, value_cur, dkey_acc, dvalue_acc, dquery_acc = carry
        anchor = (index - step + cycle_size) % cycle_size
        kpos = positions(anchor * tokens, tokens)
        kdoc = jnp.take(seg_row, kpos)
        mask = ((kpos[None, :] <= qpos[:, None]) & (kdoc[None, :] == qdoc[:, None]))[None]
        key_heads = key_cur.reshape(tokens, heads, head_dim)
        scores = (
            jnp.einsum("qhd,khd->hqk", query, key_heads, preferred_element_type=jnp.float32) * scale
        )
        probs = jnp.where(mask, jnp.exp(jnp.where(mask, scores, NEG) - lse[..., None]), 0.0)
        dvalue_acc = dvalue_acc + jnp.einsum(
            "hqk,qhd->khd", probs.astype(jnp.bfloat16), dattn, preferred_element_type=jnp.float32
        ).reshape(tokens, width)
        dprob = jnp.einsum(
            "qhd,khd->hqk",
            dattn,
            value_cur.reshape(tokens, heads, head_dim),
            preferred_element_type=jnp.float32,
        )
        dscore = (probs * (dprob - delta[..., None]) * scale).astype(jnp.bfloat16)
        dquery_acc = dquery_acc + jnp.einsum(
            "hqk,khd->qhd", dscore, key_heads, preferred_element_type=jnp.float32
        )
        dkey_acc = dkey_acc + jnp.einsum(
            "hqk,qhd->khd", dscore, query, preferred_element_type=jnp.float32
        ).reshape(tokens, width)
        key_cur, value_cur = shifted((key_cur, value_cur), "ctx", 1)
        dkey_acc, dvalue_acc = (
            shifted(dkey_acc.astype(jnp.bfloat16), "ctx", 1).astype(dkey_acc.dtype),
            shifted(dvalue_acc.astype(jnp.bfloat16), "ctx", 1).astype(dvalue_acc.dtype),
        )
        return (key_cur, value_cur, dkey_acc, dvalue_acc, dquery_acc)

    flat_zero = jnp.zeros((tokens, width), jnp.float32)
    cycle_init = (
        keys_flat,
        values,
        flat_zero,
        flat_zero,
        jnp.zeros((tokens, heads, head_dim), jnp.float32),
    )
    cycle_out = lax.fori_loop(0, cycle_size, cycle_step, cycle_init)
    dkey_sum, dvalue_sum, dquery_sum = (cycle_out[2], cycle_out[3], cycle_out[4])
    dquery = rotate(dquery_sum, cosine, sine, -1.0).reshape(tokens, width)
    dkey = rotate(dkey_sum.reshape(tokens, heads, head_dim), cosine, sine, -1.0).reshape(
        tokens, width
    )
    dproj = jnp.concatenate([dquery, dkey, dvalue_sum], axis=1)
    qkv_bias_grad = jnp.sum(dproj, axis=0)
    dproj_b = dproj.astype(jnp.bfloat16)
    normed_input_grad = contract_cols(dproj_b, w_qkv) + contract_cols(dup_b, w_up)
    gain_gradient = jnp.sum(normed_input_grad * standardized_input, axis=0)
    lnb_grad = jnp.sum(normed_input_grad, axis=0)
    scaled_rows = normed_input_grad * gain_float
    dx_rows = gradient_float + inverse_deviation * (
        scaled_rows
        - jnp.mean(scaled_rows, axis=-1, keepdims=True)
        - standardized_input * jnp.mean(scaled_rows * standardized_input, axis=-1, keepdims=True)
    )
    group_normed, group_dproj, group_dup = (
        lax.all_gather(normed_rows, "fsdp", axis=0, tiled=True),
        lax.all_gather(dproj_b, "fsdp", axis=0, tiled=True),
        lax.all_gather(dup_b, "fsdp", axis=0, tiled=True),
    )
    own_normed = own_columns(group_normed, cycle_size, shard_count, member)
    g_qkv_w, g_fc1_w = (
        lax.psum_scatter(
            contract_rows(own_normed, group_dproj).astype(jnp.bfloat16),
            "ctx",
            scatter_dimension=0,
            tiled=True,
        ).astype(jnp.float32),
        lax.psum_scatter(
            contract_rows(own_normed, group_dup).astype(jnp.bfloat16),
            "ctx",
            scatter_dimension=0,
            tiled=True,
        ).astype(jnp.float32),
    )
    layer_gain_grad, g_lnb, g_qkv_b, g_fc1_b = (
        lax.psum_scatter(gain_gradient, ("ctx", "fsdp"), scatter_dimension=0, tiled=True),
        lax.psum_scatter(lnb_grad, ("ctx", "fsdp"), scatter_dimension=0, tiled=True),
        lax.psum_scatter(qkv_bias_grad, ("ctx", "fsdp"), scatter_dimension=0, tiled=True),
        lax.psum_scatter(up_bias_grad, ("ctx", "fsdp"), scatter_dimension=0, tiled=True),
    )
    return (
        y_rows.astype(jnp.bfloat16)[None],
        dx_rows[None],
        layer_gain_grad,
        g_lnb,
        g_qkv_w,
        g_qkv_b,
        g_dense_w,
        g_dense_b,
        g_fc1_w,
        g_fc1_b,
        g_fc2_w,
        g_fc2_b,
    )


BF = jnp.bfloat16
F32 = jnp.float32
MESH = pl.DeviceIdType.MESH
HBM = pl.BlockSpec(memory_space=pl.ANY)
VM = pl.BlockSpec(memory_space=pltpu.VMEM)
DMA = pltpu.SemaphoreType.DMA
VLIM = 60 * 1024 * 1024


def place():
    ctx, z = lax.axis_index("ctx"), lax.axis_index("fsdp")
    return ctx, lax.div(ctx, 4), lax.rem(lax.div(ctx, 2), 2), lax.rem(ctx, 2), z


class Net:
    def __init__(self):
        self.ctx, self.y, self.x, self.c, self.z = place()
        self.yb, self.xb, self.cb = 1 - self.y, 1 - self.x, 1 - self.c
        self.m = self.y * 4 + self.z
        self.g = self.x * 2 + self.c
        self.to_y = {"ctx": self.ctx + 4 * (1 - 2 * self.y), "fsdp": self.z}
        self.to_x = {"ctx": self.ctx + 2 * (1 - 2 * self.x), "fsdp": self.z}
        self.to_c = {"ctx": self.ctx + 1 - 2 * self.c, "fsdp": self.z}
        self.up = {"ctx": self.ctx, "fsdp": self.z + 1}
        self.dn = {"ctx": self.ctx, "fsdp": self.z - 1}
        self.sent = []

    def member(self, q):
        flip, step = q // 4, q % 4
        z = lax.rem(self.z + step, 4)
        yy = self.yb if flip else self.y
        return {"ctx": self.ctx + flip * 4 * (1 - 2 * self.y), "fsdp": z}, yy, z

    def source(self, q):
        flip, step = q // 4, q % 4
        return (self.yb if flip else self.y), lax.rem(self.z + 4 - step, 4)

    def barrier(self, members=True, square=True):
        sem = pltpu.get_barrier_semaphore()
        peers = [self.member(q)[0] for q in range(1, 8)] if members else []
        if square:
            peers += [self.to_x, self.to_c]
        for peer in peers:
            pl.semaphore_signal(sem, inc=1, device_id=peer, device_id_type=MESH)
        pl.semaphore_wait(sem, len(peers))

    def go(self, copy, when=None):
        if when is None:
            copy.start()
        else:
            pl.when(when)(copy.start)
        self.sent.append((copy, when))

    def drain(self):
        for copy, when in self.sent:
            if when is None:
                copy.wait_send()
            else:
                pl.when(when)(copy.wait_send)


def remote(src, dst, send, recv, to):
    return pltpu.make_async_remote_copy(
        src_ref=src, dst_ref=dst, send_sem=send, recv_sem=recv, device_id=to, device_id_type=MESH
    )


def arrive(like, recv):
    pltpu.make_async_copy(like, like, recv).wait()


PARTS = ((0, 128), (128, 144))


def gather_kernel(xd, ws, es, w2, xdg, wc, eg, w2g, loc, us, ur, ds_, dr, ys, yr, as_, ar, es_, er,
                  wxs, wxr, wks, wkr, exs, exr, eks, ekr, fxs, fxr, fks, fkr):
    n = Net()
    n.barrier()

    def wrow(yy, xx, cc, zz):
        return wc.at[pl.ds(pl.multiple_of((yy * 16 + xx * 8 + cc * 4 + zz) * 64, 64), 64)]

    def wide(gg):
        return w2g.at[pl.ds(pl.multiple_of(gg * 256, 256), 256)]

    def thin(gg):
        return w2g.at[pl.ds(pl.multiple_of(1024 + gg * 64, 64), 64)]

    def shard(zz, p):
        return xdg.at[n.y * 4 + zz, pl.ds(*PARTS[p])]

    for q in range(1, 8):
        to, yy, zz = n.member(q)
        n.go(remote(es.at[yy * 4 + zz], eg.at[n.g * 8 + n.m], es_.at[q], er.at[q], to))
        n.go(remote(ws.at[yy * 4 + zz], wrow(n.y, n.x, n.c, n.z), as_.at[q], ar.at[q], to))
    for p in range(2):
        rows = pl.ds(*PARTS[p])
        n.go(remote(xd.at[rows], shard(n.z, p), us.at[p, 0], ur.at[p, 0], n.up), n.z < 3)
        n.go(remote(xd.at[rows], shard(n.z, p), ds_.at[p, 0], dr.at[p, 0], n.dn), n.z > 0)
        n.go(remote(xd.at[rows], shard(n.z, p), ys.at[p, 0], yr.at[p, 0], n.to_y))
    halves = ((pl.ds(0, 256), wide), (pl.ds(256, 64), thin))
    for k, (rows, part) in enumerate(halves):
        n.go(remote(w2.at[rows], part(n.g), fxs.at[k], fxr.at[k], n.to_x))
        n.go(remote(w2.at[rows], part(n.g), fks.at[k], fkr.at[k], n.to_c))
    own = ws.at[n.m]
    n.go(remote(own, wrow(n.y, n.x, n.c, n.z), wxs.at[0], wxr.at[0], n.to_x))
    n.go(remote(own, wrow(n.y, n.x, n.c, n.z), wks.at[0], wkr.at[0], n.to_c))
    local = [
        pltpu.make_async_copy(xd, xdg.at[n.m], loc.at[0]),
        pltpu.make_async_copy(own, wrow(n.y, n.x, n.c, n.z), loc.at[1]),
        pltpu.make_async_copy(es.at[n.m], eg.at[n.g * 8 + n.m], loc.at[2]),
        pltpu.make_async_copy(w2.at[pl.ds(0, 256)], wide(n.g), loc.at[3]),
        pltpu.make_async_copy(w2.at[pl.ds(256, 64)], thin(n.g), loc.at[4]),
    ]
    for copy in local:
        copy.start()

    def line(d, p):
        below, above = n.z >= d, n.z + d <= 3

        @pl.when(below)
        def _():
            arrive(shard(n.z - d, p), ur.at[p, d - 1])

        if d < 3:
            n.go(remote(shard(n.z - d, p), shard(n.z - d, p), us.at[p, d], ur.at[p, d], n.up),
                 below & (n.z < 3))
        n.go(remote(shard(n.z - d, p), shard(n.z - d, p), ys.at[p, d], yr.at[p, d], n.to_y), below)

        @pl.when(above)
        def _():
            arrive(shard(n.z + d, p), dr.at[p, d - 1])

        if d < 3:
            n.go(remote(shard(n.z + d, p), shard(n.z + d, p), ds_.at[p, d], dr.at[p, d], n.dn),
                 above & (n.z > 0))
        n.go(remote(shard(n.z + d, p), shard(n.z + d, p), ys.at[p, d + 3], yr.at[p, d + 3], n.to_y), above)

    def pieces(qs):
        for q in qs:
            yy, zz = n.source(q)
            block = wrow(yy, n.x, n.c, zz)
            arrive(block, ar.at[q])
            n.go(remote(block, block, wxs.at[q], wxr.at[q], n.to_x))
            n.go(remote(block, block, wks.at[q], wkr.at[q], n.to_c))

    def relay(qs):
        for q in qs:
            yy, zz = n.source(q)
            block = wrow(yy, n.xb, n.c, zz)
            arrive(block, wxr.at[q])
            n.go(remote(block, block, wks.at[8 + q], wkr.at[8 + q], n.to_c))

    line(1, 0)
    pieces((4, 1, 3))
    line(1, 1)
    pieces((5, 7, 2, 6))
    for q in range(1, 8):
        yy, zz = n.source(q)
        arrive(eg.at[n.g * 8 + yy * 4 + zz], er.at[q])
    local[2].wait()
    mine = eg.at[pl.ds(n.g * 8, 8)]
    n.go(remote(mine, mine, exs.at[0], exr.at[0], n.to_x))
    n.go(remote(mine, mine, eks.at[0], ekr.at[0], n.to_c))
    line(2, 0)
    line(2, 1)
    gx = n.xb * 2 + n.c
    for k, (rows, part) in enumerate(halves):
        arrive(part(gx), fxr.at[k])
        n.go(remote(part(gx), part(gx), fks.at[2 + k], fkr.at[2 + k], n.to_c))
    theirs = eg.at[pl.ds(gx * 8, 8)]
    relay((0, 4, 1, 3))
    line(3, 0)
    relay((5, 7, 2, 6))
    arrive(theirs, exr.at[0])
    n.go(remote(theirs, theirs, eks.at[1], ekr.at[1], n.to_c))
    line(3, 1)
    for q in range(8):
        yy, zz = n.source(q)
        arrive(wrow(yy, n.x, n.cb, zz), wkr.at[q])
        arrive(wrow(yy, n.xb, n.cb, zz), wkr.at[8 + q])
    for k in range(2):
        arrive(eg.at[pl.ds((2 * (n.xb if k else n.x) + n.cb) * 8, 8)], ekr.at[k])
        for j, (rows, part) in enumerate(halves):
            arrive(part(2 * (n.xb if k else n.x) + n.cb), fkr.at[2 * k + j])
    for p in range(2):
        rows = pl.ds(*PARTS[p])
        arrive(xdg.at[n.yb * 4 + n.z, rows], yr.at[p, 0])
        for d in range(1, 4):
            @pl.when(n.z >= d)
            def _():
                arrive(xdg.at[n.yb * 4 + n.z - d, rows], yr.at[p, d])

            @pl.when(n.z + d <= 3)
            def _():
                arrive(xdg.at[n.yb * 4 + n.z + d, rows], yr.at[p, d + 3])
    for k in (0, 1, 3, 4):
        local[k].wait()
    n.drain()


def gather_all(xd, ws, es, w2):
    sd = jax.ShapeDtypeStruct
    return pl.pallas_call(
        gather_kernel,
        name="gather_all",
        out_shape=(sd((8, 272, 2048), BF), sd((2048, 1792), BF), sd((32, 8, 1792), BF), sd((1280, 2048), BF)),
        in_specs=[VM] * 4,
        out_specs=(HBM,) * 4,
        scratch_shapes=[DMA((5,)), DMA((2, 3)), DMA((2, 3)), DMA((2, 3)), DMA((2, 3)), DMA((2, 7)), DMA((2, 7)),
                        DMA((8,)), DMA((8,)), DMA((8,)), DMA((8,)), DMA((8,)), DMA((8,)), DMA((16,)), DMA((16,)),
                        DMA((1,)), DMA((1,)), DMA((2,)), DMA((2,)), DMA((2,)), DMA((2,)), DMA((4,)), DMA((4,))],
        compiler_params=pltpu.CompilerParams(collective_id=1, has_side_effects=True, vmem_limit_bytes=VLIM),
    )(xd, ws, es, w2)


def exchange_kernel(src, dst, loc, ss, rs):
    n = Net()
    n_peer = {"ctx": n.ctx + 2 * (1 - 2 * n.x) + 1 - 2 * n.c, "fsdp": n.z}
    sem = pltpu.get_barrier_semaphore()
    for peer in (n.to_x, n.to_c, n_peer):
        pl.semaphore_signal(sem, inc=1, device_id=peer, device_id_type=MESH)
    pl.semaphore_wait(sem, 3)
    copies = []
    for k, (to, gg) in enumerate(((n_peer, 2 * n.xb + n.cb), (n.to_x, 2 * n.xb + n.c), (n.to_c, 2 * n.x + n.cb))):
        copies.append(remote(src.at[gg], dst.at[n.g], ss.at[k], rs.at[k], to))
    for copy in copies:
        copy.start()
    own = pltpu.make_async_copy(src.at[n.g], dst.at[n.g], loc)
    own.start()
    own.wait()
    for copy in copies:
        copy.wait()


def exchange(a, cid):
    return pl.pallas_call(
        exchange_kernel,
        name="exchange",
        out_shape=jax.ShapeDtypeStruct(a.shape, a.dtype),
        in_specs=[VM],
        out_specs=VM,
        scratch_shapes=[DMA, DMA((3,)), DMA((3,))],
        compiler_params=pltpu.CompilerParams(collective_id=cid, has_side_effects=True, vmem_limit_bytes=VLIM),
    )(a)


def lanes_of(shape):
    return lax.broadcasted_iota(jnp.int32, shape, len(shape) - 1)


def partner(t):
    low = lax.rem(lanes_of(t.shape), 64) < 16
    return jnp.where(low, pltpu.roll(t, 112, 1), pltpu.roll(t, 16, 1))


def dot_nt(a, b):
    return lax.dot_general(a, b, (((1,), (1,)), ((), ())), preferred_element_type=F32)


def dot_tn(a, b):
    return lax.dot_general(a, b, (((0,), (0,)), ((), ())), preferred_element_type=F32)


def project_kernel(xd, wc, w2, gain, bias, wbias, cos, sin, normed_o, qkvd_o, act_o, dup_o, dsum_o):
    xf = xd[0, 0:128, :].astype(F32)
    mean = jnp.mean(xf, axis=-1, keepdims=True)
    cen = xf - mean
    rstd = lax.rsqrt(jnp.mean(cen * cen, axis=-1, keepdims=True) + EPS)
    normed = (cen * rstd * gain[...] + bias[...]).astype(BF)
    normed_o[...] = normed
    dy = xd[0, 128:256, :]
    dd = dot_nt(dy, w2[1024:1280, :])
    half = lanes_of((128, 128)) < 64
    cosv, sinv = cos[0], sin[0]
    proj = jnp.dot(normed, wc[:, 0:768], preferred_element_type=F32) + wbias[:, 0:768]
    for g in range(4):
        t = proj[:, 128 * g : 128 * g + 128]
        qkvd_o[g, 0, :, 0:128] = (t * cosv + partner(t) * sinv).astype(BF)
        v = proj[:, 512 + 128 * (g // 2) : 640 + 128 * (g // 2)]
        d = dd[:, 128 * (g // 2) : 128 * (g // 2) + 128]
        if g % 2 == 0:
            vd = jnp.where(half, v, pltpu.roll(d, 64, 1))
        else:
            vd = jnp.where(half, pltpu.roll(v, 64, 1), d)
        qkvd_o[g, 0, :, 128:256] = vd.astype(BF)
    for k in range(4):
        cols = slice(256 * k, 256 * k + 256)
        up = jnp.dot(normed, wc[:, 768 + 256 * k : 1024 + 256 * k], preferred_element_type=F32)
        act, slope = gelu_pair(up + wbias[:, 768 + 256 * k : 1024 + 256 * k])
        act_o[:, cols] = act.astype(BF)
        dup = dot_nt(dy, w2[256 * k : 256 * k + 256, :]) * slope
        dup_o[:, cols] = dup.astype(BF)
        dsum = jnp.broadcast_to(jnp.sum(dup, axis=0, keepdims=True), (8, 256))

        @pl.when(pl.program_id(0) == 0)
        def _():
            dsum_o[:, cols] = dsum

        @pl.when(pl.program_id(0) > 0)
        def _():
            dsum_o[:, cols] += dsum


def project(xdg, wc, w2g, gain, bias, wbias, cos, sin):
    sd = jax.ShapeDtypeStruct
    one = pl.Buffered(1)

    def whole(shape):
        return pl.BlockSpec(shape, lambda i: (0,) * len(shape), pipeline_mode=one)

    return pl.pallas_call(
        project_kernel,
        name="project",
        grid=(8,),
        out_shape=(sd((1024, 2048), BF), sd((4, 8, 128, 256), BF), sd((1024, 1024), BF), sd((1024, 1024), BF),
                   sd((8, 1024), F32)),
        in_specs=[
            pl.BlockSpec((1, 272, 2048), lambda i: (i, 0, 0)),
            whole((2048, 1792)),
            whole((1280, 2048)),
            whole((1, 2048)),
            whole((1, 2048)),
            whole((1, 1792)),
            pl.BlockSpec((1, 128, 128), lambda i: (i // 4, 0, 0)),
            pl.BlockSpec((1, 128, 128), lambda i: (i // 4, 0, 0)),
        ],
        out_specs=(
            pl.BlockSpec((128, 2048), lambda i: (i, 0)),
            pl.BlockSpec((4, 1, 128, 256), lambda i: (0, i, 0, 0)),
            pl.BlockSpec((128, 1024), lambda i: (i, 0)),
            pl.BlockSpec((128, 1024), lambda i: (i, 0)),
            pl.BlockSpec((8, 1024), lambda i: (0, 0)),
        ),
        compiler_params=pltpu.CompilerParams(vmem_limit_bytes=VLIM),
    )(xdg, wc, w2g, gain, bias, wbias, cos, sin)


def attention_kernel(slot_of, a, doc_row, doc_col, cos, sin, out, sums, seq, att, dq, dk, dv):
    def where_is(p):
        r = slot_of[p]
        ctx = lax.div(r, 2)
        return lax.rem(ctx, 4), lax.div(ctx, 4), pl.ds(pl.multiple_of(lax.rem(r, 2) * 64, 64), 64)

    for p in range(16):
        g, yy, rows = where_is(p)
        seq[64 * p : 64 * p + 64, :] = a[g, yy, 0, rows, :]
    dk[...] = jnp.zeros_like(dk)
    dv[...] = jnp.zeros_like(dv)
    scale = 0.125
    low = lanes_of((256, 128)) < 64
    for i in range(4):
        k0 = max(0, i - 2) * 256
        kn = 256 * (i + 1) - k0
        rq, rk = slice(256 * i, 256 * i + 256), slice(k0, k0 + kn)
        qk, vd = seq[rq, 0:128], seq[rq, 128:256]
        kk, vv = seq[rk, 0:128], seq[rk, 128:256]
        zero = jnp.zeros((256, 128), F32)
        qs = jnp.where(low, zero, pltpu.roll(qk.astype(F32), 64, 1)).astype(BF)
        dsf = jnp.where(low, pltpu.roll(vd.astype(F32), 64, 1), zero)
        s = dot_nt(qs, kk) * scale
        qpos = 256 * i + lax.broadcasted_iota(jnp.int32, (256, kn), 0)
        kpos = k0 + lax.broadcasted_iota(jnp.int32, (256, kn), 1)
        mask = (kpos <= qpos) & (doc_row[0, :, rk] == doc_col[0, rq, :])
        s = jnp.where(mask, s, NEG)
        top = jnp.max(s, axis=-1, keepdims=True)
        e = jnp.where(mask, jnp.exp(s - top), 0.0)
        inv = 1.0 / jnp.sum(e, axis=-1, keepdims=True)
        o = jnp.dot(e.astype(BF), vv, preferred_element_type=F32) * inv
        ob = o.astype(BF)
        att[rq, :] = ob.astype(F32)
        delta = jnp.sum(dsf * ob.astype(F32), axis=-1, keepdims=True)
        pr = e * inv
        dv[rk, :] += dot_tn(pr.astype(BF), vd)
        dp = dot_nt(dsf.astype(BF), vv)
        ds = (pr * (dp - delta) * scale).astype(BF)
        dq[rq, :] = jnp.dot(ds, kk, preferred_element_type=F32)
        dk[rk, :] += dot_tn(ds, qk)
    tot = jnp.zeros((8, 256), F32)
    half = lanes_of((64, 128)) < 64
    s1 = jnp.zeros((1, 128), F32)
    s2 = jnp.zeros((1, 128), F32)
    for p in range(16):
        rows = slice(64 * p, 64 * p + 64)
        g, yy, place_rows = where_is(p)
        t = jnp.where(half, pltpu.roll(dq[rows, :], 64, 1), pltpu.roll(dk[rows, :], 64, 1))
        t = t * cos[rows, :] - partner(t) * sin[rows, :]
        u = jnp.where(half, pltpu.roll(dv[rows, :], 64, 1), pltpu.roll(att[rows, :], 64, 1))
        s1 += jnp.sum(t, axis=0, keepdims=True)
        s2 += jnp.sum(u, axis=0, keepdims=True)
        out[g, yy, 0, place_rows, 0:128] = t.astype(BF)
        out[g, yy, 0, place_rows, 128:256] = u.astype(BF)
    sums[0, :, 0:128] = jnp.broadcast_to(s1, (8, 128))
    sums[0, :, 128:256] = jnp.broadcast_to(s2, (8, 128))


def attention(slot_of, a, docs, cos, sin):
    sd = jax.ShapeDtypeStruct
    blk = pl.BlockSpec((4, 2, 1, 128, 256), lambda s, t: (0, 0, s, 0, 0))
    return pl.pallas_call(
        attention_kernel,
        name="attention",
        grid_spec=pltpu.PrefetchScalarGridSpec(
            num_scalar_prefetch=1,
            grid=(4,),
            in_specs=[
                blk,
                pl.BlockSpec((1, 1, 1024), lambda s, t: (s, 0, 0)),
                pl.BlockSpec((1, 1024, 1), lambda s, t: (s, 0, 0)),
                pl.BlockSpec((1024, 128), lambda s, t: (0, 0)),
                pl.BlockSpec((1024, 128), lambda s, t: (0, 0)),
            ],
            out_specs=(blk, pl.BlockSpec((1, 8, 256), lambda s, t: (s, 0, 0))),
            scratch_shapes=[pltpu.VMEM((1024, 256), BF)] + [pltpu.VMEM((1024, 128), F32)] * 4,
        ),
        out_shape=(sd((4, 2, 4, 128, 256), BF), sd((4, 8, 256), F32)),
        compiler_params=pltpu.CompilerParams(vmem_limit_bytes=VLIM),
    )(slot_of, a, docs[:, None, :], docs[:, :, None], cos, sin)


def add_rows(dst, srcs, rows, out=None, step=16):
    out = dst if out is None else out

    def body(i, carry):
        sl = pl.ds(pl.multiple_of(i * step, step), step)
        v = dst[sl, :].astype(F32)
        for s in srcs:
            v = v + s[sl, :].astype(F32)
        out[sl, :] = v.astype(out.dtype)
        return carry

    lax.fori_loop(0, rows // step, body, 0)


def reduce_kernel(part, dw1, dw2, e1, yo, o1, o2, eo, own, yr, ub, db, w1, r1, r2, w2, s1, s2, ev, t1, t2,
                  ol, wl, vl, yss, yrs, uss, urs, dss, drs, k1s, k1r, x1s, x1r, a1s, a1r,
                  k2s, k2r, x2s, x2r, eks, ekr, exs, exr, eas, ear, fl):
    n = Net()
    n.barrier()
    order = (3, 0, 2, 1)

    def block(yy, xx, cc):
        return dw1.at[pl.ds(pl.multiple_of((yy * 16 + xx * 8 + cc * 4) * 64, 256), 256)]

    def wide(gg):
        return dw2.at[pl.ds(pl.multiple_of(gg * 256, 256), 256)]

    def thin(gg):
        return dw2.at[pl.ds(pl.multiple_of(1024 + gg * 64, 64), 64)]

    load_own = {}
    for t in range(2):
        for k in order:
            n.go(remote(part.at[n.yb * 4 + k, t], yr.at[k, t], yss.at[t, k], yrs.at[t, k], n.to_y))
    for xx in range(2):
        gg = 2 * xx + n.cb
        n.go(remote(e1.at[pl.ds(gg * 8, 8)], t1.at[xx], eks.at[xx], ekr.at[xx], n.to_c))
        n.go(remote(wide(gg), s1.at[xx, pl.ds(0, 256)], k2s.at[xx, 0], k2r.at[xx, 0], n.to_c))
        n.go(remote(thin(gg), s1.at[xx, pl.ds(256, 64)], k2s.at[xx, 1], k2r.at[xx, 1], n.to_c))
        for yy in range(2):
            n.go(remote(block(yy, xx, n.cb), r1.at[yy * 2 + xx], k1s.at[yy * 2 + xx], k1r.at[yy * 2 + xx], n.to_c))
    loads = []
    for xx in range(2):
        gg = 2 * xx + n.c
        loads.append(pltpu.make_async_copy(e1.at[pl.ds(gg * 8, 8)], ev.at[xx], vl.at[xx, 0]))
        loads.append(pltpu.make_async_copy(wide(gg), w2.at[xx, pl.ds(0, 256)], vl.at[xx, 1]))
        loads.append(pltpu.make_async_copy(thin(gg), w2.at[xx, pl.ds(256, 64)], vl.at[xx, 2]))
        for yy in range(2):
            loads.append(pltpu.make_async_copy(block(yy, xx, n.c), w1.at[yy * 2 + xx], wl.at[yy * 2 + xx]))
    for t in range(2):
        for k in order:
            load_own[t, k] = pltpu.make_async_copy(part.at[n.y * 4 + k, t], own.at[k, t], ol.at[t, k])
    for copy in loads + list(load_own.values()):
        copy.start()
    for copy in loads:
        copy.wait()

    for xx in range(2):
        arrive(t1.at[xx], ekr.at[xx])
        ev[xx] = ev[xx] + t1[xx]
        arrive(s1.at[xx, pl.ds(0, 256)], k2r.at[xx, 0])
        arrive(s1.at[xx, pl.ds(256, 64)], k2r.at[xx, 1])
        add_rows(w2.at[xx], [s1.at[xx]], 320)
        for yy in range(2):
            arrive(r1.at[yy * 2 + xx], k1r.at[yy * 2 + xx])
            add_rows(w1.at[yy * 2 + xx], [r1.at[yy * 2 + xx]], 256)
    n.go(remote(ev.at[n.xb], t2, exs.at[0], exr.at[0], n.to_x))
    for yy in range(2):
        n.go(remote(w1.at[yy * 2 + n.xb], r2.at[yy], x1s.at[yy], x1r.at[yy], n.to_x))
    n.go(remote(w2.at[n.xb], s2, x2s.at[0], x2r.at[0], n.to_x))

    def forward(t, k):
        def send_up():
            return remote(own.at[k, t], ub.at[k, t], uss.at[t, k], urs.at[t, k], n.up)

        def send_down():
            return remote(own.at[k, t], db.at[k, t], dss.at[t, k], drs.at[t, k], n.dn)

        @pl.when(n.z != k)
        def _():
            load_own[t, k].wait()
            arrive(yr.at[k, t], yrs.at[t, k])
        if k > 0:
            @pl.when(n.z == 0)
            def _():
                add_rows(own.at[k, t], [yr.at[k, t]], 128)

            if k > 1:
                @pl.when((n.z > 0) & (n.z < k))
                def _():
                    arrive(ub.at[k, t], urs.at[t, k])
                    add_rows(own.at[k, t], [yr.at[k, t], ub.at[k, t]], 128)

            n.go(send_up(), n.z < k)
        if k < 3:
            @pl.when(n.z == 3)
            def _():
                add_rows(own.at[k, t], [yr.at[k, t]], 128)

            if k < 2:
                @pl.when((n.z < 3) & (n.z > k))
                def _():
                    arrive(db.at[k, t], drs.at[t, k])
                    add_rows(own.at[k, t], [yr.at[k, t], db.at[k, t]], 128)

            n.go(send_down(), n.z > k)

    def finish(t, k):
        @pl.when(n.z == k)
        def _():
            load_own[t, k].wait()
            arrive(yr.at[k, t], yrs.at[t, k])
            more = [yr.at[k, t]]
            if k > 0:
                arrive(ub.at[k, t], urs.at[t, k])
                more.append(ub.at[k, t])
            if k < 3:
                arrive(db.at[k, t], drs.at[t, k])
                more.append(db.at[k, t])
            add_rows(own.at[k, t], more, 128, yo.at[t])

    for k in order:
        forward(0, k)
    arrive(t2, exr.at[0])
    ev[n.x] = ev[n.x] + t2[...]
    for q in range(1, 8):
        to, yy, zz = n.member(q)
        n.go(remote(ev.at[n.x, yy * 4 + zz], eo.at[n.m], eas.at[q], ear.at[q], to))
    eo[n.m] = ev[n.x, n.m]
    for yy in range(2):
        arrive(r2.at[yy], x1r.at[yy])
        add_rows(w1.at[yy * 2 + n.x], [r2.at[yy]], 256)
    for q in (4, 1, 3, 5, 7, 2, 6):
        to, yy, zz = n.member(q)
        n.go(remote(w1.at[yy * 2 + n.x, pl.ds(pl.multiple_of(zz * 64, 64), 64)], o1.at[n.m], a1s.at[q], a1r.at[q], to))
    mine = pltpu.make_async_copy(w1.at[n.y * 2 + n.x, pl.ds(pl.multiple_of(n.z * 64, 64), 64)], o1.at[n.m], fl.at[0])
    mine.start()
    for k in order:
        forward(1, k)
    arrive(s2, x2r.at[0])
    add_rows(w2.at[n.x], [s2], 320, o2)
    for t in range(2):
        for k in range(4):
            finish(t, k)
    for q in range(1, 8):
        yy, zz = n.source(q)
        arrive(eo.at[yy * 4 + zz], ear.at[q])
        arrive(o1.at[yy * 4 + zz], a1r.at[q])
    mine.wait()
    n.drain()


def reduce_all(part, dw1, dw2, e1):
    sd = jax.ShapeDtypeStruct
    V = pltpu.VMEM
    return pl.pallas_call(
        reduce_kernel,
        name="reduce_all",
        out_shape=(sd((2, 128, 2048), F32), sd((8, 64, 1792), BF), sd((320, 2048), F32), sd((8, 16, 128), F32)),
        in_specs=[HBM, HBM, HBM, VM],
        out_specs=(VM, VM, VM, VM),
        scratch_shapes=[
            V((4, 2, 128, 2048), BF), V((4, 2, 128, 2048), BF), V((4, 2, 128, 2048), BF), V((4, 2, 128, 2048), BF),
            V((4, 256, 1792), BF), V((4, 256, 1792), BF), V((2, 256, 1792), BF),
            V((2, 320, 2048), BF), V((2, 320, 2048), BF), V((320, 2048), BF),
            V((2, 8, 16, 128), F32), V((2, 8, 16, 128), F32), V((8, 16, 128), F32),
            DMA((2, 4)), DMA((4,)), DMA((2, 3)),
            DMA((2, 4)), DMA((2, 4)), DMA((2, 4)), DMA((2, 4)), DMA((2, 4)), DMA((2, 4)),
            DMA((4,)), DMA((4,)), DMA((2,)), DMA((2,)), DMA((8,)), DMA((8,)),
            DMA((2, 2)), DMA((2, 2)), DMA((1,)), DMA((1,)),
            DMA((2,)), DMA((2,)), DMA((1,)), DMA((1,)), DMA((8,)), DMA((8,)), DMA((1,)),
        ],
        compiler_params=pltpu.CompilerParams(collective_id=3, has_side_effects=True, vmem_limit_bytes=VLIM),
    )(part, dw1, dw2, e1)


def member_columns(qkv, ff):
    rows = qkv.shape[0]
    parts = qkv.reshape(rows, 3, 2, 4, 4, 64)
    qk = parts[:, :2].transpose(2, 4, 0, 3, 1, 5).reshape(8, rows, 512)
    v = parts[:, 2].transpose(1, 3, 0, 2, 4).reshape(8, rows, 256)
    f = ff.reshape(rows, 2, 4, 4, 256).transpose(1, 3, 0, 2, 4).reshape(8, rows, 1024)
    return jnp.concatenate([qk, v, f], axis=2)


def stored_columns(a):
    rows = a.shape[1]
    qk = a[:, :, :512].reshape(2, 4, rows, 4, 2, 64).transpose(2, 4, 0, 3, 1, 5).reshape(rows, 2, 2048)
    v = a[:, :, 512:768].reshape(2, 4, rows, 4, 64).transpose(2, 0, 3, 1, 4).reshape(rows, 1, 2048)
    f = a[:, :, 768:1792].reshape(2, 4, rows, 4, 256).transpose(2, 0, 3, 1, 4).reshape(rows, 8192)
    return jnp.concatenate([qk, v], axis=1).reshape(rows, 6144), f


def rotary_lanes(pos):
    half = ROT // 2
    freqs = jnp.exp(-(2.0 * jnp.arange(half, dtype=F32) / ROT) * math.log(10000.0))
    angles = pos.astype(F32)[..., None] * freqs
    c, s = jnp.cos(angles), jnp.sin(angles)
    one = jnp.ones(pos.shape + (32,), F32)
    cos = jnp.concatenate([c, c, one] * 2, axis=-1)
    sin = jnp.concatenate([-s, s, 0.0 * one] * 2, axis=-1)
    return cos, sin


def fast_device(
    block_input, output_grad, segment, slots, ln_gain, ln_bias, qkv_w, qkv_b, dense_w, dense_b, fc1_w, fc1_b, fc2_w, fc2_b
):
    ctx, y, x, c, z = place()
    g, m = x * 2 + c, y * 4 + z
    index = ctx * 4 + z
    xb, dyb = block_input[0], output_grad[0]

    docs = jnp.zeros((16, 2048), BF).at[0, :1024].set(segment[0].astype(BF))
    xd = jnp.concatenate([xb, dyb, docs], axis=0)
    ws = member_columns(qkv_w, fc1_w)

    def spread(piece, total):
        return lax.dynamic_update_slice(jnp.zeros((total,), BF), piece, (index * piece.shape[0],))

    wb = member_columns(spread(qkv_b, 6144)[None], spread(fc1_b, 8192)[None])
    small = jnp.stack([spread(v, 2048) for v in (ln_gain, ln_bias, dense_b, fc2_b)])
    rest = jnp.zeros((1792,), BF).at[:1024].set(small[:, 1792:].reshape(1024))
    es = jnp.concatenate([jnp.concatenate([small[:, :1792], rest[None], jnp.zeros((2, 1792), BF)])[None]] * 8)
    es = jnp.concatenate([wb, es], axis=1)
    w2 = jnp.concatenate([fc2_w, dense_w], axis=0)
    xdg, wc, eg, w2g = gather_all(xd, ws, es, w2)

    ext = jnp.sum(eg.astype(F32), axis=0)
    wbias = ext[0:1]
    vecs = jnp.concatenate([ext[1:5], ext[5, :1024].reshape(4, 256)], axis=1)
    gain, lnb, ob = vecs[0:1], vecs[1:2], vecs[2:3] + vecs[3:4]
    pos_of_row = slots[:, None] * 64 + jnp.arange(64, dtype=jnp.int32)[None]
    rows2 = lax.dynamic_slice_in_dim(pos_of_row.reshape(2, 4, 128), g, 1, 1).reshape(2, 128)
    cos, sin = rotary_lanes(rows2)
    normed, qkvd, act, dup, dsum = project(xdg, wc, w2g, gain, lnb, wbias, cos, sin)

    heads_in = exchange(qkvd.reshape(4, 1024, 256), 2)
    slot_of = jnp.sum(jnp.where(slots[None, :] == jnp.arange(16, dtype=jnp.int32)[:, None], jnp.arange(16, dtype=jnp.int32)[None, :], 0), axis=1)
    cosp, sinp = rotary_lanes(jnp.arange(1024, dtype=jnp.int32))
    docs4 = xdg[0:4, 256, 0:1024].astype(F32)
    att, sums = attention(slot_of, heads_in.reshape(4, 2, 4, 128, 256), docs4, cosp, sinp)
    back = exchange(att.reshape(4, 1024, 256), 4)

    dqk = back[:, :, 0:128].transpose(1, 0, 2).reshape(1024, 512)
    dvv = back[:, :, 128:192].transpose(1, 0, 2).reshape(1024, 256)
    attn = back[:, :, 192:256].transpose(1, 0, 2).reshape(1024, 256)
    dpr = jnp.concatenate([dqk, dvv, dup], axis=1)
    up2 = jnp.concatenate([act, attn], axis=1)
    dy_all = xdg[:, 128:256].reshape(1024, 2048)
    ypart = jnp.dot(up2, w2g, preferred_element_type=F32)
    dn = contract_cols(dpr, wc)
    xf = xdg[:, 0:128].reshape(1024, 2048).astype(F32)
    cen = xf - jnp.mean(xf, axis=-1, keepdims=True)
    xhat = cen * lax.rsqrt(jnp.mean(cen * cen, axis=-1, keepdims=True) + EPS)
    gpart = jnp.sum(dn * xhat, axis=0)
    bpart = jnp.sum(dn, axis=0)
    dw1 = contract_rows(normed, dpr).astype(BF)
    dw2 = contract_rows(up2, dy_all).astype(BF)
    part = jnp.stack([ypart.astype(BF).reshape(8, 128, 2048), dn.astype(BF).reshape(8, 128, 2048)], axis=1)

    hs = jnp.sum(sums[:, 0, :], axis=0)
    colq = lax.dynamic_update_slice(jnp.zeros((512,), F32), hs[:128], (g * 128,))
    colv = lax.dynamic_update_slice(jnp.zeros((256,), F32), hs[128:192], (g * 64,))
    cols = jnp.concatenate([colq, colv, dsum[0]])

    def rows_of(v):
        return v.reshape(2, 4, 4, 64).transpose(1, 0, 2, 3).reshape(32, 64)

    dsum_y = jnp.sum(dy_all.astype(F32), axis=0)
    e1 = jnp.concatenate(
        [jnp.broadcast_to(cols, (32, 1792)), rows_of(gpart), rows_of(bpart), rows_of(dsum_y), jnp.zeros((32, 64), F32)], axis=1
    ).reshape(32, 16, 128)
    yo, o1, o2, eo = reduce_all(part, dw1, dw2, e1)

    xf = xb.astype(F32)
    cen = xf - jnp.mean(xf, axis=-1, keepdims=True)
    rstd = lax.rsqrt(jnp.mean(cen * cen, axis=-1, keepdims=True) + EPS)
    xhat = cen * rstd
    out = (xf + yo[0] + ob).astype(BF)
    gr = yo[1] * gain
    dx = dyb.astype(F32) + rstd * (
        gr - jnp.mean(gr, axis=-1, keepdims=True) - xhat * jnp.mean(gr * xhat, axis=-1, keepdims=True)
    )
    g_qkv_w, g_fc1_w = stored_columns(o1.astype(F32))
    eo = eo.reshape(8, 2048)
    sq, sf = stored_columns(eo[:, None, :1792])
    g_qkv_b = lax.dynamic_slice_in_dim(sq[0], index * 192, 192, 0)
    g_fc1_b = lax.dynamic_slice_in_dim(sf[0], index * 256, 256, 0)
    g_gain = jnp.sum(eo[:, 1792:1856], axis=0)
    g_lnb = jnp.sum(eo[:, 1856:1920], axis=0)
    g_db = eo[0, 1920:1984]
    return (out[None], dx[None], g_gain, g_lnb, g_qkv_w, g_qkv_b, o2[256:], g_db, g_fc1_w, g_fc1_b, o2[:256], g_db)


def solution(mesh):
    in_specs = (
        P("fsdp", "ctx", None),
        P("fsdp", "ctx", None),
        P("fsdp", None),
        P(),
        P(("ctx", "fsdp")),
        P(("ctx", "fsdp")),
        P(("ctx", "fsdp"), None),
        P(("ctx", "fsdp")),
        P(("ctx", "fsdp"), None),
        P(("ctx", "fsdp")),
        P(("ctx", "fsdp"), None),
        P(("ctx", "fsdp")),
        P(("ctx", "fsdp"), None),
        P(("ctx", "fsdp")),
    )
    out_specs = (
        P("fsdp", "ctx", None),
        P("fsdp", "ctx", None),
        P(("ctx", "fsdp")),
        P(("ctx", "fsdp")),
        P(("ctx", "fsdp"), None),
        P(("ctx", "fsdp")),
        P(("ctx", "fsdp"), None),
        P(("ctx", "fsdp")),
        P(("ctx", "fsdp"), None),
        P(("ctx", "fsdp")),
        P(("ctx", "fsdp"), None),
        P(("ctx", "fsdp")),
    )
    small = mesh.shape["ctx"] == 8 and mesh.shape["fsdp"] == 4
    return jax.shard_map(
        fast_device if small else per_device, mesh=mesh, in_specs=in_specs, out_specs=out_specs, check_vma=False
    )
```

```python
import math

import jax
import jax.numpy as jnp
from jax import lax
from jax.experimental import pallas as pl
from jax.experimental.pallas import tpu as pltpu
from jax.sharding import PartitionSpec as P

HEADS = 32
ROT = 32


EPS = 1e-05
GELU_C = math.sqrt(2.0 / math.pi)
NEG = -1e30


def shifted(block, axis, distance):
    devices = range(lax.axis_size(axis))
    route = [((i - distance) % len(devices), i) for i in devices]
    return lax.ppermute(block, axis, route)


def gelu_pair(upper):
    inner = GELU_C * (upper + 0.044715 * upper * upper * upper)
    tanh_val = jnp.tanh(inner)
    value = 0.5 * upper * (1.0 + tanh_val)
    slope = 0.5 * (1.0 + tanh_val) + 0.5 * upper * (1.0 - tanh_val * tanh_val) * GELU_C * (
        1.0 + 3.0 * 0.044715 * upper * upper
    )
    return (value, slope)


def rotary_tables(positions):
    half = ROT // 2
    freqs = jnp.exp(-(2.0 * jnp.arange(half, dtype=jnp.float32) / ROT) * math.log(10000.0))
    angles = positions.astype(jnp.float32)[:, None] * freqs[None, :]
    return (jnp.cos(angles)[:, None, :], jnp.sin(angles)[:, None, :])


def rotate(tensor, cosine, sine, sign):
    half = ROT // 2
    first = tensor[..., :half]
    second = tensor[..., half:ROT]
    new_first = first * cosine - sign * second * sine
    new_second = second * cosine + sign * first * sine
    return jnp.concatenate([new_first, new_second, tensor[..., ROT:]], axis=-1)


def contract_rows(left, right):
    return lax.dot_general(
        left, right, (((0,), (0,)), ((), ())), preferred_element_type=jnp.float32
    )


def contract_cols(left, right):
    return lax.dot_general(
        left, right, (((1,), (1,)), ((), ())), preferred_element_type=jnp.float32
    )


def own_columns(matrix, cycle_size, shard_count, member):
    count = matrix.shape[0]
    piece_width = matrix.shape[1] // (cycle_size * shard_count)
    parted = matrix.reshape(count, cycle_size, shard_count, piece_width)
    return lax.dynamic_slice_in_dim(parted, member, 1, 2).reshape(count, cycle_size * piece_width)


def per_device(
    block_input,
    output_grad,
    segment,
    slots,
    ln_gain,
    ln_bias,
    qkv_w,
    qkv_b,
    dense_w,
    dense_b,
    fc1_w,
    fc1_b,
    fc2_w,
    fc2_b,
):
    cycle_size = lax.axis_size("ctx")
    index = lax.axis_index("ctx")
    shard_count = lax.axis_size("fsdp")
    member = lax.axis_index("fsdp")
    tokens = block_input.shape[1]
    width = block_input.shape[2]
    stretch = tokens // 2
    heads = HEADS
    head_dim = width // heads
    scale = head_dim ** (-0.5)
    seg_row = segment[0]
    slot_ids = jnp.arange(2 * cycle_size, dtype=jnp.int32)

    def positions(start, count):
        rows = start + jnp.arange(count, dtype=jnp.int32)
        slot = rows // stretch
        owner = jnp.sum(jnp.where(slot[:, None] == slot_ids[None, :], slots[None, :], 0), axis=1)
        return owner * stretch + rows % stretch

    qpos = positions(index * tokens, tokens)
    qdoc = jnp.take(seg_row, qpos)
    cosine, sine = rotary_tables(qpos)
    gain_all, norm_bias_every, w_qkv, b_qkv, w_up, b_up = (
        lax.all_gather(ln_gain, ("ctx", "fsdp"), axis=0, tiled=True),
        lax.all_gather(ln_bias, ("ctx", "fsdp"), axis=0, tiled=True),
        lax.all_gather(qkv_w, ("ctx", "fsdp"), axis=0, tiled=True),
        lax.all_gather(qkv_b, ("ctx", "fsdp"), axis=0, tiled=True),
        lax.all_gather(fc1_w, ("ctx", "fsdp"), axis=0, tiled=True),
        lax.all_gather(fc1_b, ("ctx", "fsdp"), axis=0, tiled=True),
    )
    xf = block_input[0].astype(jnp.float32)
    row_mean = jnp.mean(xf, axis=-1, keepdims=True)
    centered_input = xf - row_mean
    inverse_deviation = lax.rsqrt(
        jnp.mean(centered_input * centered_input, axis=-1, keepdims=True) + EPS
    )
    standardized_input = centered_input * inverse_deviation
    gain_float = gain_all.astype(jnp.float32)
    normed_rows = (standardized_input * gain_float + norm_bias_every.astype(jnp.float32)).astype(
        jnp.bfloat16
    )
    proj = jnp.dot(normed_rows, w_qkv, preferred_element_type=jnp.float32) + b_qkv.astype(
        jnp.float32
    )
    query = rotate(proj[:, :width].reshape(tokens, heads, head_dim), cosine, sine, 1.0).astype(
        jnp.bfloat16
    )
    keys = rotate(
        proj[:, width : 2 * width].reshape(tokens, heads, head_dim), cosine, sine, 1.0
    ).astype(jnp.bfloat16)
    keys_flat = keys.reshape(tokens, width)
    values = proj[:, 2 * width :].astype(jnp.bfloat16)
    acc = jnp.zeros((tokens, heads, head_dim), jnp.float32)
    top = jnp.full((heads, tokens), NEG, jnp.float32)
    key_piece = lax.all_gather(keys_flat, "ctx", axis=0, tiled=True)
    value_piece = lax.all_gather(values, "ctx", axis=0, tiled=True)
    count = key_piece.shape[0]
    kpos = positions(jnp.int32(0), count)
    kdoc = jnp.take(seg_row, kpos)
    mask = ((kpos[None, :] <= qpos[:, None]) & (kdoc[None, :] == qdoc[:, None]))[None]
    scores = (
        jnp.einsum(
            "qhd,khd->hqk",
            query,
            key_piece.reshape(count, heads, head_dim),
            preferred_element_type=jnp.float32,
        )
        * scale
    )
    scores = jnp.where(mask, scores, NEG)
    new_top = jnp.maximum(top, jnp.max(scores, axis=-1))
    factor = jnp.exp(top - new_top)
    expo = jnp.where(mask, jnp.exp(scores - new_top[..., None]), 0.0)
    total = jnp.sum(expo, axis=-1)
    part_sum = jnp.einsum(
        "hqk,khd->qhd",
        expo.astype(jnp.bfloat16),
        value_piece.reshape(count, heads, head_dim),
        preferred_element_type=jnp.float32,
    )
    acc = acc * factor.T[:, :, None] + part_sum
    acc, top, total = (acc, new_top, total)
    attn_heads = (acc / total.T[:, :, None]).astype(jnp.bfloat16)
    lse = top + jnp.log(total)
    attn = attn_heads.reshape(tokens, width)
    w_dense, b_dense, w_down, b_down = (
        lax.all_gather(dense_w, ("ctx", "fsdp"), axis=0, tiled=True),
        lax.all_gather(dense_b, ("ctx", "fsdp"), axis=0, tiled=True),
        lax.all_gather(fc2_w, ("ctx", "fsdp"), axis=0, tiled=True),
        lax.all_gather(fc2_b, ("ctx", "fsdp"), axis=0, tiled=True),
    )
    upper = jnp.dot(normed_rows, w_up, preferred_element_type=jnp.float32) + b_up.astype(
        jnp.float32
    )
    act_f, slope = gelu_pair(upper)
    act = act_f.astype(jnp.bfloat16)
    y_rows = (
        xf
        + jnp.dot(attn, w_dense, preferred_element_type=jnp.float32)
        + b_dense.astype(jnp.float32)
    )
    y_rows = (
        y_rows
        + jnp.dot(act, w_down, preferred_element_type=jnp.float32)
        + b_down.astype(jnp.float32)
    )
    grad_rows = output_grad[0]
    gradient_float = grad_rows.astype(jnp.float32)
    group_attn, group_act, group_grad = (
        lax.all_gather(attn, "fsdp", axis=0, tiled=True),
        lax.all_gather(act, "fsdp", axis=0, tiled=True),
        lax.all_gather(grad_rows, "fsdp", axis=0, tiled=True),
    )
    group_bias = jnp.sum(group_grad.astype(jnp.float32), axis=0)
    own_bias = own_columns(group_bias[None], cycle_size, shard_count, member)[0]
    dense_part = contract_rows(own_columns(group_attn, cycle_size, shard_count, member), group_grad)
    down_part = contract_rows(own_columns(group_act, cycle_size, shard_count, member), group_grad)
    g_dense_w, g_dense_b, g_fc2_w, g_fc2_b = (
        lax.psum_scatter(
            dense_part.astype(jnp.bfloat16), "ctx", scatter_dimension=0, tiled=True
        ).astype(jnp.float32),
        lax.psum_scatter(
            own_bias.astype(jnp.bfloat16), "ctx", scatter_dimension=0, tiled=True
        ).astype(jnp.float32),
        lax.psum_scatter(
            down_part.astype(jnp.bfloat16), "ctx", scatter_dimension=0, tiled=True
        ).astype(jnp.float32),
        lax.psum_scatter(
            own_bias.astype(jnp.bfloat16), "ctx", scatter_dimension=0, tiled=True
        ).astype(jnp.float32),
    )
    dup = contract_cols(grad_rows, w_down) * slope
    up_bias_grad = jnp.sum(dup, axis=0)
    dup_b = dup.astype(jnp.bfloat16)
    dattn = contract_cols(grad_rows, w_dense).astype(jnp.bfloat16).reshape(tokens, heads, head_dim)
    delta = jnp.sum(dattn.astype(jnp.float32) * attn_heads.astype(jnp.float32), axis=-1).T

    def cycle_step(step, carry):
        key_cur, value_cur, dkey_acc, dvalue_acc, dquery_acc = carry
        anchor = (index - step + cycle_size) % cycle_size
        kpos = positions(anchor * tokens, tokens)
        kdoc = jnp.take(seg_row, kpos)
        mask = ((kpos[None, :] <= qpos[:, None]) & (kdoc[None, :] == qdoc[:, None]))[None]
        key_heads = key_cur.reshape(tokens, heads, head_dim)
        scores = (
            jnp.einsum("qhd,khd->hqk", query, key_heads, preferred_element_type=jnp.float32) * scale
        )
        probs = jnp.where(mask, jnp.exp(jnp.where(mask, scores, NEG) - lse[..., None]), 0.0)
        dvalue_acc = dvalue_acc + jnp.einsum(
            "hqk,qhd->khd", probs.astype(jnp.bfloat16), dattn, preferred_element_type=jnp.float32
        ).reshape(tokens, width)
        dprob = jnp.einsum(
            "qhd,khd->hqk",
            dattn,
            value_cur.reshape(tokens, heads, head_dim),
            preferred_element_type=jnp.float32,
        )
        dscore = (probs * (dprob - delta[..., None]) * scale).astype(jnp.bfloat16)
        dquery_acc = dquery_acc + jnp.einsum(
            "hqk,khd->qhd", dscore, key_heads, preferred_element_type=jnp.float32
        )
        dkey_acc = dkey_acc + jnp.einsum(
            "hqk,qhd->khd", dscore, query, preferred_element_type=jnp.float32
        ).reshape(tokens, width)
        key_cur, value_cur = shifted((key_cur, value_cur), "ctx", 1)
        dkey_acc, dvalue_acc = (
            shifted(dkey_acc.astype(jnp.bfloat16), "ctx", 1).astype(dkey_acc.dtype),
            shifted(dvalue_acc.astype(jnp.bfloat16), "ctx", 1).astype(dvalue_acc.dtype),
        )
        return (key_cur, value_cur, dkey_acc, dvalue_acc, dquery_acc)

    flat_zero = jnp.zeros((tokens, width), jnp.float32)
    cycle_init = (
        keys_flat,
        values,
        flat_zero,
        flat_zero,
        jnp.zeros((tokens, heads, head_dim), jnp.float32),
    )
    cycle_out = lax.fori_loop(0, cycle_size, cycle_step, cycle_init)
    dkey_sum, dvalue_sum, dquery_sum = (cycle_out[2], cycle_out[3], cycle_out[4])
    dquery = rotate(dquery_sum, cosine, sine, -1.0).reshape(tokens, width)
    dkey = rotate(dkey_sum.reshape(tokens, heads, head_dim), cosine, sine, -1.0).reshape(
        tokens, width
    )
    dproj = jnp.concatenate([dquery, dkey, dvalue_sum], axis=1)
    qkv_bias_grad = jnp.sum(dproj, axis=0)
    dproj_b = dproj.astype(jnp.bfloat16)
    normed_input_grad = contract_cols(dproj_b, w_qkv) + contract_cols(dup_b, w_up)
    gain_gradient = jnp.sum(normed_input_grad * standardized_input, axis=0)
    lnb_grad = jnp.sum(normed_input_grad, axis=0)
    scaled_rows = normed_input_grad * gain_float
    dx_rows = gradient_float + inverse_deviation * (
        scaled_rows
        - jnp.mean(scaled_rows, axis=-1, keepdims=True)
        - standardized_input * jnp.mean(scaled_rows * standardized_input, axis=-1, keepdims=True)
    )
    group_normed, group_dproj, group_dup = (
        lax.all_gather(normed_rows, "fsdp", axis=0, tiled=True),
        lax.all_gather(dproj_b, "fsdp", axis=0, tiled=True),
        lax.all_gather(dup_b, "fsdp", axis=0, tiled=True),
    )
    own_normed = own_columns(group_normed, cycle_size, shard_count, member)
    g_qkv_w, g_fc1_w = (
        lax.psum_scatter(
            contract_rows(own_normed, group_dproj).astype(jnp.bfloat16),
            "ctx",
            scatter_dimension=0,
            tiled=True,
        ).astype(jnp.float32),
        lax.psum_scatter(
            contract_rows(own_normed, group_dup).astype(jnp.bfloat16),
            "ctx",
            scatter_dimension=0,
            tiled=True,
        ).astype(jnp.float32),
    )
    layer_gain_grad, g_lnb, g_qkv_b, g_fc1_b = (
        lax.psum_scatter(gain_gradient, ("ctx", "fsdp"), scatter_dimension=0, tiled=True),
        lax.psum_scatter(lnb_grad, ("ctx", "fsdp"), scatter_dimension=0, tiled=True),
        lax.psum_scatter(qkv_bias_grad, ("ctx", "fsdp"), scatter_dimension=0, tiled=True),
        lax.psum_scatter(up_bias_grad, ("ctx", "fsdp"), scatter_dimension=0, tiled=True),
    )
    return (
        y_rows.astype(jnp.bfloat16)[None],
        dx_rows[None],
        layer_gain_grad,
        g_lnb,
        g_qkv_w,
        g_qkv_b,
        g_dense_w,
        g_dense_b,
        g_fc1_w,
        g_fc1_b,
        g_fc2_w,
        g_fc2_b,
    )


BF = jnp.bfloat16
F32 = jnp.float32
MESH = pl.DeviceIdType.MESH
HBM = pl.BlockSpec(memory_space=pl.ANY)
VM = pl.BlockSpec(memory_space=pltpu.VMEM)
DMA = pltpu.SemaphoreType.DMA
VLIM = 60 * 1024 * 1024


def place():
    ctx, z = lax.axis_index("ctx"), lax.axis_index("fsdp")
    return ctx, lax.div(ctx, 4), lax.rem(lax.div(ctx, 2), 2), lax.rem(ctx, 2), z


class Net:
    def __init__(self):
        self.ctx, self.y, self.x, self.c, self.z = place()
        self.yb, self.xb, self.cb = 1 - self.y, 1 - self.x, 1 - self.c
        self.m = self.y * 4 + self.z
        self.g = self.x * 2 + self.c
        self.to_y = {"ctx": self.ctx + 4 * (1 - 2 * self.y), "fsdp": self.z}
        self.to_x = {"ctx": self.ctx + 2 * (1 - 2 * self.x), "fsdp": self.z}
        self.to_c = {"ctx": self.ctx + 1 - 2 * self.c, "fsdp": self.z}
        self.up = {"ctx": self.ctx, "fsdp": self.z + 1}
        self.dn = {"ctx": self.ctx, "fsdp": self.z - 1}
        self.sent = []

    def member(self, q):
        flip, step = q // 4, q % 4
        z = lax.rem(self.z + step, 4)
        yy = self.yb if flip else self.y
        return {"ctx": self.ctx + flip * 4 * (1 - 2 * self.y), "fsdp": z}, yy, z

    def source(self, q):
        flip, step = q // 4, q % 4
        return (self.yb if flip else self.y), lax.rem(self.z + 4 - step, 4)

    def barrier(self, more=()):
        sem = pltpu.get_barrier_semaphore()
        peers = [self.member(q)[0] for q in range(1, 8)] + [self.to_x, self.to_c, *more]
        for peer in peers:
            pl.semaphore_signal(sem, inc=1, device_id=peer, device_id_type=MESH)
        pl.semaphore_wait(sem, len(peers))

    def go(self, copy, when=None):
        if when is None:
            copy.start()
        else:
            pl.when(when)(copy.start)
        self.sent.append((copy, when))

    def drain(self):
        for copy, when in self.sent:
            if when is None:
                copy.wait_send()
            else:
                pl.when(when)(copy.wait_send)


def remote(src, dst, send, recv, to):
    return pltpu.make_async_remote_copy(
        src_ref=src, dst_ref=dst, send_sem=send, recv_sem=recv, device_id=to, device_id_type=MESH
    )


def arrive(like, recv):
    pltpu.make_async_copy(like, like, recv).wait()


def head_tiles(src, dst, rows):
    qkv, ff = src
    low = lanes_of((rows, 128)) < 64

    def tile(base, h):
        t = 128 * (h // 2)
        return qkv[:, base + t : base + t + 128].astype(F32)

    def join(a, b, odd):
        if odd:
            return jnp.where(low, pltpu.roll(a, 64, 1), b).astype(BF)
        return jnp.where(low, a, pltpu.roll(b, 64, 1)).astype(BF)

    for mm in range(8):
        first = (mm // 4) * 16 + mm % 4
        odd = first % 2
        for g in range(4):
            h = first + 4 * g
            dst(mm, 128 * g, join(tile(0, h), tile(2048, h), odd))
            dst(mm, 768 + 256 * g, ff[:, 256 * h : 256 * h + 256])
        for k in range(2):
            h = first + 8 * k
            dst(mm, 512 + 128 * k, join(tile(4096, h), tile(4096, h + 4), odd))


def gather_kernel(x, dy, docs, qkv, ff, qb, fb, small, fc2, dense, cos, sin,
                  xg, dg, docg, normed_o, act_o, dup_o, wc_o, w2_o, heads, dsum, cst,
                  xv, dv, wc, w2g, eg, ws, es, nrm, act, dup, hs,
                  loc, us, ur, ds_, dr, ys, yr, as_, ar, es_, er,
                  wxs, wxr, wks, wkr, exs, exr, eks, ekr, fxs, fxr, fks, fkr, hss, hsr, hl, wb):
    n = Net()
    far = {"ctx": n.ctx + 2 * (1 - 2 * n.x) + 1 - 2 * n.c, "fsdp": n.z}
    n.barrier(more=(far,))

    def wrow(yy, xx, cc, zz):
        return wc.at[pl.ds(pl.multiple_of((yy * 16 + xx * 8 + cc * 4 + zz) * 64, 64), 64)]

    def wide(gg):
        return w2g.at[pl.ds(pl.multiple_of(gg * 256, 256), 256)]

    def thin(gg):
        return w2g.at[pl.ds(pl.multiple_of(1024 + gg * 64, 64), 64)]

    def shard(yy, zz, p):
        mm = yy * 4 + zz
        if p == 2:
            return docg.at[mm]
        return (xv, dv)[p].at[pl.ds(pl.multiple_of(mm * 128, 128), 128)]

    mine = (x, dy, docs)
    parts = (0, 1, 2)

    def tokens(p):
        n.go(remote(mine[p], shard(n.y, n.z, p), us.at[p, 0], ur.at[p, 0], n.up), n.z < 3)
        n.go(remote(mine[p], shard(n.y, n.z, p), ds_.at[p, 0], dr.at[p, 0], n.dn), n.z > 0)
        n.go(remote(mine[p], shard(n.y, n.z, p), ys.at[p, 0], yr.at[p, n.z], n.to_y))

    tokens(0)
    rows2 = ((fc2, wide), (dense, thin))
    for k, (ref, part) in enumerate(rows2):
        n.go(remote(ref, part(n.g), fxs.at[k], fxr.at[k], n.to_x))
        n.go(remote(ref, part(n.g), fks.at[k], fkr.at[k], n.to_c))

    def put_w(mm, col, value):
        ws[mm, :, col : col + value.shape[1]] = value

    def put_e(mm, col, value):
        es[mm, 0:1, col : col + value.shape[1]] = value[0:1]

    for mm in range(8):
        es[mm] = small[...]
    head_tiles((qkv, ff), put_w, 64)
    head_tiles((qb, fb), put_e, 8)
    for q in (4, 1, 3, 5, 7, 2, 6):
        to, yy, zz = n.member(q)
        n.go(remote(es.at[yy * 4 + zz], eg.at[n.g * 8 + n.m], es_.at[q], er.at[q], to))
        n.go(remote(ws.at[yy * 4 + zz], wrow(n.y, n.x, n.c, n.z), as_.at[q], ar.at[q], to))
    own = ws.at[n.m]
    n.go(remote(own, wrow(n.y, n.x, n.c, n.z), wxs.at[0], wxr.at[0], n.to_x))
    n.go(remote(own, wrow(n.y, n.x, n.c, n.z), wks.at[0], wkr.at[0], n.to_c))
    tokens(1)
    tokens(2)
    local = [
        pltpu.make_async_copy(x, shard(n.y, n.z, 0), loc.at[0]),
        pltpu.make_async_copy(dy, shard(n.y, n.z, 1), loc.at[1]),
        pltpu.make_async_copy(docs, shard(n.y, n.z, 2), loc.at[2]),
        pltpu.make_async_copy(own, wrow(n.y, n.x, n.c, n.z), loc.at[3]),
        pltpu.make_async_copy(es.at[n.m], eg.at[n.g * 8 + n.m], loc.at[4]),
        pltpu.make_async_copy(fc2, wide(n.g), loc.at[5]),
        pltpu.make_async_copy(dense, thin(n.g), loc.at[6]),
    ]
    for copy in local:
        copy.start()

    def line(d, ps):
        below, above = n.z >= d, n.z + d <= 3
        for p in ps:
            for there, zz, recv, send, nxt, more, to in (
                (below, n.z - d, ur, us, ur, n.z < 3, n.up),
                (above, n.z + d, dr, ds_, dr, n.z > 0, n.dn),
            ):
                block = shard(n.y, zz, p)

                @pl.when(there)
                def _():
                    arrive(block, recv.at[p, d - 1])

                if d < 3:
                    n.go(remote(block, block, send.at[p, d], nxt.at[p, d], to), there & more)
                slot = d if to is n.up else d + 3
                n.go(remote(block, block, ys.at[p, slot], yr.at[p, zz], n.to_y), there)

    def pieces(qs):
        for q in qs:
            yy, zz = n.source(q)
            block = wrow(yy, n.x, n.c, zz)
            arrive(block, ar.at[q])
            n.go(remote(block, block, wxs.at[q], wxr.at[q], n.to_x))
            n.go(remote(block, block, wks.at[q], wkr.at[q], n.to_c))

    def relay(qs):
        for q in qs:
            yy, zz = n.source(q)
            block = wrow(yy, n.xb, n.c, zz)
            arrive(block, wxr.at[q])
            n.go(remote(block, block, wks.at[8 + q], wkr.at[8 + q], n.to_c))

    line(1, (0,))
    pieces((4, 1, 3))
    line(1, (1, 2))
    pieces((5, 7, 2, 6))
    for q in range(1, 8):
        yy, zz = n.source(q)
        arrive(eg.at[n.g * 8 + yy * 4 + zz], er.at[q])
    local[4].wait()
    these = eg.at[pl.ds(n.g * 8, 8)]
    n.go(remote(these, these, exs.at[0], exr.at[0], n.to_x))
    n.go(remote(these, these, eks.at[0], ekr.at[0], n.to_c))
    line(2, parts)
    gx = n.xb * 2 + n.c
    for k, (ref, part) in enumerate(rows2):
        arrive(part(gx), fxr.at[k])
        n.go(remote(part(gx), part(gx), fks.at[2 + k], fkr.at[2 + k], n.to_c))
    theirs = eg.at[pl.ds(gx * 8, 8)]
    relay((0, 4, 1, 3, 5, 7, 2, 6))
    arrive(theirs, exr.at[0])
    n.go(remote(theirs, theirs, eks.at[1], ekr.at[1], n.to_c))
    line(3, parts)
    for q in range(8):
        yy, zz = n.source(q)
        arrive(wrow(yy, n.x, n.cb, zz), wkr.at[q])
        arrive(wrow(yy, n.xb, n.cb, zz), wkr.at[8 + q])
    for k in range(2):
        gg = 2 * (n.xb if k else n.x) + n.cb
        arrive(eg.at[pl.ds(gg * 8, 8)], ekr.at[k])
        for j, (ref, part) in enumerate(rows2):
            arrive(part(gg), fkr.at[2 * k + j])
    for k in (0, 1, 2, 3, 5, 6):
        local[k].wait()
    out_w = [pltpu.make_async_copy(wc, wc_o, wb.at[0]), pltpu.make_async_copy(w2g, w2_o, wb.at[1])]
    for copy in out_w:
        copy.start()

    def add_ext(i, t):
        return t + eg[i].astype(F32)

    ext = lax.fori_loop(0, 32, add_ext, jnp.zeros((8, 1792), F32))
    cst[0:1, 0:1792], cst[0:1, 1792:2048] = ext[1:2], ext[5:6, 0:256]
    cst[1:2, 0:1792], cst[1:2, 1792:2048] = ext[2:3], ext[5:6, 256:512]
    cst[2:3, 0:1792], cst[2:3, 1792:2048] = ext[3:4] + ext[4:5], ext[5:6, 512:768] + ext[5:6, 768:1024]
    cst[3:4, 0:1792], cst[3:4, 1792:2048] = ext[0:1], jnp.zeros((1, 256), F32)
    cst[4:8, :] = jnp.zeros((4, 2048), F32)
    dsum[...] = jnp.zeros_like(dsum)
    z0 = lax.div(n.z, 2)
    half = lanes_of((256, 128)) < 64

    def rows_of(j):
        yy = n.y + lax.div(j, 2) * (1 - 2 * n.y)
        zp = z0 + lax.rem(j, 2) * (1 - 2 * z0)
        return yy, zp, pl.ds(pl.multiple_of((yy * 4 + 2 * zp) * 128, 256), 256)

    def sends(j):
        yy, zp, rows = rows_of(j)
        return [
            remote(hs.at[gg, rows], heads.at[n.g, rows], hss.at[j, k], hsr.at[j, k], to)
            for k, (to, gg) in enumerate(((far, 2 * n.xb + n.cb), (n.to_x, 2 * n.xb + n.c), (n.to_c, 2 * n.x + n.cb)))
        ]

    def keeps(j):
        yy, zp, rows = rows_of(j)
        return [
            pltpu.make_async_copy(hs.at[n.g, rows], heads.at[n.g, rows], hl.at[j, 0]),
            pltpu.make_async_copy(nrm.at[rows], normed_o.at[rows], hl.at[j, 1]),
            pltpu.make_async_copy(act.at[rows], act_o.at[rows], hl.at[j, 2]),
            pltpu.make_async_copy(dup.at[rows], dup_o.at[rows], hl.at[j, 3]),
            pltpu.make_async_copy(xv.at[rows], xg.at[rows], hl.at[j, 4]),
            pltpu.make_async_copy(dv.at[rows], dg.at[rows], hl.at[j, 5]),
        ]

    def pair(j, carry):
        yy, zp, rows = rows_of(j)
        base = (yy * 4 + 2 * zp) * 128

        @pl.when(j >= 2)
        def _():
            for k in range(2):
                for p in parts:
                    arrive(shard(yy, 2 * zp + k, p), yr.at[p, 2 * zp + k])

        def norm(i, c):
            sl = pl.ds(pl.multiple_of(base + 32 * i, 32), 32)
            xf = xv[sl, :].astype(F32)
            cen = xf - jnp.mean(xf, axis=-1, keepdims=True)
            rstd = lax.rsqrt(jnp.mean(cen * cen, axis=-1, keepdims=True) + EPS)
            nrm[sl, :] = (cen * rstd * cst[0:1, :] + cst[1:2, :]).astype(BF)
            return c

        lax.fori_loop(0, 8, norm, 0)
        table = pl.ds(pl.multiple_of(yy * 128, 128), 128)
        cosv = jnp.concatenate([cos[table, :]] * 2, axis=0)
        sinv = jnp.concatenate([sin[table, :]] * 2, axis=0)
        for k in range(2):
            t2 = jnp.dot(nrm[rows, :], wc[:, 256 * k : 256 * k + 256], preferred_element_type=F32)
            t2 = t2 + cst[3:4, 256 * k : 256 * k + 256]
            for i in range(2):
                t = t2[:, 128 * i : 128 * i + 128]
                hs[2 * k + i, rows, 0:128] = (t * cosv + partner(t) * sinv).astype(BF)
        v4 = jnp.dot(nrm[rows, :], wc[:, 512:768], preferred_element_type=F32) + cst[3:4, 512:768]
        d4 = dot_nt(dv[rows, :], w2g[1024:1280, :])
        for g in range(4):
            v, d = (t[:, 128 * (g // 2) : 128 * (g // 2) + 128] for t in (v4, d4))
            if g % 2 == 0:
                vd = jnp.where(half, v, pltpu.roll(d, 64, 1))
            else:
                vd = jnp.where(half, pltpu.roll(v, 64, 1), d)
            hs[g, rows, 128:256] = vd.astype(BF)
        for copy in sends(j):
            copy.start()
        for k in range(4):
            cols, wcols = slice(256 * k, 256 * k + 256), slice(768 + 256 * k, 1024 + 256 * k)
            up = jnp.dot(nrm[rows, :], wc[:, wcols], preferred_element_type=F32) + cst[3:4, wcols]
            a, slope = gelu_pair(up)
            act[rows, cols] = a.astype(BF)
            du = dot_nt(dv[rows, :], w2g[cols, :]) * slope
            dup[rows, cols] = du.astype(BF)
            dsum[:, cols] += jnp.broadcast_to(jnp.sum(du, axis=0, keepdims=True), (8, 256))
        for copy in keeps(j):
            copy.start()
        return carry

    lax.fori_loop(0, 4, pair, 0)
    for j in range(4):
        for copy in sends(j):
            copy.wait()
        for copy in keeps(j):
            copy.wait()
    for copy in out_w:
        copy.wait()
    n.drain()


def gather_all(x, dy, docs, qkv, ff, qb, fb, small, fc2, dense, cos, sin):
    sd = jax.ShapeDtypeStruct
    V = pltpu.VMEM
    return pl.pallas_call(
        gather_kernel,
        name="gather_all",
        out_shape=(sd((1024, 2048), BF), sd((1024, 2048), BF), sd((8, 8, 1024), BF), sd((1024, 2048), BF),
                   sd((1024, 1024), BF), sd((1024, 1024), BF), sd((2048, 1792), BF), sd((1280, 2048), BF),
                   sd((4, 1024, 256), BF), sd((8, 1024), F32), sd((8, 2048), F32)),
        in_specs=[VM] * 12,
        out_specs=(HBM, HBM, VM, HBM, HBM, HBM, HBM, HBM, HBM, VM, VM),
        scratch_shapes=[V((1024, 2048), BF), V((1024, 2048), BF), V((2048, 1792), BF), V((1280, 2048), BF),
                        V((32, 8, 1792), BF), V((8, 64, 1792), BF), V((8, 8, 1792), BF),
                        V((1024, 2048), BF), V((1024, 1024), BF), V((1024, 1024), BF), V((4, 1024, 256), BF),
                        DMA((7,)), DMA((3, 3)), DMA((3, 3)), DMA((3, 3)), DMA((3, 3)), DMA((3, 7)), DMA((3, 4)),
                        DMA((8,)), DMA((8,)), DMA((8,)), DMA((8,)), DMA((8,)), DMA((8,)), DMA((16,)), DMA((16,)),
                        DMA((1,)), DMA((1,)), DMA((2,)), DMA((2,)), DMA((2,)), DMA((2,)), DMA((4,)), DMA((4,)),
                        DMA((4, 3)), DMA((4, 3)), DMA((4, 6)), DMA((2,))],
        compiler_params=pltpu.CompilerParams(collective_id=1, has_side_effects=True, vmem_limit_bytes=VLIM),
    )(x, dy, docs, qkv, ff, qb, fb, small, fc2, dense, cos, sin)


def exchange_kernel(src, dst, loc, ss, rs):
    n = Net()
    n_peer = {"ctx": n.ctx + 2 * (1 - 2 * n.x) + 1 - 2 * n.c, "fsdp": n.z}
    sem = pltpu.get_barrier_semaphore()
    for peer in (n.to_x, n.to_c, n_peer):
        pl.semaphore_signal(sem, inc=1, device_id=peer, device_id_type=MESH)
    pl.semaphore_wait(sem, 3)
    copies = []
    for k, (to, gg) in enumerate(((n_peer, 2 * n.xb + n.cb), (n.to_x, 2 * n.xb + n.c), (n.to_c, 2 * n.x + n.cb))):
        copies.append(remote(src.at[gg], dst.at[n.g], ss.at[k], rs.at[k], to))
    for copy in copies:
        copy.start()
    own = pltpu.make_async_copy(src.at[n.g], dst.at[n.g], loc)
    own.start()
    own.wait()
    for copy in copies:
        copy.wait()


def exchange(a, cid):
    return pl.pallas_call(
        exchange_kernel,
        name="exchange",
        out_shape=jax.ShapeDtypeStruct(a.shape, a.dtype),
        in_specs=[VM],
        out_specs=VM,
        scratch_shapes=[DMA, DMA((3,)), DMA((3,))],
        compiler_params=pltpu.CompilerParams(collective_id=cid, has_side_effects=True, vmem_limit_bytes=VLIM),
    )(a)


def lanes_of(shape):
    return lax.broadcasted_iota(jnp.int32, shape, len(shape) - 1)


def partner(t):
    low = lax.rem(lanes_of(t.shape), 64) < 16
    return jnp.where(low, pltpu.roll(t, 112, 1), pltpu.roll(t, 16, 1))


def dot_nt(a, b):
    return lax.dot_general(a, b, (((1,), (1,)), ((), ())), preferred_element_type=F32)


def dot_tn(a, b):
    return lax.dot_general(a, b, (((0,), (0,)), ((), ())), preferred_element_type=F32)


def attention_kernel(slot_of, a, docs, cos, sin, out, sums, seq, att, dq, dk, dv):
    def where_is(p):
        r = slot_of[p]
        ctx = lax.div(r, 2)
        return lax.rem(ctx, 4), lax.div(ctx, 4), pl.ds(pl.multiple_of(lax.rem(r, 2) * 64, 64), 64)

    for p in range(16):
        g, yy, rows = where_is(p)
        seq[64 * p : 64 * p + 64, :] = a[g, yy, 0, rows, :]
    dk[...] = jnp.zeros_like(dk)
    dv[...] = jnp.zeros_like(dv)
    scale = 0.125
    low = lanes_of((256, 128)) < 64
    for i in range(4):
        k0 = max(0, i - 2) * 256
        kn = 256 * (i + 1) - k0
        rq, rk = slice(256 * i, 256 * i + 256), slice(k0, k0 + kn)
        qk, vd = seq[rq, 0:128], seq[rq, 128:256]
        kk, vv = seq[rk, 0:128], seq[rk, 128:256]
        zero = jnp.zeros((256, 128), F32)
        qs = jnp.where(low, zero, pltpu.roll(qk.astype(F32), 64, 1)).astype(BF)
        dsf = jnp.where(low, pltpu.roll(vd.astype(F32), 64, 1), zero)
        s = dot_nt(qs, kk) * scale
        qpos = 256 * i + lax.broadcasted_iota(jnp.int32, (256, kn), 0)
        kpos = k0 + lax.broadcasted_iota(jnp.int32, (256, kn), 1)
        own = jnp.broadcast_to(docs[0, 0:1, rq].astype(F32), (128, 256)).T[:, 0:1]
        mask = (kpos <= qpos) & (docs[0, 0:1, rk].astype(F32) == own)
        s = jnp.where(mask, s, NEG)
        top = jnp.max(s, axis=-1, keepdims=True)
        e = jnp.where(mask, jnp.exp(s - top), 0.0)
        inv = 1.0 / jnp.sum(e, axis=-1, keepdims=True)
        o = jnp.dot(e.astype(BF), vv, preferred_element_type=F32) * inv
        ob = o.astype(BF)
        att[rq, :] = ob.astype(F32)
        delta = jnp.sum(dsf * ob.astype(F32), axis=-1, keepdims=True)
        pr = e * inv
        dv[rk, :] += dot_tn(pr.astype(BF), vd)
        dp = dot_nt(dsf.astype(BF), vv)
        ds = (pr * (dp - delta) * scale).astype(BF)
        dq[rq, :] = jnp.dot(ds, kk, preferred_element_type=F32)
        dk[rk, :] += dot_tn(ds, qk)
    tot = jnp.zeros((8, 256), F32)
    half = lanes_of((64, 128)) < 64
    s1 = jnp.zeros((1, 128), F32)
    s2 = jnp.zeros((1, 128), F32)
    for p in range(16):
        rows = slice(64 * p, 64 * p + 64)
        g, yy, place_rows = where_is(p)
        t = jnp.where(half, pltpu.roll(dq[rows, :], 64, 1), pltpu.roll(dk[rows, :], 64, 1))
        t = t * cos[rows, :] - partner(t) * sin[rows, :]
        u = jnp.where(half, pltpu.roll(dv[rows, :], 64, 1), pltpu.roll(att[rows, :], 64, 1))
        s1 += jnp.sum(t, axis=0, keepdims=True)
        s2 += jnp.sum(u, axis=0, keepdims=True)
        out[g, yy, 0, place_rows, 0:128] = t.astype(BF)
        out[g, yy, 0, place_rows, 128:256] = u.astype(BF)
    sums[0, :, 0:128] = jnp.broadcast_to(s1, (8, 128))
    sums[0, :, 128:256] = jnp.broadcast_to(s2, (8, 128))


def attention(slot_of, a, docs, cos, sin):
    sd = jax.ShapeDtypeStruct
    blk = pl.BlockSpec((4, 2, 1, 128, 256), lambda s, t: (0, 0, s, 0, 0))
    return pl.pallas_call(
        attention_kernel,
        name="attention",
        grid_spec=pltpu.PrefetchScalarGridSpec(
            num_scalar_prefetch=1,
            grid=(4,),
            in_specs=[
                blk,
                pl.BlockSpec((1, 8, 1024), lambda s, t: (s, 0, 0)),
                pl.BlockSpec((1024, 128), lambda s, t: (0, 0)),
                pl.BlockSpec((1024, 128), lambda s, t: (0, 0)),
            ],
            out_specs=(blk, pl.BlockSpec((1, 8, 256), lambda s, t: (s, 0, 0))),
            scratch_shapes=[pltpu.VMEM((1024, 256), BF)] + [pltpu.VMEM((1024, 128), F32)] * 4,
        ),
        out_shape=(sd((4, 2, 4, 128, 256), BF), sd((4, 8, 256), F32)),
        compiler_params=pltpu.CompilerParams(vmem_limit_bytes=VLIM),
    )(slot_of, a, docs, cos, sin)


def add_rows(dst, srcs, rows, out=None, step=16):
    out = dst if out is None else out

    def body(i, carry):
        sl = pl.ds(pl.multiple_of(i * step, step), step)
        v = dst[sl, :].astype(F32)
        for s in srcs:
            v = v + s[sl, :].astype(F32)
        out[sl, :] = v.astype(out.dtype)
        return carry

    lax.fori_loop(0, rows // step, body, 0)


def reduce_kernel(part, dw1, dw2, e1, yo, o1, o2, eo, own, yr, ub, db, w1, r1, r2, w2, s1, s2, ev, t1, t2,
                  ol, wl, vl, yss, yrs, uss, urs, dss, drs, k1s, k1r, x1s, x1r, a1s, a1r,
                  k2s, k2r, x2s, x2r, eks, ekr, exs, exr, eas, ear, fl):
    n = Net()
    n.barrier()
    order = (3, 0, 2, 1)

    def block(yy, xx, cc):
        return dw1.at[pl.ds(pl.multiple_of((yy * 16 + xx * 8 + cc * 4) * 64, 256), 256)]

    def wide(gg):
        return dw2.at[pl.ds(pl.multiple_of(gg * 256, 256), 256)]

    def thin(gg):
        return dw2.at[pl.ds(pl.multiple_of(1024 + gg * 64, 64), 64)]

    load_own = {}
    for t in range(2):
        for k in order:
            n.go(remote(part.at[n.yb * 4 + k, t], yr.at[k, t], yss.at[t, k], yrs.at[t, k], n.to_y))
    for xx in range(2):
        gg = 2 * xx + n.cb
        n.go(remote(e1.at[pl.ds(gg * 8, 8)], t1.at[xx], eks.at[xx], ekr.at[xx], n.to_c))
        n.go(remote(wide(gg), s1.at[xx, pl.ds(0, 256)], k2s.at[xx, 0], k2r.at[xx, 0], n.to_c))
        n.go(remote(thin(gg), s1.at[xx, pl.ds(256, 64)], k2s.at[xx, 1], k2r.at[xx, 1], n.to_c))
        for yy in range(2):
            n.go(remote(block(yy, xx, n.cb), r1.at[yy * 2 + xx], k1s.at[yy * 2 + xx], k1r.at[yy * 2 + xx], n.to_c))
    loads = []
    for xx in range(2):
        gg = 2 * xx + n.c
        loads.append(pltpu.make_async_copy(e1.at[pl.ds(gg * 8, 8)], ev.at[xx], vl.at[xx, 0]))
        loads.append(pltpu.make_async_copy(wide(gg), w2.at[xx, pl.ds(0, 256)], vl.at[xx, 1]))
        loads.append(pltpu.make_async_copy(thin(gg), w2.at[xx, pl.ds(256, 64)], vl.at[xx, 2]))
        for yy in range(2):
            loads.append(pltpu.make_async_copy(block(yy, xx, n.c), w1.at[yy * 2 + xx], wl.at[yy * 2 + xx]))
    for t in range(2):
        for k in order:
            load_own[t, k] = pltpu.make_async_copy(part.at[n.y * 4 + k, t], own.at[k, t], ol.at[t, k])
    for copy in loads + list(load_own.values()):
        copy.start()
    for copy in loads:
        copy.wait()

    for xx in range(2):
        arrive(t1.at[xx], ekr.at[xx])
        ev[xx] = ev[xx] + t1[xx]
        arrive(s1.at[xx, pl.ds(0, 256)], k2r.at[xx, 0])
        arrive(s1.at[xx, pl.ds(256, 64)], k2r.at[xx, 1])
        add_rows(w2.at[xx], [s1.at[xx]], 320)
        for yy in range(2):
            arrive(r1.at[yy * 2 + xx], k1r.at[yy * 2 + xx])
            add_rows(w1.at[yy * 2 + xx], [r1.at[yy * 2 + xx]], 256)
    n.go(remote(ev.at[n.xb], t2, exs.at[0], exr.at[0], n.to_x))
    for yy in range(2):
        n.go(remote(w1.at[yy * 2 + n.xb], r2.at[yy], x1s.at[yy], x1r.at[yy], n.to_x))
    n.go(remote(w2.at[n.xb], s2, x2s.at[0], x2r.at[0], n.to_x))

    def forward(t, k):
        def send_up():
            return remote(own.at[k, t], ub.at[k, t], uss.at[t, k], urs.at[t, k], n.up)

        def send_down():
            return remote(own.at[k, t], db.at[k, t], dss.at[t, k], drs.at[t, k], n.dn)

        @pl.when(n.z != k)
        def _():
            load_own[t, k].wait()
            arrive(yr.at[k, t], yrs.at[t, k])
        if k > 0:
            @pl.when(n.z == 0)
            def _():
                add_rows(own.at[k, t], [yr.at[k, t]], 128)

            if k > 1:
                @pl.when((n.z > 0) & (n.z < k))
                def _():
                    arrive(ub.at[k, t], urs.at[t, k])
                    add_rows(own.at[k, t], [yr.at[k, t], ub.at[k, t]], 128)

            n.go(send_up(), n.z < k)
        if k < 3:
            @pl.when(n.z == 3)
            def _():
                add_rows(own.at[k, t], [yr.at[k, t]], 128)

            if k < 2:
                @pl.when((n.z < 3) & (n.z > k))
                def _():
                    arrive(db.at[k, t], drs.at[t, k])
                    add_rows(own.at[k, t], [yr.at[k, t], db.at[k, t]], 128)

            n.go(send_down(), n.z > k)

    def finish(t, k):
        @pl.when(n.z == k)
        def _():
            load_own[t, k].wait()
            arrive(yr.at[k, t], yrs.at[t, k])
            more = [yr.at[k, t]]
            if k > 0:
                arrive(ub.at[k, t], urs.at[t, k])
                more.append(ub.at[k, t])
            if k < 3:
                arrive(db.at[k, t], drs.at[t, k])
                more.append(db.at[k, t])
            add_rows(own.at[k, t], more, 128, yo.at[t])

    for k in order:
        forward(0, k)
    arrive(t2, exr.at[0])
    ev[n.x] = ev[n.x] + t2[...]
    for q in range(1, 8):
        to, yy, zz = n.member(q)
        n.go(remote(ev.at[n.x, yy * 4 + zz], eo.at[n.m], eas.at[q], ear.at[q], to))
    eo[n.m] = ev[n.x, n.m]
    for yy in range(2):
        arrive(r2.at[yy], x1r.at[yy])
        add_rows(w1.at[yy * 2 + n.x], [r2.at[yy]], 256)
    for q in (4, 1, 3, 5, 7, 2, 6):
        to, yy, zz = n.member(q)
        n.go(remote(w1.at[yy * 2 + n.x, pl.ds(pl.multiple_of(zz * 64, 64), 64)], o1.at[n.m], a1s.at[q], a1r.at[q], to))
    mine = pltpu.make_async_copy(w1.at[n.y * 2 + n.x, pl.ds(pl.multiple_of(n.z * 64, 64), 64)], o1.at[n.m], fl.at[0])
    mine.start()
    for k in order:
        forward(1, k)
    arrive(s2, x2r.at[0])
    add_rows(w2.at[n.x], [s2], 320, o2)
    for t in range(2):
        for k in range(4):
            finish(t, k)
    for q in range(1, 8):
        yy, zz = n.source(q)
        arrive(eo.at[yy * 4 + zz], ear.at[q])
        arrive(o1.at[yy * 4 + zz], a1r.at[q])
    mine.wait()
    n.drain()


def reduce_all(part, dw1, dw2, e1):
    sd = jax.ShapeDtypeStruct
    V = pltpu.VMEM
    return pl.pallas_call(
        reduce_kernel,
        name="reduce_all",
        out_shape=(sd((2, 128, 2048), F32), sd((8, 64, 1792), BF), sd((320, 2048), F32), sd((8, 16, 128), F32)),
        in_specs=[HBM, HBM, HBM, VM],
        out_specs=(VM, VM, VM, VM),
        scratch_shapes=[
            V((4, 2, 128, 2048), BF), V((4, 2, 128, 2048), BF), V((4, 2, 128, 2048), BF), V((4, 2, 128, 2048), BF),
            V((4, 256, 1792), BF), V((4, 256, 1792), BF), V((2, 256, 1792), BF),
            V((2, 320, 2048), BF), V((2, 320, 2048), BF), V((320, 2048), BF),
            V((2, 8, 16, 128), F32), V((2, 8, 16, 128), F32), V((8, 16, 128), F32),
            DMA((2, 4)), DMA((4,)), DMA((2, 3)),
            DMA((2, 4)), DMA((2, 4)), DMA((2, 4)), DMA((2, 4)), DMA((2, 4)), DMA((2, 4)),
            DMA((4,)), DMA((4,)), DMA((2,)), DMA((2,)), DMA((8,)), DMA((8,)),
            DMA((2, 2)), DMA((2, 2)), DMA((1,)), DMA((1,)),
            DMA((2,)), DMA((2,)), DMA((1,)), DMA((1,)), DMA((8,)), DMA((8,)), DMA((1,)),
        ],
        compiler_params=pltpu.CompilerParams(collective_id=3, has_side_effects=True, vmem_limit_bytes=VLIM),
    )(part, dw1, dw2, e1)


def member_columns(qkv, ff):
    rows = qkv.shape[0]
    parts = qkv.reshape(rows, 3, 2, 4, 4, 64)
    qk = parts[:, :2].transpose(2, 4, 0, 3, 1, 5).reshape(8, rows, 512)
    v = parts[:, 2].transpose(1, 3, 0, 2, 4).reshape(8, rows, 256)
    f = ff.reshape(rows, 2, 4, 4, 256).transpose(1, 3, 0, 2, 4).reshape(8, rows, 1024)
    return jnp.concatenate([qk, v, f], axis=2)


def stored_columns(a):
    rows = a.shape[1]
    qk = a[:, :, :512].reshape(2, 4, rows, 4, 2, 64).transpose(2, 4, 0, 3, 1, 5).reshape(rows, 2, 2048)
    v = a[:, :, 512:768].reshape(2, 4, rows, 4, 64).transpose(2, 0, 3, 1, 4).reshape(rows, 1, 2048)
    f = a[:, :, 768:1792].reshape(2, 4, rows, 4, 256).transpose(2, 0, 3, 1, 4).reshape(rows, 8192)
    return jnp.concatenate([qk, v], axis=1).reshape(rows, 6144), f


def rotary_lanes(pos):
    lane = jnp.arange(128, dtype=jnp.int32) % 64
    freqs = jnp.exp(-(2.0 * (lane % (ROT // 2)).astype(F32) / ROT) * math.log(10000.0))
    angles = pos.astype(F32)[:, None] * freqs[None]
    turns = lane < ROT
    sign = jnp.where(turns, jnp.where(lane < ROT // 2, -1.0, 1.0), 0.0)
    return jnp.where(turns, jnp.cos(angles), 1.0), jnp.sin(angles) * sign


def fast_device(
    block_input, output_grad, segment, slots, ln_gain, ln_bias, qkv_w, qkv_b, dense_w, dense_b, fc1_w, fc1_b, fc2_w, fc2_b
):
    ctx, y, x, c, z = place()
    g, m = x * 2 + c, y * 4 + z
    index = ctx * 4 + z
    xb, dyb = block_input[0], output_grad[0]

    def spread(piece, total):
        count = piece.shape[0]
        own = jnp.arange(total, dtype=jnp.int32) // count == index
        return jnp.where(own, jnp.tile(piece, total // count), jnp.zeros((), BF))

    docs = jnp.broadcast_to(segment.astype(BF), (8, 1024))
    qb = jnp.broadcast_to(spread(qkv_b, 6144)[None], (8, 6144))
    fb = jnp.broadcast_to(spread(fc1_b, 8192)[None], (8, 8192))
    vecs = jnp.stack([spread(v, 2048) for v in (ln_gain, ln_bias, dense_b, fc2_b)])
    rest = jnp.pad(vecs[:, 1792:].reshape(1, 1024), ((0, 0), (0, 768)))
    small = jnp.concatenate([jnp.zeros((1, 1792), BF), vecs[:, :1792], rest, jnp.zeros((2, 1792), BF)], axis=0)
    pairs = lax.dynamic_slice_in_dim(slots.reshape(2, 4, 2), g, 1, 1).reshape(4)
    rows = (pairs[:, None] * 64 + jnp.arange(64, dtype=jnp.int32)[None]).reshape(256)
    cos2, sin2 = rotary_lanes(rows)
    cos, sin = rotary_lanes(jnp.arange(1024, dtype=jnp.int32))
    xg, dg, docg, normed, act, dup, wc, w2g, heads, dsum, cst = gather_all(
        xb, dyb, docs, qkv_w, fc1_w, qb, fb, small, fc2_w, dense_w, cos2, sin2
    )
    gain, ob = cst[0:1], cst[2:3]
    slot_of = jnp.sum(jnp.where(slots[None, :] == jnp.arange(16, dtype=jnp.int32)[:, None], jnp.arange(16, dtype=jnp.int32)[None, :], 0), axis=1)
    att, sums = attention(slot_of, heads.reshape(4, 2, 4, 128, 256), docg, cos, sin)
    back = exchange(att.reshape(4, 1024, 256), 4)

    dqk = back[:, :, 0:128].transpose(1, 0, 2).reshape(1024, 512)
    dvv = back[:, :, 128:192].transpose(1, 0, 2).reshape(1024, 256)
    attn = back[:, :, 192:256].transpose(1, 0, 2).reshape(1024, 256)
    dpr = jnp.concatenate([dqk, dvv, dup], axis=1)
    up2 = jnp.concatenate([act, attn], axis=1)
    dy_all = dg
    ypart = jnp.dot(up2, w2g, preferred_element_type=F32)
    dn = contract_cols(dpr, wc)
    xf = xg.astype(F32)
    cen = xf - jnp.mean(xf, axis=-1, keepdims=True)
    xhat = cen * lax.rsqrt(jnp.mean(cen * cen, axis=-1, keepdims=True) + EPS)
    gpart = jnp.sum(dn * xhat, axis=0)
    bpart = jnp.sum(dn, axis=0)
    dw1 = contract_rows(normed, dpr).astype(BF)
    dw2 = contract_rows(up2, dy_all).astype(BF)
    part = jnp.stack([ypart.astype(BF).reshape(8, 128, 2048), dn.astype(BF).reshape(8, 128, 2048)], axis=1)

    hs = jnp.sum(sums[:, 0, :], axis=0)
    colq = lax.dynamic_update_slice(jnp.zeros((512,), F32), hs[:128], (g * 128,))
    colv = lax.dynamic_update_slice(jnp.zeros((256,), F32), hs[128:192], (g * 64,))
    cols = jnp.concatenate([colq, colv, dsum[0]])

    def rows_of(v):
        return v.reshape(2, 4, 4, 64).transpose(1, 0, 2, 3).reshape(32, 64)

    dsum_y = jnp.sum(dy_all.astype(F32), axis=0)
    e1 = jnp.concatenate(
        [jnp.broadcast_to(cols, (32, 1792)), rows_of(gpart), rows_of(bpart), rows_of(dsum_y), jnp.zeros((32, 64), F32)], axis=1
    ).reshape(32, 16, 128)
    yo, o1, o2, eo = reduce_all(part, dw1, dw2, e1)

    xf = xb.astype(F32)
    cen = xf - jnp.mean(xf, axis=-1, keepdims=True)
    rstd = lax.rsqrt(jnp.mean(cen * cen, axis=-1, keepdims=True) + EPS)
    xhat = cen * rstd
    out = (xf + yo[0] + ob).astype(BF)
    gr = yo[1] * gain
    dx = dyb.astype(F32) + rstd * (
        gr - jnp.mean(gr, axis=-1, keepdims=True) - xhat * jnp.mean(gr * xhat, axis=-1, keepdims=True)
    )
    g_qkv_w, g_fc1_w = stored_columns(o1.astype(F32))
    eo = eo.reshape(8, 2048)
    sq, sf = stored_columns(eo[:, None, :1792])
    g_qkv_b = lax.dynamic_slice_in_dim(sq[0], index * 192, 192, 0)
    g_fc1_b = lax.dynamic_slice_in_dim(sf[0], index * 256, 256, 0)
    g_gain = jnp.sum(eo[:, 1792:1856], axis=0)
    g_lnb = jnp.sum(eo[:, 1856:1920], axis=0)
    g_db = eo[0, 1920:1984]
    return (out[None], dx[None], g_gain, g_lnb, g_qkv_w, g_qkv_b, o2[256:], g_db, g_fc1_w, g_fc1_b, o2[:256], g_db)


def solution(mesh):
    in_specs = (
        P("fsdp", "ctx", None),
        P("fsdp", "ctx", None),
        P("fsdp", None),
        P(),
        P(("ctx", "fsdp")),
        P(("ctx", "fsdp")),
        P(("ctx", "fsdp"), None),
        P(("ctx", "fsdp")),
        P(("ctx", "fsdp"), None),
        P(("ctx", "fsdp")),
        P(("ctx", "fsdp"), None),
        P(("ctx", "fsdp")),
        P(("ctx", "fsdp"), None),
        P(("ctx", "fsdp")),
    )
    out_specs = (
        P("fsdp", "ctx", None),
        P("fsdp", "ctx", None),
        P(("ctx", "fsdp")),
        P(("ctx", "fsdp")),
        P(("ctx", "fsdp"), None),
        P(("ctx", "fsdp")),
        P(("ctx", "fsdp"), None),
        P(("ctx", "fsdp")),
        P(("ctx", "fsdp"), None),
        P(("ctx", "fsdp")),
        P(("ctx", "fsdp"), None),
        P(("ctx", "fsdp")),
    )
    small = mesh.shape["ctx"] == 8 and mesh.shape["fsdp"] == 4
    return jax.shard_map(
        fast_device if small else per_device, mesh=mesh, in_specs=in_specs, out_specs=out_specs, check_vma=False
    )
```

```python
import math

import jax
import jax.numpy as jnp
from jax import lax
from jax.experimental import pallas as pl
from jax.experimental.pallas import tpu as pltpu
from jax.sharding import PartitionSpec as P

HEADS = 32
ROT = 32


EPS = 1e-05
GELU_C = math.sqrt(2.0 / math.pi)
NEG = -1e30


def shifted(block, axis, distance):
    devices = range(lax.axis_size(axis))
    route = [((i - distance) % len(devices), i) for i in devices]
    return lax.ppermute(block, axis, route)


def gelu_pair(upper):
    inner = GELU_C * (upper + 0.044715 * upper * upper * upper)
    tanh_val = jnp.tanh(inner)
    value = 0.5 * upper * (1.0 + tanh_val)
    slope = 0.5 * (1.0 + tanh_val) + 0.5 * upper * (1.0 - tanh_val * tanh_val) * GELU_C * (
        1.0 + 3.0 * 0.044715 * upper * upper
    )
    return (value, slope)


def rotary_tables(positions):
    half = ROT // 2
    freqs = jnp.exp(-(2.0 * jnp.arange(half, dtype=jnp.float32) / ROT) * math.log(10000.0))
    angles = positions.astype(jnp.float32)[:, None] * freqs[None, :]
    return (jnp.cos(angles)[:, None, :], jnp.sin(angles)[:, None, :])


def rotate(tensor, cosine, sine, sign):
    half = ROT // 2
    first = tensor[..., :half]
    second = tensor[..., half:ROT]
    new_first = first * cosine - sign * second * sine
    new_second = second * cosine + sign * first * sine
    return jnp.concatenate([new_first, new_second, tensor[..., ROT:]], axis=-1)


def contract_rows(left, right):
    return lax.dot_general(
        left, right, (((0,), (0,)), ((), ())), preferred_element_type=jnp.float32
    )


def contract_cols(left, right):
    return lax.dot_general(
        left, right, (((1,), (1,)), ((), ())), preferred_element_type=jnp.float32
    )


def own_columns(matrix, cycle_size, shard_count, member):
    count = matrix.shape[0]
    piece_width = matrix.shape[1] // (cycle_size * shard_count)
    parted = matrix.reshape(count, cycle_size, shard_count, piece_width)
    return lax.dynamic_slice_in_dim(parted, member, 1, 2).reshape(count, cycle_size * piece_width)


def per_device(
    block_input,
    output_grad,
    segment,
    slots,
    ln_gain,
    ln_bias,
    qkv_w,
    qkv_b,
    dense_w,
    dense_b,
    fc1_w,
    fc1_b,
    fc2_w,
    fc2_b,
):
    cycle_size = lax.axis_size("ctx")
    index = lax.axis_index("ctx")
    shard_count = lax.axis_size("fsdp")
    member = lax.axis_index("fsdp")
    tokens = block_input.shape[1]
    width = block_input.shape[2]
    stretch = tokens // 2
    heads = HEADS
    head_dim = width // heads
    scale = head_dim ** (-0.5)
    seg_row = segment[0]
    slot_ids = jnp.arange(2 * cycle_size, dtype=jnp.int32)

    def positions(start, count):
        rows = start + jnp.arange(count, dtype=jnp.int32)
        slot = rows // stretch
        owner = jnp.sum(jnp.where(slot[:, None] == slot_ids[None, :], slots[None, :], 0), axis=1)
        return owner * stretch + rows % stretch

    qpos = positions(index * tokens, tokens)
    qdoc = jnp.take(seg_row, qpos)
    cosine, sine = rotary_tables(qpos)
    gain_all, norm_bias_every, w_qkv, b_qkv, w_up, b_up = (
        lax.all_gather(ln_gain, ("ctx", "fsdp"), axis=0, tiled=True),
        lax.all_gather(ln_bias, ("ctx", "fsdp"), axis=0, tiled=True),
        lax.all_gather(qkv_w, ("ctx", "fsdp"), axis=0, tiled=True),
        lax.all_gather(qkv_b, ("ctx", "fsdp"), axis=0, tiled=True),
        lax.all_gather(fc1_w, ("ctx", "fsdp"), axis=0, tiled=True),
        lax.all_gather(fc1_b, ("ctx", "fsdp"), axis=0, tiled=True),
    )
    xf = block_input[0].astype(jnp.float32)
    row_mean = jnp.mean(xf, axis=-1, keepdims=True)
    centered_input = xf - row_mean
    inverse_deviation = lax.rsqrt(
        jnp.mean(centered_input * centered_input, axis=-1, keepdims=True) + EPS
    )
    standardized_input = centered_input * inverse_deviation
    gain_float = gain_all.astype(jnp.float32)
    normed_rows = (standardized_input * gain_float + norm_bias_every.astype(jnp.float32)).astype(
        jnp.bfloat16
    )
    proj = jnp.dot(normed_rows, w_qkv, preferred_element_type=jnp.float32) + b_qkv.astype(
        jnp.float32
    )
    query = rotate(proj[:, :width].reshape(tokens, heads, head_dim), cosine, sine, 1.0).astype(
        jnp.bfloat16
    )
    keys = rotate(
        proj[:, width : 2 * width].reshape(tokens, heads, head_dim), cosine, sine, 1.0
    ).astype(jnp.bfloat16)
    keys_flat = keys.reshape(tokens, width)
    values = proj[:, 2 * width :].astype(jnp.bfloat16)
    acc = jnp.zeros((tokens, heads, head_dim), jnp.float32)
    top = jnp.full((heads, tokens), NEG, jnp.float32)
    key_piece = lax.all_gather(keys_flat, "ctx", axis=0, tiled=True)
    value_piece = lax.all_gather(values, "ctx", axis=0, tiled=True)
    count = key_piece.shape[0]
    kpos = positions(jnp.int32(0), count)
    kdoc = jnp.take(seg_row, kpos)
    mask = ((kpos[None, :] <= qpos[:, None]) & (kdoc[None, :] == qdoc[:, None]))[None]
    scores = (
        jnp.einsum(
            "qhd,khd->hqk",
            query,
            key_piece.reshape(count, heads, head_dim),
            preferred_element_type=jnp.float32,
        )
        * scale
    )
    scores = jnp.where(mask, scores, NEG)
    new_top = jnp.maximum(top, jnp.max(scores, axis=-1))
    factor = jnp.exp(top - new_top)
    expo = jnp.where(mask, jnp.exp(scores - new_top[..., None]), 0.0)
    total = jnp.sum(expo, axis=-1)
    part_sum = jnp.einsum(
        "hqk,khd->qhd",
        expo.astype(jnp.bfloat16),
        value_piece.reshape(count, heads, head_dim),
        preferred_element_type=jnp.float32,
    )
    acc = acc * factor.T[:, :, None] + part_sum
    acc, top, total = (acc, new_top, total)
    attn_heads = (acc / total.T[:, :, None]).astype(jnp.bfloat16)
    lse = top + jnp.log(total)
    attn = attn_heads.reshape(tokens, width)
    w_dense, b_dense, w_down, b_down = (
        lax.all_gather(dense_w, ("ctx", "fsdp"), axis=0, tiled=True),
        lax.all_gather(dense_b, ("ctx", "fsdp"), axis=0, tiled=True),
        lax.all_gather(fc2_w, ("ctx", "fsdp"), axis=0, tiled=True),
        lax.all_gather(fc2_b, ("ctx", "fsdp"), axis=0, tiled=True),
    )
    upper = jnp.dot(normed_rows, w_up, preferred_element_type=jnp.float32) + b_up.astype(
        jnp.float32
    )
    act_f, slope = gelu_pair(upper)
    act = act_f.astype(jnp.bfloat16)
    y_rows = (
        xf
        + jnp.dot(attn, w_dense, preferred_element_type=jnp.float32)
        + b_dense.astype(jnp.float32)
    )
    y_rows = (
        y_rows
        + jnp.dot(act, w_down, preferred_element_type=jnp.float32)
        + b_down.astype(jnp.float32)
    )
    grad_rows = output_grad[0]
    gradient_float = grad_rows.astype(jnp.float32)
    group_attn, group_act, group_grad = (
        lax.all_gather(attn, "fsdp", axis=0, tiled=True),
        lax.all_gather(act, "fsdp", axis=0, tiled=True),
        lax.all_gather(grad_rows, "fsdp", axis=0, tiled=True),
    )
    group_bias = jnp.sum(group_grad.astype(jnp.float32), axis=0)
    own_bias = own_columns(group_bias[None], cycle_size, shard_count, member)[0]
    dense_part = contract_rows(own_columns(group_attn, cycle_size, shard_count, member), group_grad)
    down_part = contract_rows(own_columns(group_act, cycle_size, shard_count, member), group_grad)
    g_dense_w, g_dense_b, g_fc2_w, g_fc2_b = (
        lax.psum_scatter(
            dense_part.astype(jnp.bfloat16), "ctx", scatter_dimension=0, tiled=True
        ).astype(jnp.float32),
        lax.psum_scatter(
            own_bias.astype(jnp.bfloat16), "ctx", scatter_dimension=0, tiled=True
        ).astype(jnp.float32),
        lax.psum_scatter(
            down_part.astype(jnp.bfloat16), "ctx", scatter_dimension=0, tiled=True
        ).astype(jnp.float32),
        lax.psum_scatter(
            own_bias.astype(jnp.bfloat16), "ctx", scatter_dimension=0, tiled=True
        ).astype(jnp.float32),
    )
    dup = contract_cols(grad_rows, w_down) * slope
    up_bias_grad = jnp.sum(dup, axis=0)
    dup_b = dup.astype(jnp.bfloat16)
    dattn = contract_cols(grad_rows, w_dense).astype(jnp.bfloat16).reshape(tokens, heads, head_dim)
    delta = jnp.sum(dattn.astype(jnp.float32) * attn_heads.astype(jnp.float32), axis=-1).T

    def cycle_step(step, carry):
        key_cur, value_cur, dkey_acc, dvalue_acc, dquery_acc = carry
        anchor = (index - step + cycle_size) % cycle_size
        kpos = positions(anchor * tokens, tokens)
        kdoc = jnp.take(seg_row, kpos)
        mask = ((kpos[None, :] <= qpos[:, None]) & (kdoc[None, :] == qdoc[:, None]))[None]
        key_heads = key_cur.reshape(tokens, heads, head_dim)
        scores = (
            jnp.einsum("qhd,khd->hqk", query, key_heads, preferred_element_type=jnp.float32) * scale
        )
        probs = jnp.where(mask, jnp.exp(jnp.where(mask, scores, NEG) - lse[..., None]), 0.0)
        dvalue_acc = dvalue_acc + jnp.einsum(
            "hqk,qhd->khd", probs.astype(jnp.bfloat16), dattn, preferred_element_type=jnp.float32
        ).reshape(tokens, width)
        dprob = jnp.einsum(
            "qhd,khd->hqk",
            dattn,
            value_cur.reshape(tokens, heads, head_dim),
            preferred_element_type=jnp.float32,
        )
        dscore = (probs * (dprob - delta[..., None]) * scale).astype(jnp.bfloat16)
        dquery_acc = dquery_acc + jnp.einsum(
            "hqk,khd->qhd", dscore, key_heads, preferred_element_type=jnp.float32
        )
        dkey_acc = dkey_acc + jnp.einsum(
            "hqk,qhd->khd", dscore, query, preferred_element_type=jnp.float32
        ).reshape(tokens, width)
        key_cur, value_cur = shifted((key_cur, value_cur), "ctx", 1)
        dkey_acc, dvalue_acc = (
            shifted(dkey_acc.astype(jnp.bfloat16), "ctx", 1).astype(dkey_acc.dtype),
            shifted(dvalue_acc.astype(jnp.bfloat16), "ctx", 1).astype(dvalue_acc.dtype),
        )
        return (key_cur, value_cur, dkey_acc, dvalue_acc, dquery_acc)

    flat_zero = jnp.zeros((tokens, width), jnp.float32)
    cycle_init = (
        keys_flat,
        values,
        flat_zero,
        flat_zero,
        jnp.zeros((tokens, heads, head_dim), jnp.float32),
    )
    cycle_out = lax.fori_loop(0, cycle_size, cycle_step, cycle_init)
    dkey_sum, dvalue_sum, dquery_sum = (cycle_out[2], cycle_out[3], cycle_out[4])
    dquery = rotate(dquery_sum, cosine, sine, -1.0).reshape(tokens, width)
    dkey = rotate(dkey_sum.reshape(tokens, heads, head_dim), cosine, sine, -1.0).reshape(
        tokens, width
    )
    dproj = jnp.concatenate([dquery, dkey, dvalue_sum], axis=1)
    qkv_bias_grad = jnp.sum(dproj, axis=0)
    dproj_b = dproj.astype(jnp.bfloat16)
    normed_input_grad = contract_cols(dproj_b, w_qkv) + contract_cols(dup_b, w_up)
    gain_gradient = jnp.sum(normed_input_grad * standardized_input, axis=0)
    lnb_grad = jnp.sum(normed_input_grad, axis=0)
    scaled_rows = normed_input_grad * gain_float
    dx_rows = gradient_float + inverse_deviation * (
        scaled_rows
        - jnp.mean(scaled_rows, axis=-1, keepdims=True)
        - standardized_input * jnp.mean(scaled_rows * standardized_input, axis=-1, keepdims=True)
    )
    group_normed, group_dproj, group_dup = (
        lax.all_gather(normed_rows, "fsdp", axis=0, tiled=True),
        lax.all_gather(dproj_b, "fsdp", axis=0, tiled=True),
        lax.all_gather(dup_b, "fsdp", axis=0, tiled=True),
    )
    own_normed = own_columns(group_normed, cycle_size, shard_count, member)
    g_qkv_w, g_fc1_w = (
        lax.psum_scatter(
            contract_rows(own_normed, group_dproj).astype(jnp.bfloat16),
            "ctx",
            scatter_dimension=0,
            tiled=True,
        ).astype(jnp.float32),
        lax.psum_scatter(
            contract_rows(own_normed, group_dup).astype(jnp.bfloat16),
            "ctx",
            scatter_dimension=0,
            tiled=True,
        ).astype(jnp.float32),
    )
    layer_gain_grad, g_lnb, g_qkv_b, g_fc1_b = (
        lax.psum_scatter(gain_gradient, ("ctx", "fsdp"), scatter_dimension=0, tiled=True),
        lax.psum_scatter(lnb_grad, ("ctx", "fsdp"), scatter_dimension=0, tiled=True),
        lax.psum_scatter(qkv_bias_grad, ("ctx", "fsdp"), scatter_dimension=0, tiled=True),
        lax.psum_scatter(up_bias_grad, ("ctx", "fsdp"), scatter_dimension=0, tiled=True),
    )
    return (
        y_rows.astype(jnp.bfloat16)[None],
        dx_rows[None],
        layer_gain_grad,
        g_lnb,
        g_qkv_w,
        g_qkv_b,
        g_dense_w,
        g_dense_b,
        g_fc1_w,
        g_fc1_b,
        g_fc2_w,
        g_fc2_b,
    )


BF = jnp.bfloat16
F32 = jnp.float32
MESH = pl.DeviceIdType.MESH
HBM = pl.BlockSpec(memory_space=pl.ANY)
VM = pl.BlockSpec(memory_space=pltpu.VMEM)
DMA = pltpu.SemaphoreType.DMA
VLIM = 60 * 1024 * 1024


def place():
    ctx, z = lax.axis_index("ctx"), lax.axis_index("fsdp")
    return ctx, lax.div(ctx, 4), lax.rem(lax.div(ctx, 2), 2), lax.rem(ctx, 2), z


class Net:
    def __init__(self):
        self.ctx, self.y, self.x, self.c, self.z = place()
        self.yb, self.xb, self.cb = 1 - self.y, 1 - self.x, 1 - self.c
        self.m = self.y * 4 + self.z
        self.g = self.x * 2 + self.c
        self.to_y = {"ctx": self.ctx + 4 * (1 - 2 * self.y), "fsdp": self.z}
        self.to_x = {"ctx": self.ctx + 2 * (1 - 2 * self.x), "fsdp": self.z}
        self.to_c = {"ctx": self.ctx + 1 - 2 * self.c, "fsdp": self.z}
        self.up = {"ctx": self.ctx, "fsdp": self.z + 1}
        self.dn = {"ctx": self.ctx, "fsdp": self.z - 1}
        self.sent = []

    def member(self, q):
        flip, step = q // 4, q % 4
        z = lax.rem(self.z + step, 4)
        yy = self.yb if flip else self.y
        return {"ctx": self.ctx + flip * 4 * (1 - 2 * self.y), "fsdp": z}, yy, z

    def source(self, q):
        flip, step = q // 4, q % 4
        return (self.yb if flip else self.y), lax.rem(self.z + 4 - step, 4)

    def barrier(self, more=()):
        sem = pltpu.get_barrier_semaphore()
        peers = [self.member(q)[0] for q in range(1, 8)] + [self.to_x, self.to_c, *more]
        for peer in peers:
            pl.semaphore_signal(sem, inc=1, device_id=peer, device_id_type=MESH)
        pl.semaphore_wait(sem, len(peers))

    def go(self, copy, when=None):
        if when is None:
            copy.start()
        else:
            pl.when(when)(copy.start)
        self.sent.append((copy, when))

    def drain(self):
        for copy, when in self.sent:
            if when is None:
                copy.wait_send()
            else:
                pl.when(when)(copy.wait_send)


def remote(src, dst, send, recv, to):
    return pltpu.make_async_remote_copy(
        src_ref=src, dst_ref=dst, send_sem=send, recv_sem=recv, device_id=to, device_id_type=MESH
    )


def arrive(like, recv):
    pltpu.make_async_copy(like, like, recv).wait()


def head_tiles(src, dst, rows):
    qkv, ff = src
    low = lanes_of((rows, 128)) < 64

    def tile(base, h):
        t = 128 * (h // 2)
        return qkv[:, base + t : base + t + 128].astype(F32)

    def join(a, b, odd):
        if odd:
            return jnp.where(low, pltpu.roll(a, 64, 1), b).astype(BF)
        return jnp.where(low, a, pltpu.roll(b, 64, 1)).astype(BF)

    for mm in range(8):
        first = (mm // 4) * 16 + mm % 4
        odd = first % 2
        for g in range(4):
            h = first + 4 * g
            dst(mm, 128 * g, join(tile(0, h), tile(2048, h), odd))
            dst(mm, 768 + 256 * g, ff[:, 256 * h : 256 * h + 256])
        for k in range(2):
            h = first + 8 * k
            dst(mm, 512 + 128 * k, join(tile(4096, h), tile(4096, h + 4), odd))


def gather_kernel(x, dy, docs, qkv, ff, qb, fb, small, fc2, dense, cos, sin,
                  xg, dg, docg, normed_o, act_o, dup_o, wc_o, w2_o, heads, dsum, cst,
                  xv, dv, wc, w2g, eg, ws, es, nrm, act, dup, hs,
                  loc, us, ur, ds_, dr, ys, yr, as_, ar, es_, er,
                  wxs, wxr, wks, wkr, exs, exr, eks, ekr, fxs, fxr, fks, fkr, hss, hsr, hl, wb):
    n = Net()
    far = {"ctx": n.ctx + 2 * (1 - 2 * n.x) + 1 - 2 * n.c, "fsdp": n.z}
    n.barrier(more=(far,))

    def wrow(yy, xx, cc, zz):
        return wc.at[pl.ds(pl.multiple_of((yy * 16 + xx * 8 + cc * 4 + zz) * 64, 64), 64)]

    def wide(gg):
        return w2g.at[pl.ds(pl.multiple_of(gg * 256, 256), 256)]

    def thin(gg):
        return w2g.at[pl.ds(pl.multiple_of(1024 + gg * 64, 64), 64)]

    def shard(yy, zz, p):
        mm = yy * 4 + zz
        if p == 2:
            return docg.at[mm]
        return (xv, dv)[p].at[pl.ds(pl.multiple_of(mm * 128, 128), 128)]

    mine = (x, dy, docs)
    parts = (0, 1, 2)

    def tokens(p):
        n.go(remote(mine[p], shard(n.y, n.z, p), us.at[p, 0], ur.at[p, 0], n.up), n.z < 3)
        n.go(remote(mine[p], shard(n.y, n.z, p), ds_.at[p, 0], dr.at[p, 0], n.dn), n.z > 0)
        n.go(remote(mine[p], shard(n.y, n.z, p), ys.at[p, 0], yr.at[p, n.z], n.to_y))

    tokens(0)
    rows2 = ((fc2, wide), (dense, thin))
    for k, (ref, part) in enumerate(rows2):
        n.go(remote(ref, part(n.g), fxs.at[k], fxr.at[k], n.to_x))
        n.go(remote(ref, part(n.g), fks.at[k], fkr.at[k], n.to_c))

    def put_w(mm, col, value):
        ws[mm, :, col : col + value.shape[1]] = value

    def put_e(mm, col, value):
        es[mm, 0:1, col : col + value.shape[1]] = value[0:1]

    for mm in range(8):
        es[mm] = small[...]
    head_tiles((qkv, ff), put_w, 64)
    head_tiles((qb, fb), put_e, 8)
    for q in (4, 1, 3, 5, 7, 2, 6):
        to, yy, zz = n.member(q)
        n.go(remote(es.at[yy * 4 + zz], eg.at[n.g * 8 + n.m], es_.at[q], er.at[q], to))
        n.go(remote(ws.at[yy * 4 + zz], wrow(n.y, n.x, n.c, n.z), as_.at[q], ar.at[q], to))
    own = ws.at[n.m]
    n.go(remote(own, wrow(n.y, n.x, n.c, n.z), wxs.at[0], wxr.at[0], n.to_x))
    n.go(remote(own, wrow(n.y, n.x, n.c, n.z), wks.at[0], wkr.at[0], n.to_c))
    tokens(1)
    tokens(2)
    local = [
        pltpu.make_async_copy(x, shard(n.y, n.z, 0), loc.at[0]),
        pltpu.make_async_copy(dy, shard(n.y, n.z, 1), loc.at[1]),
        pltpu.make_async_copy(docs, shard(n.y, n.z, 2), loc.at[2]),
        pltpu.make_async_copy(own, wrow(n.y, n.x, n.c, n.z), loc.at[3]),
        pltpu.make_async_copy(es.at[n.m], eg.at[n.g * 8 + n.m], loc.at[4]),
        pltpu.make_async_copy(fc2, wide(n.g), loc.at[5]),
        pltpu.make_async_copy(dense, thin(n.g), loc.at[6]),
    ]
    for copy in local:
        copy.start()

    def line(d, ps):
        below, above = n.z >= d, n.z + d <= 3
        for p in ps:
            for there, zz, recv, send, nxt, more, to in (
                (below, n.z - d, ur, us, ur, n.z < 3, n.up),
                (above, n.z + d, dr, ds_, dr, n.z > 0, n.dn),
            ):
                block = shard(n.y, zz, p)

                @pl.when(there)
                def _():
                    arrive(block, recv.at[p, d - 1])

                if d < 3:
                    n.go(remote(block, block, send.at[p, d], nxt.at[p, d], to), there & more)
                slot = d if to is n.up else d + 3
                n.go(remote(block, block, ys.at[p, slot], yr.at[p, zz], n.to_y), there)

    def pieces(qs):
        for q in qs:
            yy, zz = n.source(q)
            block = wrow(yy, n.x, n.c, zz)
            arrive(block, ar.at[q])
            n.go(remote(block, block, wxs.at[q], wxr.at[q], n.to_x))
            n.go(remote(block, block, wks.at[q], wkr.at[q], n.to_c))

    def relay(qs):
        for q in qs:
            yy, zz = n.source(q)
            block = wrow(yy, n.xb, n.c, zz)
            arrive(block, wxr.at[q])
            n.go(remote(block, block, wks.at[8 + q], wkr.at[8 + q], n.to_c))

    line(1, (0,))
    pieces((4, 1, 3))
    line(1, (1, 2))
    pieces((5, 7, 2, 6))
    for q in range(1, 8):
        yy, zz = n.source(q)
        arrive(eg.at[n.g * 8 + yy * 4 + zz], er.at[q])
    local[4].wait()
    these = eg.at[pl.ds(n.g * 8, 8)]
    n.go(remote(these, these, exs.at[0], exr.at[0], n.to_x))
    n.go(remote(these, these, eks.at[0], ekr.at[0], n.to_c))
    line(2, parts)
    gx = n.xb * 2 + n.c
    for k, (ref, part) in enumerate(rows2):
        arrive(part(gx), fxr.at[k])
        n.go(remote(part(gx), part(gx), fks.at[2 + k], fkr.at[2 + k], n.to_c))
    theirs = eg.at[pl.ds(gx * 8, 8)]
    relay((0, 4, 1, 3, 5, 7, 2, 6))
    arrive(theirs, exr.at[0])
    n.go(remote(theirs, theirs, eks.at[1], ekr.at[1], n.to_c))
    line(3, parts)
    for q in range(8):
        yy, zz = n.source(q)
        arrive(wrow(yy, n.x, n.cb, zz), wkr.at[q])
        arrive(wrow(yy, n.xb, n.cb, zz), wkr.at[8 + q])
    for k in range(2):
        gg = 2 * (n.xb if k else n.x) + n.cb
        arrive(eg.at[pl.ds(gg * 8, 8)], ekr.at[k])
        for j, (ref, part) in enumerate(rows2):
            arrive(part(gg), fkr.at[2 * k + j])
    for k in (0, 1, 2, 3, 5, 6):
        local[k].wait()
    out_w = [pltpu.make_async_copy(wc, wc_o, wb.at[0]), pltpu.make_async_copy(w2g, w2_o, wb.at[1])]
    for copy in out_w:
        copy.start()

    def add_ext(i, t):
        return t + eg[i].astype(F32)

    ext = lax.fori_loop(0, 32, add_ext, jnp.zeros((8, 1792), F32))
    cst[0:1, 0:1792], cst[0:1, 1792:2048] = ext[1:2], ext[5:6, 0:256]
    cst[1:2, 0:1792], cst[1:2, 1792:2048] = ext[2:3], ext[5:6, 256:512]
    cst[2:3, 0:1792], cst[2:3, 1792:2048] = ext[3:4] + ext[4:5], ext[5:6, 512:768] + ext[5:6, 768:1024]
    cst[3:4, 0:1792], cst[3:4, 1792:2048] = ext[0:1], jnp.zeros((1, 256), F32)
    cst[4:8, :] = jnp.zeros((4, 2048), F32)
    dsum[...] = jnp.zeros_like(dsum)
    z0 = lax.div(n.z, 2)
    half = lanes_of((256, 128)) < 64

    def rows_of(j):
        yy = n.y + lax.div(j, 2) * (1 - 2 * n.y)
        zp = z0 + lax.rem(j, 2) * (1 - 2 * z0)
        return yy, zp, pl.ds(pl.multiple_of((yy * 4 + 2 * zp) * 128, 256), 256)

    def sends(j):
        yy, zp, rows = rows_of(j)
        return [
            remote(hs.at[gg, rows], heads.at[n.g, rows], hss.at[j, k], hsr.at[j, k], to)
            for k, (to, gg) in enumerate(((far, 2 * n.xb + n.cb), (n.to_x, 2 * n.xb + n.c), (n.to_c, 2 * n.x + n.cb)))
        ]

    def keeps(j):
        yy, zp, rows = rows_of(j)
        return [
            pltpu.make_async_copy(hs.at[n.g, rows], heads.at[n.g, rows], hl.at[j, 0]),
            pltpu.make_async_copy(nrm.at[rows], normed_o.at[rows], hl.at[j, 1]),
            pltpu.make_async_copy(act.at[rows], act_o.at[rows], hl.at[j, 2]),
            pltpu.make_async_copy(dup.at[rows], dup_o.at[rows], hl.at[j, 3]),
            pltpu.make_async_copy(xv.at[rows], xg.at[rows], hl.at[j, 4]),
            pltpu.make_async_copy(dv.at[rows], dg.at[rows], hl.at[j, 5]),
        ]

    def pair(j, carry):
        yy, zp, rows = rows_of(j)
        base = (yy * 4 + 2 * zp) * 128

        @pl.when(j >= 2)
        def _():
            for k in range(2):
                for p in parts:
                    arrive(shard(yy, 2 * zp + k, p), yr.at[p, 2 * zp + k])

        def norm(i, c):
            sl = pl.ds(pl.multiple_of(base + 32 * i, 32), 32)
            xf = xv[sl, :].astype(F32)
            cen = xf - jnp.mean(xf, axis=-1, keepdims=True)
            rstd = lax.rsqrt(jnp.mean(cen * cen, axis=-1, keepdims=True) + EPS)
            nrm[sl, :] = (cen * rstd * cst[0:1, :] + cst[1:2, :]).astype(BF)
            return c

        lax.fori_loop(0, 8, norm, 0)
        table = pl.ds(pl.multiple_of(yy * 128, 128), 128)
        cosv = jnp.concatenate([cos[table, :]] * 2, axis=0)
        sinv = jnp.concatenate([sin[table, :]] * 2, axis=0)
        for k in range(2):
            t2 = jnp.dot(nrm[rows, :], wc[:, 256 * k : 256 * k + 256], preferred_element_type=F32)
            t2 = t2 + cst[3:4, 256 * k : 256 * k + 256]
            for i in range(2):
                t = t2[:, 128 * i : 128 * i + 128]
                hs[2 * k + i, rows, 0:128] = (t * cosv + partner(t) * sinv).astype(BF)
        v4 = jnp.dot(nrm[rows, :], wc[:, 512:768], preferred_element_type=F32) + cst[3:4, 512:768]
        d4 = dot_nt(dv[rows, :], w2g[1024:1280, :])
        for g in range(4):
            v, d = (t[:, 128 * (g // 2) : 128 * (g // 2) + 128] for t in (v4, d4))
            if g % 2 == 0:
                vd = jnp.where(half, v, pltpu.roll(d, 64, 1))
            else:
                vd = jnp.where(half, pltpu.roll(v, 64, 1), d)
            hs[g, rows, 128:256] = vd.astype(BF)
        for copy in sends(j):
            copy.start()
        for k in range(4):
            cols, wcols = slice(256 * k, 256 * k + 256), slice(768 + 256 * k, 1024 + 256 * k)
            up = jnp.dot(nrm[rows, :], wc[:, wcols], preferred_element_type=F32) + cst[3:4, wcols]
            a, slope = gelu_pair(up)
            act[rows, cols] = a.astype(BF)
            du = dot_nt(dv[rows, :], w2g[cols, :]) * slope
            dup[rows, cols] = du.astype(BF)
            dsum[:, cols] += jnp.broadcast_to(jnp.sum(du, axis=0, keepdims=True), (8, 256))
        for copy in keeps(j):
            copy.start()
        return carry

    lax.fori_loop(0, 4, pair, 0)
    for j in range(4):
        for copy in sends(j):
            copy.wait()
        for copy in keeps(j):
            copy.wait()
    for copy in out_w:
        copy.wait()
    n.drain()


def gather_all(x, dy, docs, qkv, ff, qb, fb, small, fc2, dense, cos, sin):
    sd = jax.ShapeDtypeStruct
    V = pltpu.VMEM
    return pl.pallas_call(
        gather_kernel,
        name="gather_all",
        out_shape=(sd((1024, 2048), BF), sd((1024, 2048), BF), sd((8, 8, 1024), BF), sd((1024, 2048), BF),
                   sd((1024, 1024), BF), sd((1024, 1024), BF), sd((2048, 1792), BF), sd((1280, 2048), BF),
                   sd((4, 1024, 256), BF), sd((8, 1024), F32), sd((8, 2048), F32)),
        in_specs=[VM] * 12,
        out_specs=(HBM, HBM, VM, HBM, HBM, HBM, HBM, HBM, HBM, VM, VM),
        scratch_shapes=[V((1024, 2048), BF), V((1024, 2048), BF), V((2048, 1792), BF), V((1280, 2048), BF),
                        V((32, 8, 1792), BF), V((8, 64, 1792), BF), V((8, 8, 1792), BF),
                        V((1024, 2048), BF), V((1024, 1024), BF), V((1024, 1024), BF), V((4, 1024, 256), BF),
                        DMA((7,)), DMA((3, 3)), DMA((3, 3)), DMA((3, 3)), DMA((3, 3)), DMA((3, 7)), DMA((3, 4)),
                        DMA((8,)), DMA((8,)), DMA((8,)), DMA((8,)), DMA((8,)), DMA((8,)), DMA((16,)), DMA((16,)),
                        DMA((1,)), DMA((1,)), DMA((2,)), DMA((2,)), DMA((2,)), DMA((2,)), DMA((4,)), DMA((4,)),
                        DMA((4, 3)), DMA((4, 3)), DMA((4, 6)), DMA((2,))],
        compiler_params=pltpu.CompilerParams(collective_id=1, has_side_effects=True, vmem_limit_bytes=VLIM),
    )(x, dy, docs, qkv, ff, qb, fb, small, fc2, dense, cos, sin)


def lanes_of(shape):
    return lax.broadcasted_iota(jnp.int32, shape, len(shape) - 1)


def partner(t):
    low = lax.rem(lanes_of(t.shape), 64) < 16
    return jnp.where(low, pltpu.roll(t, 112, 1), pltpu.roll(t, 16, 1))


def dot_nt(a, b):
    return lax.dot_general(a, b, (((1,), (1,)), ((), ())), preferred_element_type=F32)


def dot_tn(a, b):
    return lax.dot_general(a, b, (((0,), (0,)), ((), ())), preferred_element_type=F32)


def attention_kernel(slot_of, a, docs, cos, sin, out, sums, seq, att, dq, dk, dv):
    def where_is(p):
        r = slot_of[p]
        ctx = lax.div(r, 2)
        return lax.rem(ctx, 4), lax.div(ctx, 4), pl.ds(pl.multiple_of(lax.rem(r, 2) * 64, 64), 64)

    for p in range(16):
        g, yy, rows = where_is(p)
        seq[64 * p : 64 * p + 64, :] = a[g, yy, 0, rows, :]
    dk[...] = jnp.zeros_like(dk)
    dv[...] = jnp.zeros_like(dv)
    scale = 0.125
    low = lanes_of((256, 128)) < 64
    for i in range(4):
        k0 = max(0, i - 2) * 256
        kn = 256 * (i + 1) - k0
        rq, rk = slice(256 * i, 256 * i + 256), slice(k0, k0 + kn)
        qk, vd = seq[rq, 0:128], seq[rq, 128:256]
        kk, vv = seq[rk, 0:128], seq[rk, 128:256]
        zero = jnp.zeros((256, 128), F32)
        qs = jnp.where(low, zero, pltpu.roll(qk.astype(F32), 64, 1)).astype(BF)
        dsf = jnp.where(low, pltpu.roll(vd.astype(F32), 64, 1), zero)
        s = dot_nt(qs, kk) * scale
        qpos = 256 * i + lax.broadcasted_iota(jnp.int32, (256, kn), 0)
        kpos = k0 + lax.broadcasted_iota(jnp.int32, (256, kn), 1)
        own = jnp.broadcast_to(docs[0, 0:1, rq].astype(F32), (128, 256)).T[:, 0:1]
        mask = (kpos <= qpos) & (docs[0, 0:1, rk].astype(F32) == own)
        s = jnp.where(mask, s, NEG)
        top = jnp.max(s, axis=-1, keepdims=True)
        e = jnp.where(mask, jnp.exp(s - top), 0.0)
        inv = 1.0 / jnp.sum(e, axis=-1, keepdims=True)
        o = jnp.dot(e.astype(BF), vv, preferred_element_type=F32) * inv
        ob = o.astype(BF)
        att[rq, :] = ob.astype(F32)
        delta = jnp.sum(dsf * ob.astype(F32), axis=-1, keepdims=True)
        pr = e * inv
        dv[rk, :] += dot_tn(pr.astype(BF), vd)
        dp = dot_nt(dsf.astype(BF), vv)
        ds = (pr * (dp - delta) * scale).astype(BF)
        dq[rq, :] = jnp.dot(ds, kk, preferred_element_type=F32)
        dk[rk, :] += dot_tn(ds, qk)
    tot = jnp.zeros((8, 256), F32)
    half = lanes_of((64, 128)) < 64
    s1 = jnp.zeros((1, 128), F32)
    s2 = jnp.zeros((1, 128), F32)
    for p in range(16):
        rows = slice(64 * p, 64 * p + 64)
        g, yy, place_rows = where_is(p)
        t = jnp.where(half, pltpu.roll(dq[rows, :], 64, 1), pltpu.roll(dk[rows, :], 64, 1))
        t = t * cos[rows, :] - partner(t) * sin[rows, :]
        u = jnp.where(half, pltpu.roll(dv[rows, :], 64, 1), pltpu.roll(att[rows, :], 64, 1))
        s1 += jnp.sum(t, axis=0, keepdims=True)
        s2 += jnp.sum(u, axis=0, keepdims=True)
        out[g, yy, 0, place_rows, 0:128] = t.astype(BF)
        out[g, yy, 0, place_rows, 128:256] = u.astype(BF)
    sums[0, :, 0:128] = jnp.broadcast_to(s1, (8, 128))
    sums[0, :, 128:256] = jnp.broadcast_to(s2, (8, 128))


def attention(slot_of, a, docs, cos, sin):
    sd = jax.ShapeDtypeStruct
    blk = pl.BlockSpec((4, 2, 1, 128, 256), lambda s, t: (0, 0, s, 0, 0))
    return pl.pallas_call(
        attention_kernel,
        name="attention",
        grid_spec=pltpu.PrefetchScalarGridSpec(
            num_scalar_prefetch=1,
            grid=(4,),
            in_specs=[
                blk,
                pl.BlockSpec((1, 8, 1024), lambda s, t: (s, 0, 0)),
                pl.BlockSpec((1024, 128), lambda s, t: (0, 0)),
                pl.BlockSpec((1024, 128), lambda s, t: (0, 0)),
            ],
            out_specs=(blk, pl.BlockSpec((1, 8, 256), lambda s, t: (s, 0, 0))),
            scratch_shapes=[pltpu.VMEM((1024, 256), BF)] + [pltpu.VMEM((1024, 128), F32)] * 4,
        ),
        out_shape=(sd((4, 2, 4, 128, 256), BF), sd((4, 8, 256), F32)),
        compiler_params=pltpu.CompilerParams(vmem_limit_bytes=VLIM),
    )(slot_of, a, docs, cos, sin)


def add_rows(dst, srcs, rows, out=None, step=16):
    out = dst if out is None else out

    def body(i, carry):
        sl = pl.ds(pl.multiple_of(i * step, step), step)
        v = dst[sl, :].astype(F32)
        for s in srcs:
            v = v + s[sl, :].astype(F32)
        out[sl, :] = v.astype(out.dtype)
        return carry

    lax.fori_loop(0, rows // step, body, 0)


def reduce_kernel(att, normed_i, dy_i, x_i, act_i, dup_i, wc_i, w2_i, sums, dsum,
                  yo, o1, o2, eo, dbo,
                  nrm, dy, wc, w2, dpr, up2, rec, ysend, yr, ud, own, r1, st1, r2, s1, st2, s2, thin2, xst, mu, rs, acc, ev, t1, t2, d1,
                  hss, hsr, hl, ld, xl, yss, yrs, uss, urs, k1s, k1r, x1s, x1r, a1s, a1r,
                  k2s, k2r, x2s, x2r, eks, ekr, exs, exr, eas, ear, dbs, dbr, fl):
    n = Net()
    far = {"ctx": n.ctx + 2 * (1 - 2 * n.x) + 1 - 2 * n.c, "fsdp": n.z}
    n.barrier(more=(far,))
    z0 = lax.div(n.z, 2)
    zf = 1 - z0

    def halves(k):
        yy = n.y if k % 2 else n.yb
        tile = 0 if k >= 2 else 1
        return pl.ds(pl.multiple_of(yy * 512, 512), 512), pl.ds(128 * tile, 128)

    for k in range(4):
        rows, lanes = halves(k)
        for i, (to, gg) in enumerate(((far, 2 * n.xb + n.cb), (n.to_x, 2 * n.xb + n.c), (n.to_c, 2 * n.x + n.cb))):
            n.go(remote(att.at[gg, rows, lanes], rec.at[n.g, rows, lanes], hss.at[k, i], hsr.at[k, i], to))
    keep = pltpu.make_async_copy(att.at[n.g], rec.at[n.g], hl.at[0])
    loads = [
        pltpu.make_async_copy(dy_i, dy, ld.at[0]),
        pltpu.make_async_copy(act_i, up2.at[:, pl.ds(0, 1024)], ld.at[1]),
        pltpu.make_async_copy(w2_i, w2, ld.at[2]),
        pltpu.make_async_copy(dup_i, dpr.at[:, pl.ds(768, 1024)], ld.at[3]),
        pltpu.make_async_copy(normed_i, nrm, ld.at[4]),
        pltpu.make_async_copy(wc_i, wc, ld.at[5]),
    ]
    for copy in loads[:2] + [keep] + loads[2:]:
        copy.start()

    def heads_in(k):
        rows, lanes = halves(k)
        for i, gg in enumerate((2 * n.xb + n.cb, 2 * n.xb + n.c, 2 * n.x + n.cb)):
            arrive(rec.at[gg, rows, lanes], hsr.at[k, i])

    low = lanes_of((64, 128)) < 64

    def split(k):
        yy = n.y if k % 2 else n.yb

        def body(i, carry):
            sl = pl.ds(pl.multiple_of(yy * 512 + 64 * i, 64), 64)
            for p in range(2):
                a, b = rec[2 * p, sl, 128:256].astype(F32), rec[2 * p + 1, sl, 128:256].astype(F32)
                up2[sl, 1024 + 128 * p : 1152 + 128 * p] = jnp.where(low, pltpu.roll(a, 64, 1), b).astype(BF)
                dpr[sl, 512 + 128 * p : 640 + 128 * p] = jnp.where(low, a, pltpu.roll(b, 64, 1)).astype(BF)
            return carry

        lax.fori_loop(0, 8, body, 0)

    def pair_rows(yy, zp):
        return pl.ds(pl.multiple_of((yy * 4 + 2 * zp) * 128, 256), 256)

    def into(dst, zp, cols, value):
        dst(2 * zp)[:, cols] = value[0:128].astype(BF)
        dst(2 * zp + 1)[:, cols] = value[128:256].astype(BF)

    def y_pair(yy, zp, dst):
        rows = pair_rows(yy, zp)
        for k in range(4):
            cols = slice(512 * k, 512 * k + 512)
            into(dst, zp, cols, jnp.dot(up2[rows, :], w2[:, cols], preferred_element_type=F32))

    def dn_pair(yy, zp, dst):
        rows = pair_rows(yy, zp)
        load = pltpu.make_async_copy(x_i.at[rows], xst, xl.at[0])
        load.start()
        load.wait()

        def stats(i, carry):
            sl = pl.ds(pl.multiple_of(32 * i, 32), 32)
            xf = xst[sl, :].astype(F32)
            mean = jnp.mean(xf, axis=-1, keepdims=True)
            cen = xf - mean
            mu[sl, :] = jnp.broadcast_to(mean, (32, 128))
            rs[sl, :] = jnp.broadcast_to(lax.rsqrt(jnp.mean(cen * cen, axis=-1, keepdims=True) + EPS), (32, 128))
            return carry

        lax.fori_loop(0, 8, stats, 0)
        for k in range(8):
            cols = slice(256 * k, 256 * k + 256)
            d = dot_nt(dpr[rows, :], wc[cols, :])
            xh = (xst[:, cols].astype(F32) - mu[:, 0:1]) * rs[:, 0:1]
            acc[0:1, cols] += jnp.sum(d * xh, axis=0, keepdims=True)
            acc[1:2, cols] += jnp.sum(d, axis=0, keepdims=True)
            into(dst, zp, cols, d)

    def send_y(t, buf, k, j):
        n.go(remote(buf, yr.at[k, t], yss.at[t, j], yrs.at[t, k], n.to_y))

    def w1_rows(yy, xx, cc):
        return pl.ds(pl.multiple_of((yy * 16 + xx * 8 + cc * 4) * 64, 256), 256)

    def w1_part(yy, xx, cc, cols):
        return dot_tn(nrm[:, w1_rows(yy, xx, cc)], dpr[:, cols])

    def w2_cols(gg):
        return pl.ds(pl.multiple_of(gg * 256, 256), 256)

    wide, thin = pl.ds(0, 256), pl.ds(256, 64)
    acc[...] = jnp.zeros_like(acc)

    loads[0].wait()
    loads[1].wait()
    for xx in range(2):
        for k in range(4):
            cols = slice(512 * k, 512 * k + 512)
            st2[xx, 0:256, cols] = dot_tn(up2[:, w2_cols(2 * xx + n.cb)], dy[:, cols]).astype(BF)
        n.go(remote(st2.at[xx, wide], s1.at[xx, wide], k2s.at[xx, 0], k2r.at[xx, 0], n.to_c))
    loads[2].wait()
    keep.wait()
    heads_in(0)
    split(0)
    y_pair(n.yb, zf, lambda k: ysend.at[k])
    send_y(0, ysend.at[3 * zf], 3 * zf, 0)
    send_y(0, ysend.at[1 + zf], 1 + zf, 1)
    zn = n.z + 1 - 2 * lax.rem(n.z, 2)
    y_pair(n.yb, z0, lambda k: ysend.at[k])
    send_y(0, ysend.at[zn], zn, 2)
    send_y(0, ysend.at[n.z], n.z, 3)
    heads_in(1)
    split(1)
    for zp in (zf, z0):
        y_pair(n.y, zp, lambda k: own.at[k, 0])
    for xx in range(2):
        for k in range(4):
            cols = slice(512 * k, 512 * k + 512)
            two = dot_tn(up2[:, 1024 + 128 * xx : 1152 + 128 * xx], dy[:, cols])
            st2[xx, 256:320, cols] = jnp.where(n.c == 0, two[64:128], two[0:64]).astype(BF)
            thin2[64 * xx : 64 * xx + 64, cols] = jnp.where(n.c == 0, two[0:64], two[64:128]).astype(BF)
        n.go(remote(st2.at[xx, thin], s1.at[xx, thin], k2s.at[xx, 1], k2r.at[xx, 1], n.to_c))
    heads_in(2)
    heads_in(3)

    def whole(i, carry):
        sl = pl.ds(pl.multiple_of(64 * i, 64), 64)
        for g in range(4):
            dpr[sl, 128 * g : 128 * g + 128] = rec[g, sl, 0:128]
        return carry

    lax.fori_loop(0, 16, whole, 0)
    loads[3].wait()
    loads[4].wait()
    staged = []
    for k, (yy, xx) in enumerate(((0, 0), (1, 0), (0, 1), (1, 1))):
        if k >= 2:
            staged[k - 2].wait_send()
        for i in range(7):
            cols = slice(256 * i, 256 * i + 256)
            st1[k % 2, :, cols] = w1_part(yy, xx, n.cb, cols).astype(BF)
        copy = remote(st1.at[k % 2], r1.at[yy * 2 + xx], k1s.at[k], k1r.at[yy * 2 + xx], n.to_c)
        copy.start()
        staged.append(copy)

    def w1_own(yy, xx):
        block = r1.at[yy * 2 + xx]
        arrive(block, k1r.at[yy * 2 + xx])
        for i in range(7):
            cols = slice(256 * i, 256 * i + 256)
            block[:, cols] = (block[:, cols].astype(F32) + w1_part(yy, xx, n.c, cols)).astype(BF)

    def w2_own(xx):
        gg = 2 * xx + n.c
        arrive(s1.at[xx, wide], k2r.at[xx, 0])
        arrive(s1.at[xx, thin], k2r.at[xx, 1])
        for k in range(4):
            cols = slice(512 * k, 512 * k + 512)
            s1[xx, 0:256, cols] = (s1[xx, 0:256, cols].astype(F32) + dot_tn(up2[:, w2_cols(gg)], dy[:, cols])).astype(BF)
        mine = pl.ds(pl.multiple_of(64 * xx, 64), 64)
        s1[xx, 256:320, :] = (s1[xx, 256:320, :].astype(F32) + thin2[mine, :].astype(F32)).astype(BF)

    for yy in range(2):
        w1_own(yy, n.xb)
        n.go(remote(r1.at[yy * 2 + n.xb], r2.at[yy], x1s.at[yy], x1r.at[yy], n.to_x))
    loads[5].wait()
    def spare_at(k):
        return w2.at[pl.ds(pl.multiple_of(128 * k, 128), 128)]

    dn_pair(n.yb, zf, spare_at)
    send_y(1, spare_at(3 * zf), 3 * zf, 0)
    send_y(1, spare_at(1 + zf), 1 + zf, 1)
    dn_pair(n.yb, z0, spare_at)
    send_y(1, spare_at(zn), zn, 2)
    send_y(1, spare_at(n.z), n.z, 3)

    def forward(t, j):
        k = (3 * zf, 1 + zf, zn)[j]
        up = jnp.where(k > n.z, 1, 0)
        slot = k + up
        block = own.at[k, t]
        arrive(yr.at[k, t], yrs.at[t, k])
        inner = (n.z > 0) & (k > n.z) | (n.z < 3) & (k < n.z)

        @pl.when(inner)
        def _():
            arrive(ud.at[slot, t], urs.at[t, slot])
            add_rows(block, [yr.at[k, t], ud.at[slot, t]], 128)

        @pl.when(jnp.logical_not(inner))
        def _():
            add_rows(block, [yr.at[k, t]], 128)

        to = {"ctx": n.ctx, "fsdp": n.z + 2 * up - 1}
        n.go(remote(block, ud.at[slot, t], uss.at[t, j], urs.at[t, slot], to))

    def finish(t):
        k = n.z
        arrive(yr.at[k, t], yrs.at[t, k])

        @pl.when(n.z > 0)
        def _():
            arrive(ud.at[k + 1, t], urs.at[t, k + 1])

        @pl.when(n.z < 3)
        def _():
            arrive(ud.at[k, t], urs.at[t, k])

        @pl.when(n.z == 0)
        def _():
            add_rows(own.at[k, t], [yr.at[k, t], ud.at[k, t]], 128, yo.at[t])

        @pl.when(n.z == 3)
        def _():
            add_rows(own.at[k, t], [yr.at[k, t], ud.at[k + 1, t]], 128, yo.at[t])

        @pl.when((n.z > 0) & (n.z < 3))
        def _():
            add_rows(own.at[k, t], [yr.at[k, t], ud.at[k, t], ud.at[k + 1, t]], 128, yo.at[t])

    forward(0, 0)
    forward(0, 1)
    w2_own(n.xb)
    staged[2].wait_send()
    staged[3].wait_send()
    n.go(remote(s1.at[n.xb], s2, x2s.at[0], x2r.at[0], n.to_x))
    forward(0, 2)
    for zp in (zf, z0):
        dn_pair(n.y, zp, lambda k: own.at[k, 1])
    forward(1, 0)
    ones = jnp.ones((8, 1024), BF)
    d1[0] = jnp.dot(ones, dy[...], preferred_element_type=F32)
    tot = sums[0, 0:1, :] + sums[1, 0:1, :] + sums[2, 0:1, :] + sums[3, 0:1, :]
    lo1 = lanes_of((1, 128)) < 64
    zero = jnp.zeros((1, 128), F32)
    vsum = jnp.where(n.c == 0, jnp.where(lo1, tot[:, 128:256], zero), jnp.where(lo1, zero, pltpu.roll(tot[:, 128:256], 64, 1)))
    for g in range(4):
        for mm in range(8):
            e = ev.at[g * 8 + mm]
            for k in range(4):
                e[k : k + 1, :] = jnp.where(n.g == k, tot[:, 0:128], zero)
            for k in range(2):
                e[4 + k : 5 + k, :] = jnp.where(n.x == k, vsum, zero)
            for k in range(8):
                e[6 + k : 7 + k, :] = dsum[0:1, 128 * k : 128 * k + 128]
            tile = 128 * ((mm // 4) * 8 + g * 2 + (mm % 4) // 2)
            e[14:15, :] = acc[0:1, tile : tile + 128]
            e[15:16, :] = acc[1:2, tile : tile + 128]
    for xx in range(2):
        n.go(remote(ev.at[pl.ds((2 * xx + n.cb) * 8, 8)], t1.at[xx], eks.at[xx], ekr.at[xx], n.to_c))
    n.go(remote(d1.at[0], d1.at[1], dbs.at[0], dbr.at[0], n.to_c))
    for yy in range(2):
        w1_own(yy, n.x)
    forward(1, 1)
    for xx in range(2):
        arrive(t1.at[xx], ekr.at[xx])
        sl = pl.ds((2 * xx + n.c) * 8, 8)
        ev[sl] = ev[sl] + t1[xx]
    arrive(d1.at[1], dbr.at[0])
    d1[2] = d1[0] + d1[1]
    n.go(remote(ev.at[pl.ds((2 * n.xb + n.c) * 8, 8)], t2, exs.at[0], exr.at[0], n.to_x))
    n.go(remote(d1.at[2], d1.at[3], dbs.at[1], dbr.at[1], n.to_x))
    w2_own(n.x)
    for yy in range(2):
        arrive(r2.at[yy], x1r.at[yy])
        add_rows(r1.at[yy * 2 + n.x], [r2.at[yy]], 256)
    for q in (4, 1, 3, 5, 7, 2, 6):
        to, yy, zz = n.member(q)
        n.go(remote(r1.at[yy * 2 + n.x, pl.ds(pl.multiple_of(zz * 64, 64), 64)], o1.at[n.m], a1s.at[q], a1r.at[q], to))
    mine = pltpu.make_async_copy(r1.at[n.y * 2 + n.x, pl.ds(pl.multiple_of(n.z * 64, 64), 64)], o1.at[n.m], fl.at[0])
    mine.start()
    arrive(t2, exr.at[0])
    final = pl.ds(n.g * 8, 8)
    ev[final] = ev[final] + t2[...]
    for q in range(1, 8):
        to, yy, zz = n.member(q)
        n.go(remote(ev.at[n.g * 8 + yy * 4 + zz], eo.at[n.m], eas.at[q], ear.at[q], to))
    eo[n.m] = ev[n.g * 8 + n.m]
    arrive(d1.at[3], dbr.at[1])
    dbo[...] = d1[2] + d1[3]
    forward(1, 2)
    finish(0)
    arrive(s2, x2r.at[0])
    add_rows(s1.at[n.x], [s2], 320)
    out2 = pltpu.make_async_copy(s1.at[n.x], o2, fl.at[1])
    out2.start()
    finish(1)
    for q in range(1, 8):
        yy, zz = n.source(q)
        arrive(eo.at[yy * 4 + zz], ear.at[q])
        arrive(o1.at[yy * 4 + zz], a1r.at[q])
    mine.wait()
    out2.wait()
    n.drain()


def reduce_all(att, normed, dy, x, act, dup, wc, w2, sums, dsum):
    sd = jax.ShapeDtypeStruct
    V = pltpu.VMEM
    return pl.pallas_call(
        reduce_kernel,
        name="reduce_all",
        out_shape=(sd((2, 128, 2048), F32), sd((8, 64, 1792), BF), sd((320, 2048), BF), sd((8, 16, 128), F32),
                   sd((8, 2048), F32)),
        in_specs=[HBM] * 8 + [VM] * 2,
        out_specs=(VM, HBM, HBM, VM, VM),
        scratch_shapes=[
            V((1024, 2048), BF), V((1024, 2048), BF), V((2048, 1792), BF), V((1280, 2048), BF),
            V((1024, 1792), BF), V((1024, 1280), BF), V((4, 1024, 256), BF),
            V((4, 128, 2048), BF), V((4, 2, 128, 2048), BF), V((5, 2, 128, 2048), BF), V((4, 2, 128, 2048), BF),
            V((4, 256, 1792), BF), V((2, 256, 1792), BF), V((2, 256, 1792), BF),
            V((2, 320, 2048), BF), V((2, 320, 2048), BF), V((320, 2048), BF), V((128, 2048), BF),
            V((256, 2048), BF), V((256, 128), F32), V((256, 128), F32), V((8, 2048), F32),
            V((32, 16, 128), F32), V((2, 8, 16, 128), F32), V((8, 16, 128), F32), V((4, 8, 2048), F32),
            DMA((4, 3)), DMA((4, 3)), DMA((1,)), DMA((6,)), DMA((1,)),
            DMA((2, 4)), DMA((2, 4)), DMA((2, 3)), DMA((2, 5)),
            DMA((4,)), DMA((4,)), DMA((2,)), DMA((2,)), DMA((8,)), DMA((8,)),
            DMA((2, 2)), DMA((2, 2)), DMA((1,)), DMA((1,)),
            DMA((2,)), DMA((2,)), DMA((1,)), DMA((1,)), DMA((8,)), DMA((8,)), DMA((2,)), DMA((2,)), DMA((2,)),
        ],
        compiler_params=pltpu.CompilerParams(collective_id=3, has_side_effects=True, vmem_limit_bytes=67000000),
    )(att, normed, dy, x, act, dup, wc, w2, sums, dsum)


def finish_kernel(x, dy, yo, o1, o2, cst, y, dx, dqkv, dff, dfc2, ddense):
    low = lanes_of((64, 128)) < 64
    for i in range(16):
        yy, g, zp = i // 8, (i // 2) % 4, i % 2
        a, b = yy * 4 + 2 * zp, yy * 4 + 2 * zp + 1
        cols = slice(128 * i, 128 * i + 128)
        src = slice(128 * g, 128 * g + 128)
        even, odd = o1[a, :, src].astype(F32), o1[b, :, src].astype(F32)
        dqkv[:, cols] = jnp.where(low, even, pltpu.roll(odd, 64, 1))
        dqkv[:, 2048 + 128 * i : 2176 + 128 * i] = jnp.where(low, pltpu.roll(even, 64, 1), odd)
        src = slice(512 + 128 * (g // 2), 640 + 128 * (g // 2))
        even, odd = o1[a, :, src].astype(F32), o1[b, :, src].astype(F32)
        if g % 2 == 0:
            v = jnp.where(low, even, pltpu.roll(odd, 64, 1))
        else:
            v = jnp.where(low, pltpu.roll(even, 64, 1), odd)
        dqkv[:, 4096 + 128 * i : 4224 + 128 * i] = v
    for h in range(32):
        mm, g = (h // 16) * 4 + h % 4, (h // 4) % 4
        dff[:, 256 * h : 256 * h + 256] = o1[mm, :, 768 + 256 * g : 1024 + 256 * g].astype(F32)
    dfc2[...] = o2[0:256, :].astype(F32)
    ddense[...] = o2[256:320, :].astype(F32)

    def body(i, carry):
        sl = pl.ds(pl.multiple_of(16 * i, 16), 16)
        xf = x[sl, :].astype(F32)
        cen = xf - jnp.mean(xf, axis=-1, keepdims=True)
        rstd = lax.rsqrt(jnp.mean(cen * cen, axis=-1, keepdims=True) + EPS)
        xhat = cen * rstd
        y[sl, :] = (xf + yo[0, sl, :] + cst[2:3, :]).astype(BF)
        gr = yo[1, sl, :] * cst[0:1, :]
        dx[sl, :] = dy[sl, :].astype(F32) + rstd * (
            gr - jnp.mean(gr, axis=-1, keepdims=True) - xhat * jnp.mean(gr * xhat, axis=-1, keepdims=True)
        )
        return carry

    lax.fori_loop(0, 8, body, 0)


def finish_all(x, dy, yo, o1, o2, cst):
    sd = jax.ShapeDtypeStruct
    return pl.pallas_call(
        finish_kernel,
        name="finish_all",
        out_shape=(sd((128, 2048), BF), sd((128, 2048), F32), sd((64, 6144), F32), sd((64, 8192), F32),
                   sd((256, 2048), F32), sd((64, 2048), F32)),
        in_specs=[VM] * 6,
        out_specs=(VM,) * 6,
        compiler_params=pltpu.CompilerParams(vmem_limit_bytes=VLIM),
    )(x, dy, yo, o1, o2, cst)


def stored_columns(a):
    rows = a.shape[1]
    qk = a[:, :, :512].reshape(2, 4, rows, 4, 2, 64).transpose(2, 4, 0, 3, 1, 5).reshape(rows, 2, 2048)
    v = a[:, :, 512:768].reshape(2, 4, rows, 4, 64).transpose(2, 0, 3, 1, 4).reshape(rows, 1, 2048)
    f = a[:, :, 768:1792].reshape(2, 4, rows, 4, 256).transpose(2, 0, 3, 1, 4).reshape(rows, 8192)
    return jnp.concatenate([qk, v], axis=1).reshape(rows, 6144), f


def rotary_lanes(pos):
    lane = jnp.arange(128, dtype=jnp.int32) % 64
    freqs = jnp.exp(-(2.0 * (lane % (ROT // 2)).astype(F32) / ROT) * math.log(10000.0))
    angles = pos.astype(F32)[:, None] * freqs[None]
    turns = lane < ROT
    sign = jnp.where(turns, jnp.where(lane < ROT // 2, -1.0, 1.0), 0.0)
    return jnp.where(turns, jnp.cos(angles), 1.0), jnp.sin(angles) * sign


def fast_device(
    block_input, output_grad, segment, slots, ln_gain, ln_bias, qkv_w, qkv_b, dense_w, dense_b, fc1_w, fc1_b, fc2_w, fc2_b
):
    ctx, y, x, c, z = place()
    g, m = x * 2 + c, y * 4 + z
    index = ctx * 4 + z
    xb, dyb = block_input[0], output_grad[0]

    def spread(piece, total):
        count = piece.shape[0]
        own = jnp.arange(total, dtype=jnp.int32) // count == index
        return jnp.where(own, jnp.tile(piece, total // count), jnp.zeros((), BF))

    docs = jnp.broadcast_to(segment.astype(BF), (8, 1024))
    qb = jnp.broadcast_to(spread(qkv_b, 6144)[None], (8, 6144))
    fb = jnp.broadcast_to(spread(fc1_b, 8192)[None], (8, 8192))
    vecs = jnp.stack([spread(v, 2048) for v in (ln_gain, ln_bias, dense_b, fc2_b)])
    rest = jnp.pad(vecs[:, 1792:].reshape(1, 1024), ((0, 0), (0, 768)))
    small = jnp.concatenate([jnp.zeros((1, 1792), BF), vecs[:, :1792], rest, jnp.zeros((2, 1792), BF)], axis=0)
    pairs = lax.dynamic_slice_in_dim(slots.reshape(2, 4, 2), g, 1, 1).reshape(4)
    rows = (pairs[:, None] * 64 + jnp.arange(64, dtype=jnp.int32)[None]).reshape(256)
    cos2, sin2 = rotary_lanes(rows)
    cos, sin = rotary_lanes(jnp.arange(1024, dtype=jnp.int32))
    xg, dg, docg, normed, act, dup, wc, w2g, heads, dsum, cst = gather_all(
        xb, dyb, docs, qkv_w, fc1_w, qb, fb, small, fc2_w, dense_w, cos2, sin2
    )
    slot_of = jnp.sum(jnp.where(slots[None, :] == jnp.arange(16, dtype=jnp.int32)[:, None], jnp.arange(16, dtype=jnp.int32)[None, :], 0), axis=1)
    att, sums = attention(slot_of, heads.reshape(4, 2, 4, 128, 256), docg, cos, sin)
    yo, o1, o2, eo, dbo = reduce_all(att.reshape(4, 1024, 256), normed, dg, xg, act, dup, wc, w2g, sums, dsum)
    out, dx, g_qkv_w, g_fc1_w, g_fc2_w, g_dense_w = finish_all(xb, dyb, yo, o1, o2, cst)
    eo = eo.reshape(8, 2048)
    sq, sf = stored_columns(eo[:, None, :1792])
    g_qkv_b = lax.dynamic_slice_in_dim(sq[0], index * 192, 192, 0)
    g_fc1_b = lax.dynamic_slice_in_dim(sf[0], index * 256, 256, 0)
    tiles = jnp.sum(eo[:, 1792:].reshape(8, 2, 2, 64), axis=0)
    both = lax.dynamic_slice_in_dim(tiles, z % 2, 1, 1)
    g_db = lax.dynamic_slice_in_dim(dbo[0], index * 64, 64, 0)
    return (out[None], dx[None], both[0, 0], both[1, 0], g_qkv_w, g_qkv_b, g_dense_w, g_db, g_fc1_w, g_fc1_b, g_fc2_w, g_db)


def solution(mesh):
    in_specs = (
        P("fsdp", "ctx", None),
        P("fsdp", "ctx", None),
        P("fsdp", None),
        P(),
        P(("ctx", "fsdp")),
        P(("ctx", "fsdp")),
        P(("ctx", "fsdp"), None),
        P(("ctx", "fsdp")),
        P(("ctx", "fsdp"), None),
        P(("ctx", "fsdp")),
        P(("ctx", "fsdp"), None),
        P(("ctx", "fsdp")),
        P(("ctx", "fsdp"), None),
        P(("ctx", "fsdp")),
    )
    out_specs = (
        P("fsdp", "ctx", None),
        P("fsdp", "ctx", None),
        P(("ctx", "fsdp")),
        P(("ctx", "fsdp")),
        P(("ctx", "fsdp"), None),
        P(("ctx", "fsdp")),
        P(("ctx", "fsdp"), None),
        P(("ctx", "fsdp")),
        P(("ctx", "fsdp"), None),
        P(("ctx", "fsdp")),
        P(("ctx", "fsdp"), None),
        P(("ctx", "fsdp")),
    )
    small = mesh.shape["ctx"] == 8 and mesh.shape["fsdp"] == 4
    return jax.shard_map(
        fast_device if small else per_device, mesh=mesh, in_specs=in_specs, out_specs=out_specs, check_vma=False
    )
```

```python
import math

import jax
import jax.numpy as jnp
from jax import lax
from jax.experimental import pallas as pl
from jax.experimental.pallas import tpu as pltpu
from jax.sharding import PartitionSpec as P

HEADS = 32
ROT = 32


EPS = 1e-05
GELU_C = math.sqrt(2.0 / math.pi)
NEG = -1e30


def shifted(block, axis, distance):
    devices = range(lax.axis_size(axis))
    route = [((i - distance) % len(devices), i) for i in devices]
    return lax.ppermute(block, axis, route)


def gelu_pair(upper):
    inner = GELU_C * (upper + 0.044715 * upper * upper * upper)
    tanh_val = jnp.tanh(inner)
    value = 0.5 * upper * (1.0 + tanh_val)
    slope = 0.5 * (1.0 + tanh_val) + 0.5 * upper * (1.0 - tanh_val * tanh_val) * GELU_C * (
        1.0 + 3.0 * 0.044715 * upper * upper
    )
    return (value, slope)


def rotary_tables(positions):
    half = ROT // 2
    freqs = jnp.exp(-(2.0 * jnp.arange(half, dtype=jnp.float32) / ROT) * math.log(10000.0))
    angles = positions.astype(jnp.float32)[:, None] * freqs[None, :]
    return (jnp.cos(angles)[:, None, :], jnp.sin(angles)[:, None, :])


def rotate(tensor, cosine, sine, sign):
    half = ROT // 2
    first = tensor[..., :half]
    second = tensor[..., half:ROT]
    new_first = first * cosine - sign * second * sine
    new_second = second * cosine + sign * first * sine
    return jnp.concatenate([new_first, new_second, tensor[..., ROT:]], axis=-1)


def contract_rows(left, right):
    return lax.dot_general(
        left, right, (((0,), (0,)), ((), ())), preferred_element_type=jnp.float32
    )


def contract_cols(left, right):
    return lax.dot_general(
        left, right, (((1,), (1,)), ((), ())), preferred_element_type=jnp.float32
    )


def own_columns(matrix, cycle_size, shard_count, member):
    count = matrix.shape[0]
    piece_width = matrix.shape[1] // (cycle_size * shard_count)
    parted = matrix.reshape(count, cycle_size, shard_count, piece_width)
    return lax.dynamic_slice_in_dim(parted, member, 1, 2).reshape(count, cycle_size * piece_width)


def per_device(
    block_input,
    output_grad,
    segment,
    slots,
    ln_gain,
    ln_bias,
    qkv_w,
    qkv_b,
    dense_w,
    dense_b,
    fc1_w,
    fc1_b,
    fc2_w,
    fc2_b,
):
    cycle_size = lax.axis_size("ctx")
    index = lax.axis_index("ctx")
    shard_count = lax.axis_size("fsdp")
    member = lax.axis_index("fsdp")
    tokens = block_input.shape[1]
    width = block_input.shape[2]
    stretch = tokens // 2
    heads = HEADS
    head_dim = width // heads
    scale = head_dim ** (-0.5)
    seg_row = segment[0]
    slot_ids = jnp.arange(2 * cycle_size, dtype=jnp.int32)

    def positions(start, count):
        rows = start + jnp.arange(count, dtype=jnp.int32)
        slot = rows // stretch
        owner = jnp.sum(jnp.where(slot[:, None] == slot_ids[None, :], slots[None, :], 0), axis=1)
        return owner * stretch + rows % stretch

    qpos = positions(index * tokens, tokens)
    qdoc = jnp.take(seg_row, qpos)
    cosine, sine = rotary_tables(qpos)
    gain_all, norm_bias_every, w_qkv, b_qkv, w_up, b_up = (
        lax.all_gather(ln_gain, ("ctx", "fsdp"), axis=0, tiled=True),
        lax.all_gather(ln_bias, ("ctx", "fsdp"), axis=0, tiled=True),
        lax.all_gather(qkv_w, ("ctx", "fsdp"), axis=0, tiled=True),
        lax.all_gather(qkv_b, ("ctx", "fsdp"), axis=0, tiled=True),
        lax.all_gather(fc1_w, ("ctx", "fsdp"), axis=0, tiled=True),
        lax.all_gather(fc1_b, ("ctx", "fsdp"), axis=0, tiled=True),
    )
    xf = block_input[0].astype(jnp.float32)
    row_mean = jnp.mean(xf, axis=-1, keepdims=True)
    centered_input = xf - row_mean
    inverse_deviation = lax.rsqrt(
        jnp.mean(centered_input * centered_input, axis=-1, keepdims=True) + EPS
    )
    standardized_input = centered_input * inverse_deviation
    gain_float = gain_all.astype(jnp.float32)
    normed_rows = (standardized_input * gain_float + norm_bias_every.astype(jnp.float32)).astype(
        jnp.bfloat16
    )
    proj = jnp.dot(normed_rows, w_qkv, preferred_element_type=jnp.float32) + b_qkv.astype(
        jnp.float32
    )
    query = rotate(proj[:, :width].reshape(tokens, heads, head_dim), cosine, sine, 1.0).astype(
        jnp.bfloat16
    )
    keys = rotate(
        proj[:, width : 2 * width].reshape(tokens, heads, head_dim), cosine, sine, 1.0
    ).astype(jnp.bfloat16)
    keys_flat = keys.reshape(tokens, width)
    values = proj[:, 2 * width :].astype(jnp.bfloat16)
    acc = jnp.zeros((tokens, heads, head_dim), jnp.float32)
    top = jnp.full((heads, tokens), NEG, jnp.float32)
    key_piece = lax.all_gather(keys_flat, "ctx", axis=0, tiled=True)
    value_piece = lax.all_gather(values, "ctx", axis=0, tiled=True)
    count = key_piece.shape[0]
    kpos = positions(jnp.int32(0), count)
    kdoc = jnp.take(seg_row, kpos)
    mask = ((kpos[None, :] <= qpos[:, None]) & (kdoc[None, :] == qdoc[:, None]))[None]
    scores = (
        jnp.einsum(
            "qhd,khd->hqk",
            query,
            key_piece.reshape(count, heads, head_dim),
            preferred_element_type=jnp.float32,
        )
        * scale
    )
    scores = jnp.where(mask, scores, NEG)
    new_top = jnp.maximum(top, jnp.max(scores, axis=-1))
    factor = jnp.exp(top - new_top)
    expo = jnp.where(mask, jnp.exp(scores - new_top[..., None]), 0.0)
    total = jnp.sum(expo, axis=-1)
    part_sum = jnp.einsum(
        "hqk,khd->qhd",
        expo.astype(jnp.bfloat16),
        value_piece.reshape(count, heads, head_dim),
        preferred_element_type=jnp.float32,
    )
    acc = acc * factor.T[:, :, None] + part_sum
    acc, top, total = (acc, new_top, total)
    attn_heads = (acc / total.T[:, :, None]).astype(jnp.bfloat16)
    lse = top + jnp.log(total)
    attn = attn_heads.reshape(tokens, width)
    w_dense, b_dense, w_down, b_down = (
        lax.all_gather(dense_w, ("ctx", "fsdp"), axis=0, tiled=True),
        lax.all_gather(dense_b, ("ctx", "fsdp"), axis=0, tiled=True),
        lax.all_gather(fc2_w, ("ctx", "fsdp"), axis=0, tiled=True),
        lax.all_gather(fc2_b, ("ctx", "fsdp"), axis=0, tiled=True),
    )
    upper = jnp.dot(normed_rows, w_up, preferred_element_type=jnp.float32) + b_up.astype(
        jnp.float32
    )
    act_f, slope = gelu_pair(upper)
    act = act_f.astype(jnp.bfloat16)
    y_rows = (
        xf
        + jnp.dot(attn, w_dense, preferred_element_type=jnp.float32)
        + b_dense.astype(jnp.float32)
    )
    y_rows = (
        y_rows
        + jnp.dot(act, w_down, preferred_element_type=jnp.float32)
        + b_down.astype(jnp.float32)
    )
    grad_rows = output_grad[0]
    gradient_float = grad_rows.astype(jnp.float32)
    group_attn, group_act, group_grad = (
        lax.all_gather(attn, "fsdp", axis=0, tiled=True),
        lax.all_gather(act, "fsdp", axis=0, tiled=True),
        lax.all_gather(grad_rows, "fsdp", axis=0, tiled=True),
    )
    group_bias = jnp.sum(group_grad.astype(jnp.float32), axis=0)
    own_bias = own_columns(group_bias[None], cycle_size, shard_count, member)[0]
    dense_part = contract_rows(own_columns(group_attn, cycle_size, shard_count, member), group_grad)
    down_part = contract_rows(own_columns(group_act, cycle_size, shard_count, member), group_grad)
    g_dense_w, g_dense_b, g_fc2_w, g_fc2_b = (
        lax.psum_scatter(
            dense_part.astype(jnp.bfloat16), "ctx", scatter_dimension=0, tiled=True
        ).astype(jnp.float32),
        lax.psum_scatter(
            own_bias.astype(jnp.bfloat16), "ctx", scatter_dimension=0, tiled=True
        ).astype(jnp.float32),
        lax.psum_scatter(
            down_part.astype(jnp.bfloat16), "ctx", scatter_dimension=0, tiled=True
        ).astype(jnp.float32),
        lax.psum_scatter(
            own_bias.astype(jnp.bfloat16), "ctx", scatter_dimension=0, tiled=True
        ).astype(jnp.float32),
    )
    dup = contract_cols(grad_rows, w_down) * slope
    up_bias_grad = jnp.sum(dup, axis=0)
    dup_b = dup.astype(jnp.bfloat16)
    dattn = contract_cols(grad_rows, w_dense).astype(jnp.bfloat16).reshape(tokens, heads, head_dim)
    delta = jnp.sum(dattn.astype(jnp.float32) * attn_heads.astype(jnp.float32), axis=-1).T

    def cycle_step(step, carry):
        key_cur, value_cur, dkey_acc, dvalue_acc, dquery_acc = carry
        anchor = (index - step + cycle_size) % cycle_size
        kpos = positions(anchor * tokens, tokens)
        kdoc = jnp.take(seg_row, kpos)
        mask = ((kpos[None, :] <= qpos[:, None]) & (kdoc[None, :] == qdoc[:, None]))[None]
        key_heads = key_cur.reshape(tokens, heads, head_dim)
        scores = (
            jnp.einsum("qhd,khd->hqk", query, key_heads, preferred_element_type=jnp.float32) * scale
        )
        probs = jnp.where(mask, jnp.exp(jnp.where(mask, scores, NEG) - lse[..., None]), 0.0)
        dvalue_acc = dvalue_acc + jnp.einsum(
            "hqk,qhd->khd", probs.astype(jnp.bfloat16), dattn, preferred_element_type=jnp.float32
        ).reshape(tokens, width)
        dprob = jnp.einsum(
            "qhd,khd->hqk",
            dattn,
            value_cur.reshape(tokens, heads, head_dim),
            preferred_element_type=jnp.float32,
        )
        dscore = (probs * (dprob - delta[..., None]) * scale).astype(jnp.bfloat16)
        dquery_acc = dquery_acc + jnp.einsum(
            "hqk,khd->qhd", dscore, key_heads, preferred_element_type=jnp.float32
        )
        dkey_acc = dkey_acc + jnp.einsum(
            "hqk,qhd->khd", dscore, query, preferred_element_type=jnp.float32
        ).reshape(tokens, width)
        key_cur, value_cur = shifted((key_cur, value_cur), "ctx", 1)
        dkey_acc, dvalue_acc = (
            shifted(dkey_acc.astype(jnp.bfloat16), "ctx", 1).astype(dkey_acc.dtype),
            shifted(dvalue_acc.astype(jnp.bfloat16), "ctx", 1).astype(dvalue_acc.dtype),
        )
        return (key_cur, value_cur, dkey_acc, dvalue_acc, dquery_acc)

    flat_zero = jnp.zeros((tokens, width), jnp.float32)
    cycle_init = (
        keys_flat,
        values,
        flat_zero,
        flat_zero,
        jnp.zeros((tokens, heads, head_dim), jnp.float32),
    )
    cycle_out = lax.fori_loop(0, cycle_size, cycle_step, cycle_init)
    dkey_sum, dvalue_sum, dquery_sum = (cycle_out[2], cycle_out[3], cycle_out[4])
    dquery = rotate(dquery_sum, cosine, sine, -1.0).reshape(tokens, width)
    dkey = rotate(dkey_sum.reshape(tokens, heads, head_dim), cosine, sine, -1.0).reshape(
        tokens, width
    )
    dproj = jnp.concatenate([dquery, dkey, dvalue_sum], axis=1)
    qkv_bias_grad = jnp.sum(dproj, axis=0)
    dproj_b = dproj.astype(jnp.bfloat16)
    normed_input_grad = contract_cols(dproj_b, w_qkv) + contract_cols(dup_b, w_up)
    gain_gradient = jnp.sum(normed_input_grad * standardized_input, axis=0)
    lnb_grad = jnp.sum(normed_input_grad, axis=0)
    scaled_rows = normed_input_grad * gain_float
    dx_rows = gradient_float + inverse_deviation * (
        scaled_rows
        - jnp.mean(scaled_rows, axis=-1, keepdims=True)
        - standardized_input * jnp.mean(scaled_rows * standardized_input, axis=-1, keepdims=True)
    )
    group_normed, group_dproj, group_dup = (
        lax.all_gather(normed_rows, "fsdp", axis=0, tiled=True),
        lax.all_gather(dproj_b, "fsdp", axis=0, tiled=True),
        lax.all_gather(dup_b, "fsdp", axis=0, tiled=True),
    )
    own_normed = own_columns(group_normed, cycle_size, shard_count, member)
    g_qkv_w, g_fc1_w = (
        lax.psum_scatter(
            contract_rows(own_normed, group_dproj).astype(jnp.bfloat16),
            "ctx",
            scatter_dimension=0,
            tiled=True,
        ).astype(jnp.float32),
        lax.psum_scatter(
            contract_rows(own_normed, group_dup).astype(jnp.bfloat16),
            "ctx",
            scatter_dimension=0,
            tiled=True,
        ).astype(jnp.float32),
    )
    layer_gain_grad, g_lnb, g_qkv_b, g_fc1_b = (
        lax.psum_scatter(gain_gradient, ("ctx", "fsdp"), scatter_dimension=0, tiled=True),
        lax.psum_scatter(lnb_grad, ("ctx", "fsdp"), scatter_dimension=0, tiled=True),
        lax.psum_scatter(qkv_bias_grad, ("ctx", "fsdp"), scatter_dimension=0, tiled=True),
        lax.psum_scatter(up_bias_grad, ("ctx", "fsdp"), scatter_dimension=0, tiled=True),
    )
    return (
        y_rows.astype(jnp.bfloat16)[None],
        dx_rows[None],
        layer_gain_grad,
        g_lnb,
        g_qkv_w,
        g_qkv_b,
        g_dense_w,
        g_dense_b,
        g_fc1_w,
        g_fc1_b,
        g_fc2_w,
        g_fc2_b,
    )


BF = jnp.bfloat16
F32 = jnp.float32
MESH = pl.DeviceIdType.MESH
HBM = pl.BlockSpec(memory_space=pl.ANY)
VM = pl.BlockSpec(memory_space=pltpu.VMEM)
DMA = pltpu.SemaphoreType.DMA
VLIM = 60 * 1024 * 1024


def place():
    ctx, z = lax.axis_index("ctx"), lax.axis_index("fsdp")
    return ctx, lax.div(ctx, 4), lax.rem(lax.div(ctx, 2), 2), lax.rem(ctx, 2), z


class Net:
    def __init__(self):
        self.ctx, self.y, self.x, self.c, self.z = place()
        self.yb, self.xb, self.cb = 1 - self.y, 1 - self.x, 1 - self.c
        self.m = self.y * 4 + self.z
        self.g = self.x * 2 + self.c
        self.to_y = {"ctx": self.ctx + 4 * (1 - 2 * self.y), "fsdp": self.z}
        self.to_x = {"ctx": self.ctx + 2 * (1 - 2 * self.x), "fsdp": self.z}
        self.to_c = {"ctx": self.ctx + 1 - 2 * self.c, "fsdp": self.z}
        self.up = {"ctx": self.ctx, "fsdp": self.z + 1}
        self.dn = {"ctx": self.ctx, "fsdp": self.z - 1}
        self.sent = []

    def member(self, q):
        flip, step = q // 4, q % 4
        z = lax.rem(self.z + step, 4)
        yy = self.yb if flip else self.y
        return {"ctx": self.ctx + flip * 4 * (1 - 2 * self.y), "fsdp": z}, yy, z

    def source(self, q):
        flip, step = q // 4, q % 4
        return (self.yb if flip else self.y), lax.rem(self.z + 4 - step, 4)

    def barrier(self, more=()):
        sem = pltpu.get_barrier_semaphore()
        peers = [self.member(q)[0] for q in range(1, 8)] + [self.to_x, self.to_c, *more]
        for peer in peers:
            pl.semaphore_signal(sem, inc=1, device_id=peer, device_id_type=MESH)
        pl.semaphore_wait(sem, len(peers))

    def go(self, copy, when=None):
        if when is None:
            copy.start()
        else:
            pl.when(when)(copy.start)
        self.sent.append((copy, when))

    def drain(self):
        for copy, when in self.sent:
            if when is None:
                copy.wait_send()
            else:
                pl.when(when)(copy.wait_send)


def remote(src, dst, send, recv, to):
    return pltpu.make_async_remote_copy(
        src_ref=src, dst_ref=dst, send_sem=send, recv_sem=recv, device_id=to, device_id_type=MESH
    )


def arrive(like, recv):
    pltpu.make_async_copy(like, like, recv).wait()


def head_tiles(src, dst, rows):
    qkv, ff = src
    low = lanes_of((rows, 128)) < 64

    def tile(base, h):
        t = 128 * (h // 2)
        return qkv[:, base + t : base + t + 128].astype(F32)

    def join(a, b, odd):
        if odd:
            return jnp.where(low, pltpu.roll(a, 64, 1), b).astype(BF)
        return jnp.where(low, a, pltpu.roll(b, 64, 1)).astype(BF)

    for mm in range(8):
        first = (mm // 4) * 16 + mm % 4
        odd = first % 2
        for g in range(4):
            h = first + 4 * g
            dst(mm, 128 * g, join(tile(0, h), tile(2048, h), odd))
            dst(mm, 768 + 256 * g, ff[:, 256 * h : 256 * h + 256])
        for k in range(2):
            h = first + 8 * k
            dst(mm, 512 + 128 * k, join(tile(4096, h), tile(4096, h + 4), odd))


def gather_kernel(x, dy, docs, qkv, ff, qb, fb, small, fc2, dense, cos, sin,
                  xg, dg, docg, normed_o, act_o, dup_o, wc_o, w2_o, heads, dsum, cst,
                  xv, dv, wc, w2g, eg, ws, es, nrm, act, dup, hs,
                  loc, us, ur, ds_, dr, ys, yr, as_, ar, es_, er,
                  wxs, wxr, wks, wkr, exs, exr, eks, ekr, fxs, fxr, fks, fkr, hss, hsr, hl, wb):
    n = Net()
    far = {"ctx": n.ctx + 2 * (1 - 2 * n.x) + 1 - 2 * n.c, "fsdp": n.z}
    n.barrier(more=(far,))

    def wrow(yy, xx, cc, zz):
        return wc.at[pl.ds(pl.multiple_of((yy * 16 + xx * 8 + cc * 4 + zz) * 64, 64), 64)]

    def wide(gg):
        return w2g.at[pl.ds(pl.multiple_of(gg * 256, 256), 256)]

    def thin(gg):
        return w2g.at[pl.ds(pl.multiple_of(1024 + gg * 64, 64), 64)]

    def shard(yy, zz, p):
        mm = yy * 4 + zz
        if p == 2:
            return docg.at[mm]
        return (xv, dv)[p].at[pl.ds(pl.multiple_of(mm * 128, 128), 128)]

    mine = (x, dy, docs)
    parts = (0, 1, 2)

    def tokens(p):
        n.go(remote(mine[p], shard(n.y, n.z, p), us.at[p, 0], ur.at[p, 0], n.up), n.z < 3)
        n.go(remote(mine[p], shard(n.y, n.z, p), ds_.at[p, 0], dr.at[p, 0], n.dn), n.z > 0)
        n.go(remote(mine[p], shard(n.y, n.z, p), ys.at[p, 0], yr.at[p, n.z], n.to_y))

    tokens(0)
    rows2 = ((fc2, wide), (dense, thin))
    for k, (ref, part) in enumerate(rows2):
        n.go(remote(ref, part(n.g), fxs.at[k], fxr.at[k], n.to_x))
        n.go(remote(ref, part(n.g), fks.at[k], fkr.at[k], n.to_c))

    def put_w(mm, col, value):
        ws[mm, :, col : col + value.shape[1]] = value

    def put_e(mm, col, value):
        es[mm, 0:1, col : col + value.shape[1]] = value[0:1]

    for mm in range(8):
        es[mm] = small[...]
    head_tiles((qkv, ff), put_w, 64)
    head_tiles((qb, fb), put_e, 8)
    for q in (4, 1, 3, 5, 7, 2, 6):
        to, yy, zz = n.member(q)
        n.go(remote(es.at[yy * 4 + zz], eg.at[n.g * 8 + n.m], es_.at[q], er.at[q], to))
        n.go(remote(ws.at[yy * 4 + zz], wrow(n.y, n.x, n.c, n.z), as_.at[q], ar.at[q], to))
    own = ws.at[n.m]
    n.go(remote(own, wrow(n.y, n.x, n.c, n.z), wxs.at[0], wxr.at[0], n.to_x))
    n.go(remote(own, wrow(n.y, n.x, n.c, n.z), wks.at[0], wkr.at[0], n.to_c))
    tokens(1)
    tokens(2)
    local = [
        pltpu.make_async_copy(x, shard(n.y, n.z, 0), loc.at[0]),
        pltpu.make_async_copy(dy, shard(n.y, n.z, 1), loc.at[1]),
        pltpu.make_async_copy(docs, shard(n.y, n.z, 2), loc.at[2]),
        pltpu.make_async_copy(own, wrow(n.y, n.x, n.c, n.z), loc.at[3]),
        pltpu.make_async_copy(es.at[n.m], eg.at[n.g * 8 + n.m], loc.at[4]),
        pltpu.make_async_copy(fc2, wide(n.g), loc.at[5]),
        pltpu.make_async_copy(dense, thin(n.g), loc.at[6]),
    ]
    for copy in local:
        copy.start()

    def line(d, ps):
        below, above = n.z >= d, n.z + d <= 3
        for p in ps:
            for there, zz, recv, send, nxt, more, to in (
                (below, n.z - d, ur, us, ur, n.z < 3, n.up),
                (above, n.z + d, dr, ds_, dr, n.z > 0, n.dn),
            ):
                block = shard(n.y, zz, p)

                @pl.when(there)
                def _():
                    arrive(block, recv.at[p, d - 1])

                if d < 3:
                    n.go(remote(block, block, send.at[p, d], nxt.at[p, d], to), there & more)
                slot = d if to is n.up else d + 3
                n.go(remote(block, block, ys.at[p, slot], yr.at[p, zz], n.to_y), there)

    def pieces(qs):
        for q in qs:
            yy, zz = n.source(q)
            block = wrow(yy, n.x, n.c, zz)
            arrive(block, ar.at[q])
            n.go(remote(block, block, wxs.at[q], wxr.at[q], n.to_x))
            n.go(remote(block, block, wks.at[q], wkr.at[q], n.to_c))

    def relay(qs):
        for q in qs:
            yy, zz = n.source(q)
            block = wrow(yy, n.xb, n.c, zz)
            arrive(block, wxr.at[q])
            n.go(remote(block, block, wks.at[8 + q], wkr.at[8 + q], n.to_c))

    line(1, (0,))
    pieces((4, 1, 3))
    line(1, (1, 2))
    pieces((5, 7, 2, 6))
    for q in range(1, 8):
        yy, zz = n.source(q)
        arrive(eg.at[n.g * 8 + yy * 4 + zz], er.at[q])
    local[4].wait()
    these = eg.at[pl.ds(n.g * 8, 8)]
    n.go(remote(these, these, exs.at[0], exr.at[0], n.to_x))
    n.go(remote(these, these, eks.at[0], ekr.at[0], n.to_c))
    line(2, parts)
    gx = n.xb * 2 + n.c
    for k, (ref, part) in enumerate(rows2):
        arrive(part(gx), fxr.at[k])
        n.go(remote(part(gx), part(gx), fks.at[2 + k], fkr.at[2 + k], n.to_c))
    theirs = eg.at[pl.ds(gx * 8, 8)]
    relay((0, 4, 1, 3, 5, 7, 2, 6))
    arrive(theirs, exr.at[0])
    n.go(remote(theirs, theirs, eks.at[1], ekr.at[1], n.to_c))
    for q in range(8):
        yy, zz = n.source(q)
        arrive(wrow(yy, n.x, n.cb, zz), wkr.at[q])
        arrive(wrow(yy, n.xb, n.cb, zz), wkr.at[8 + q])
    for k in range(2):
        gg = 2 * (n.xb if k else n.x) + n.cb
        arrive(eg.at[pl.ds(gg * 8, 8)], ekr.at[k])
        for j, (ref, part) in enumerate(rows2):
            arrive(part(gg), fkr.at[2 * k + j])
    for k in (0, 1, 2, 3, 5, 6):
        local[k].wait()
    out_w = [pltpu.make_async_copy(wc, wc_o, wb.at[0]), pltpu.make_async_copy(w2g, w2_o, wb.at[1])]
    for copy in out_w:
        copy.start()

    def add_ext(i, t):
        return t + eg[i].astype(F32)

    ext = lax.fori_loop(0, 32, add_ext, jnp.zeros((8, 1792), F32))
    cst[0:1, 0:1792], cst[0:1, 1792:2048] = ext[1:2], ext[5:6, 0:256]
    cst[1:2, 0:1792], cst[1:2, 1792:2048] = ext[2:3], ext[5:6, 256:512]
    cst[2:3, 0:1792], cst[2:3, 1792:2048] = ext[3:4] + ext[4:5], ext[5:6, 512:768] + ext[5:6, 768:1024]
    cst[3:4, 0:1792], cst[3:4, 1792:2048] = ext[0:1], jnp.zeros((1, 256), F32)
    cst[4:8, :] = jnp.zeros((4, 2048), F32)
    dsum[...] = jnp.zeros_like(dsum)
    z0 = lax.div(n.z, 2)
    half = lanes_of((256, 128)) < 64

    def rows_of(j):
        yy = n.y + lax.rem(j, 2) * (1 - 2 * n.y)
        zp = z0 + lax.div(j, 2) * (1 - 2 * z0)
        return yy, zp, pl.ds(pl.multiple_of((yy * 4 + 2 * zp) * 128, 256), 256)

    def sends(j):
        yy, zp, rows = rows_of(j)
        return [
            remote(hs.at[gg, rows], heads.at[n.g, rows], hss.at[j, k], hsr.at[j, k], to)
            for k, (to, gg) in enumerate(((far, 2 * n.xb + n.cb), (n.to_x, 2 * n.xb + n.c), (n.to_c, 2 * n.x + n.cb)))
        ]

    def keeps(j):
        yy, zp, rows = rows_of(j)
        return [
            pltpu.make_async_copy(hs.at[n.g, rows], heads.at[n.g, rows], hl.at[j, 0]),
            pltpu.make_async_copy(nrm.at[rows], normed_o.at[rows], hl.at[j, 1]),
            pltpu.make_async_copy(act.at[rows], act_o.at[rows], hl.at[j, 2]),
            pltpu.make_async_copy(dup.at[rows], dup_o.at[rows], hl.at[j, 3]),
            pltpu.make_async_copy(xv.at[rows], xg.at[rows], hl.at[j, 4]),
            pltpu.make_async_copy(dv.at[rows], dg.at[rows], hl.at[j, 5]),
        ]

    def pair(j, carry):
        yy, zp, rows = rows_of(j)
        base = (yy * 4 + 2 * zp) * 128

        @pl.when(lax.rem(j, 2) == 1)
        def _():
            for k in range(2):
                for p in parts:
                    arrive(shard(yy, 2 * zp + k, p), yr.at[p, 2 * zp + k])

        def norm(i, c):
            sl = pl.ds(pl.multiple_of(base + 32 * i, 32), 32)
            xf = xv[sl, :].astype(F32)
            cen = xf - jnp.mean(xf, axis=-1, keepdims=True)
            rstd = lax.rsqrt(jnp.mean(cen * cen, axis=-1, keepdims=True) + EPS)
            nrm[sl, :] = (cen * rstd * cst[0:1, :] + cst[1:2, :]).astype(BF)
            return c

        lax.fori_loop(0, 8, norm, 0)
        table = pl.ds(pl.multiple_of(yy * 128, 128), 128)
        cosv = jnp.concatenate([cos[table, :]] * 2, axis=0)
        sinv = jnp.concatenate([sin[table, :]] * 2, axis=0)
        for k in range(2):
            t2 = jnp.dot(nrm[rows, :], wc[:, 256 * k : 256 * k + 256], preferred_element_type=F32)
            t2 = t2 + cst[3:4, 256 * k : 256 * k + 256]
            for i in range(2):
                t = t2[:, 128 * i : 128 * i + 128]
                hs[2 * k + i, rows, 0:128] = (t * cosv + partner(t) * sinv).astype(BF)
        v4 = jnp.dot(nrm[rows, :], wc[:, 512:768], preferred_element_type=F32) + cst[3:4, 512:768]
        d4 = dot_nt(dv[rows, :], w2g[1024:1280, :])
        for g in range(4):
            v, d = (t[:, 128 * (g // 2) : 128 * (g // 2) + 128] for t in (v4, d4))
            if g % 2 == 0:
                vd = jnp.where(half, v, pltpu.roll(d, 64, 1))
            else:
                vd = jnp.where(half, pltpu.roll(v, 64, 1), d)
            hs[g, rows, 128:256] = vd.astype(BF)
        for copy in sends(j):
            copy.start()
        for k in range(4):
            cols, wcols = slice(256 * k, 256 * k + 256), slice(768 + 256 * k, 1024 + 256 * k)
            up = jnp.dot(nrm[rows, :], wc[:, wcols], preferred_element_type=F32) + cst[3:4, wcols]
            a, slope = gelu_pair(up)
            act[rows, cols] = a.astype(BF)
            du = dot_nt(dv[rows, :], w2g[cols, :]) * slope
            dup[rows, cols] = du.astype(BF)
            dsum[:, cols] += jnp.broadcast_to(jnp.sum(du, axis=0, keepdims=True), (8, 256))
        for copy in keeps(j):
            copy.start()
        return carry

    lax.fori_loop(0, 2, pair, 0)
    line(3, parts)
    lax.fori_loop(2, 4, pair, 0)
    for j in range(4):
        for copy in sends(j):
            copy.wait()
        for copy in keeps(j):
            copy.wait()
    for copy in out_w:
        copy.wait()
    n.drain()


def gather_all(x, dy, docs, qkv, ff, qb, fb, small, fc2, dense, cos, sin):
    sd = jax.ShapeDtypeStruct
    V = pltpu.VMEM
    return pl.pallas_call(
        gather_kernel,
        name="gather_all",
        out_shape=(sd((1024, 2048), BF), sd((1024, 2048), BF), sd((8, 8, 1024), BF), sd((1024, 2048), BF),
                   sd((1024, 1024), BF), sd((1024, 1024), BF), sd((2048, 1792), BF), sd((1280, 2048), BF),
                   sd((4, 1024, 256), BF), sd((8, 1024), F32), sd((8, 2048), F32)),
        in_specs=[VM] * 12,
        out_specs=(HBM, HBM, VM, HBM, HBM, HBM, HBM, HBM, HBM, VM, VM),
        scratch_shapes=[V((1024, 2048), BF), V((1024, 2048), BF), V((2048, 1792), BF), V((1280, 2048), BF),
                        V((32, 8, 1792), BF), V((8, 64, 1792), BF), V((8, 8, 1792), BF),
                        V((1024, 2048), BF), V((1024, 1024), BF), V((1024, 1024), BF), V((4, 1024, 256), BF),
                        DMA((7,)), DMA((3, 3)), DMA((3, 3)), DMA((3, 3)), DMA((3, 3)), DMA((3, 7)), DMA((3, 4)),
                        DMA((8,)), DMA((8,)), DMA((8,)), DMA((8,)), DMA((8,)), DMA((8,)), DMA((16,)), DMA((16,)),
                        DMA((1,)), DMA((1,)), DMA((2,)), DMA((2,)), DMA((2,)), DMA((2,)), DMA((4,)), DMA((4,)),
                        DMA((4, 3)), DMA((4, 3)), DMA((4, 6)), DMA((2,))],
        compiler_params=pltpu.CompilerParams(collective_id=1, has_side_effects=True, vmem_limit_bytes=VLIM),
    )(x, dy, docs, qkv, ff, qb, fb, small, fc2, dense, cos, sin)


def lanes_of(shape):
    return lax.broadcasted_iota(jnp.int32, shape, len(shape) - 1)


def partner(t):
    low = lax.rem(lanes_of(t.shape), 64) < 16
    return jnp.where(low, pltpu.roll(t, 112, 1), pltpu.roll(t, 16, 1))


def dot_nt(a, b):
    return lax.dot_general(a, b, (((1,), (1,)), ((), ())), preferred_element_type=F32)


def dot_tn(a, b):
    return lax.dot_general(a, b, (((0,), (0,)), ((), ())), preferred_element_type=F32)


def attention_kernel(slot_of, a, docs, cos, sin, out, sums, seq, att, dq, dk, dv):
    def where_is(p):
        r = slot_of[p]
        ctx = lax.div(r, 2)
        return lax.rem(ctx, 4), lax.div(ctx, 4), pl.ds(pl.multiple_of(lax.rem(r, 2) * 64, 64), 64)

    for p in range(16):
        g, yy, rows = where_is(p)
        seq[64 * p : 64 * p + 64, :] = a[g, yy, 0, rows, :]
    dk[...] = jnp.zeros_like(dk)
    dv[...] = jnp.zeros_like(dv)
    scale = 0.125
    low = lanes_of((256, 128)) < 64
    for i in range(4):
        k0 = max(0, i - 2) * 256
        kn = 256 * (i + 1) - k0
        rq, rk = slice(256 * i, 256 * i + 256), slice(k0, k0 + kn)
        qk, vd = seq[rq, 0:128], seq[rq, 128:256]
        kk, vv = seq[rk, 0:128], seq[rk, 128:256]
        zero = jnp.zeros((256, 128), F32)
        qs = jnp.where(low, zero, pltpu.roll(qk.astype(F32), 64, 1)).astype(BF)
        dsf = jnp.where(low, pltpu.roll(vd.astype(F32), 64, 1), zero)
        s = dot_nt(qs, kk) * scale
        qpos = 256 * i + lax.broadcasted_iota(jnp.int32, (256, kn), 0)
        kpos = k0 + lax.broadcasted_iota(jnp.int32, (256, kn), 1)
        own = jnp.broadcast_to(docs[0, 0:1, rq].astype(F32), (128, 256)).T[:, 0:1]
        mask = (kpos <= qpos) & (docs[0, 0:1, rk].astype(F32) == own)
        s = jnp.where(mask, s, NEG)
        top = jnp.max(s, axis=-1, keepdims=True)
        e = jnp.where(mask, jnp.exp(s - top), 0.0)
        inv = 1.0 / jnp.sum(e, axis=-1, keepdims=True)
        o = jnp.dot(e.astype(BF), vv, preferred_element_type=F32) * inv
        ob = o.astype(BF)
        att[rq, :] = ob.astype(F32)
        delta = jnp.sum(dsf * ob.astype(F32), axis=-1, keepdims=True)
        pr = e * inv
        dv[rk, :] += dot_tn(pr.astype(BF), vd)
        dp = dot_nt(dsf.astype(BF), vv)
        ds = (pr * (dp - delta) * scale).astype(BF)
        dq[rq, :] = jnp.dot(ds, kk, preferred_element_type=F32)
        dk[rk, :] += dot_tn(ds, qk)
    tot = jnp.zeros((8, 256), F32)
    half = lanes_of((64, 128)) < 64
    s1 = jnp.zeros((1, 128), F32)
    s2 = jnp.zeros((1, 128), F32)
    for p in range(16):
        rows = slice(64 * p, 64 * p + 64)
        g, yy, place_rows = where_is(p)
        t = jnp.where(half, pltpu.roll(dq[rows, :], 64, 1), pltpu.roll(dk[rows, :], 64, 1))
        t = t * cos[rows, :] - partner(t) * sin[rows, :]
        u = jnp.where(half, pltpu.roll(dv[rows, :], 64, 1), pltpu.roll(att[rows, :], 64, 1))
        s1 += jnp.sum(t, axis=0, keepdims=True)
        s2 += jnp.sum(u, axis=0, keepdims=True)
        out[g, yy, 0, place_rows, 0:128] = t.astype(BF)
        out[g, yy, 0, place_rows, 128:256] = u.astype(BF)
    sums[0, :, 0:128] = jnp.broadcast_to(s1, (8, 128))
    sums[0, :, 128:256] = jnp.broadcast_to(s2, (8, 128))


def attention(slot_of, a, docs, cos, sin):
    sd = jax.ShapeDtypeStruct
    blk = pl.BlockSpec((4, 2, 1, 128, 256), lambda s, t: (0, 0, s, 0, 0))
    return pl.pallas_call(
        attention_kernel,
        name="attention",
        grid_spec=pltpu.PrefetchScalarGridSpec(
            num_scalar_prefetch=1,
            grid=(4,),
            in_specs=[
                blk,
                pl.BlockSpec((1, 8, 1024), lambda s, t: (s, 0, 0)),
                pl.BlockSpec((1024, 128), lambda s, t: (0, 0)),
                pl.BlockSpec((1024, 128), lambda s, t: (0, 0)),
            ],
            out_specs=(blk, pl.BlockSpec((1, 8, 256), lambda s, t: (s, 0, 0))),
            scratch_shapes=[pltpu.VMEM((1024, 256), BF)] + [pltpu.VMEM((1024, 128), F32)] * 4,
        ),
        out_shape=(sd((4, 2, 4, 128, 256), BF), sd((4, 8, 256), F32)),
        compiler_params=pltpu.CompilerParams(vmem_limit_bytes=VLIM),
    )(slot_of, a, docs, cos, sin)


def add_rows(dst, srcs, rows, out=None, step=16):
    out = dst if out is None else out

    def body(i, carry):
        sl = pl.ds(pl.multiple_of(i * step, step), step)
        v = dst[sl, :].astype(F32)
        for s in srcs:
            v = v + s[sl, :].astype(F32)
        out[sl, :] = v.astype(out.dtype)
        return carry

    lax.fori_loop(0, rows // step, body, 0)


def reduce_kernel(att, normed_i, dy_i, x_i, act_i, dup_i, wc_i, w2_i, sums, dsum,
                  yo, o1, o2, eo, dbo,
                  nrm, dy, wc, w2, dpr, up2, rec, ysend, yr, ud, own, r1, st1, r2, s1, st2, s2, thin2, flip, xst, mu, rs, acc, ev, t1, t2, d1,
                  hss, hsr, hl, ld, xl, yss, yrs, uss, urs, k1s, k1r, x1s, x1r, a1s, a1r,
                  k2s, k2r, x2s, x2r, eks, ekr, exs, exr, eas, ear, dbs, dbr, fl):
    n = Net()
    far = {"ctx": n.ctx + 2 * (1 - 2 * n.x) + 1 - 2 * n.c, "fsdp": n.z}
    n.barrier(more=(far,))
    z0 = lax.div(n.z, 2)
    zf = 1 - z0

    def halves(k):
        yy = n.y if k % 2 else n.yb
        tile = 0 if k >= 2 else 1
        return pl.ds(pl.multiple_of(yy * 512, 512), 512), pl.ds(128 * tile, 128)

    for k in range(4):
        rows, lanes = halves(k)
        for i, (to, gg) in enumerate(((far, 2 * n.xb + n.cb), (n.to_x, 2 * n.xb + n.c), (n.to_c, 2 * n.x + n.cb))):
            n.go(remote(att.at[gg, rows, lanes], rec.at[n.g, rows, lanes], hss.at[k, i], hsr.at[k, i], to))
    keep = pltpu.make_async_copy(att.at[n.g], rec.at[n.g], hl.at[0])
    loads = [
        pltpu.make_async_copy(dy_i, dy, ld.at[0]),
        pltpu.make_async_copy(act_i, up2.at[:, pl.ds(0, 1024)], ld.at[1]),
        pltpu.make_async_copy(w2_i, w2, ld.at[2]),
        pltpu.make_async_copy(dup_i, dpr.at[:, pl.ds(768, 1024)], ld.at[3]),
        pltpu.make_async_copy(normed_i, nrm, ld.at[4]),
        pltpu.make_async_copy(wc_i, wc, ld.at[5]),
    ]
    for copy in loads[:2] + [keep] + loads[2:]:
        copy.start()

    def heads_in(k):
        rows, lanes = halves(k)
        for i, gg in enumerate((2 * n.xb + n.cb, 2 * n.xb + n.c, 2 * n.x + n.cb)):
            arrive(rec.at[gg, rows, lanes], hsr.at[k, i])

    low = lanes_of((64, 128)) < 64

    def split(k):
        yy = n.y if k % 2 else n.yb

        def body(i, carry):
            sl = pl.ds(pl.multiple_of(yy * 512 + 64 * i, 64), 64)
            for p in range(2):
                a, b = rec[2 * p, sl, 128:256].astype(F32), rec[2 * p + 1, sl, 128:256].astype(F32)
                up2[sl, 1024 + 128 * p : 1152 + 128 * p] = jnp.where(low, pltpu.roll(a, 64, 1), b).astype(BF)
                dpr[sl, 512 + 128 * p : 640 + 128 * p] = jnp.where(low, a, pltpu.roll(b, 64, 1)).astype(BF)
            return carry

        lax.fori_loop(0, 8, body, 0)

    def pair_rows(yy, zp):
        return pl.ds(pl.multiple_of((yy * 4 + 2 * zp) * 128, 256), 256)

    def into(dst, zp, cols, value):
        dst(2 * zp)[:, cols] = value[0:128].astype(BF)
        dst(2 * zp + 1)[:, cols] = value[128:256].astype(BF)

    def chunks(count, width, body):
        def step(i, carry):
            body(pl.ds(pl.multiple_of(i * width, width), width))
            return carry

        lax.fori_loop(0, count, step, 0)

    def y_pair(yy, zp, dst):
        rows = pair_rows(yy, zp)

        def body(cols):
            into(dst, zp, cols, jnp.dot(up2[rows, :], w2[:, cols], preferred_element_type=F32))

        chunks(4, 512, body)

    def dn_pair(yy, zp, dst):
        rows = pair_rows(yy, zp)
        load = pltpu.make_async_copy(x_i.at[rows], xst, xl.at[0])
        load.start()
        load.wait()

        def stats(i, carry):
            sl = pl.ds(pl.multiple_of(32 * i, 32), 32)
            xf = xst[sl, :].astype(F32)
            mean = jnp.mean(xf, axis=-1, keepdims=True)
            cen = xf - mean
            mu[sl, :] = jnp.broadcast_to(mean, (32, 128))
            rs[sl, :] = jnp.broadcast_to(lax.rsqrt(jnp.mean(cen * cen, axis=-1, keepdims=True) + EPS), (32, 128))
            return carry

        lax.fori_loop(0, 8, stats, 0)

        def body(cols):
            d = dot_nt(dpr[rows, :], wc[cols, :])
            xh = (xst[:, cols].astype(F32) - mu[:, 0:1]) * rs[:, 0:1]
            acc[0:1, cols] += jnp.sum(d * xh, axis=0, keepdims=True)
            acc[1:2, cols] += jnp.sum(d, axis=0, keepdims=True)
            into(dst, zp, cols, d)

        chunks(8, 256, body)

    def send_y(t, buf, k, j):
        n.go(remote(buf, yr.at[k, t], yss.at[t, j], yrs.at[t, k], n.to_y))

    def w1_rows(yy, xx, cc):
        return pl.ds(pl.multiple_of((yy * 16 + xx * 8 + cc * 4) * 64, 256), 256)

    def w1_part(yy, xx, cc, write):
        flip[...] = nrm[:, w1_rows(yy, xx, cc)].T
        chunks(7, 256, lambda cols: write(cols, jnp.dot(flip[...], dpr[:, cols], preferred_element_type=F32)))

    def w2_part(gg, write):
        flip[...] = up2[:, pl.ds(pl.multiple_of(gg * 256, 256), 256)].T
        chunks(4, 512, lambda cols: write(cols, jnp.dot(flip[...], dy[:, cols], preferred_element_type=F32)))

    wide, thin = pl.ds(0, 256), pl.ds(256, 64)
    acc[...] = jnp.zeros_like(acc)

    loads[0].wait()
    loads[1].wait()

    def other_wide(xx, carry):
        def write(cols, value):
            st2[xx, 0:256, cols] = value.astype(BF)

        w2_part(2 * xx + n.cb, write)
        return carry

    lax.fori_loop(0, 2, other_wide, 0)
    for xx in range(2):
        n.go(remote(st2.at[xx, wide], s1.at[xx, wide], k2s.at[xx, 0], k2r.at[xx, 0], n.to_c))
    loads[2].wait()
    keep.wait()
    heads_in(0)
    split(0)
    zn = n.z + 1 - 2 * lax.rem(n.z, 2)
    y_pair(n.yb, zf, lambda k: ysend.at[k])
    send_y(0, ysend.at[3 * zf], 3 * zf, 0)
    send_y(0, ysend.at[1 + zf], 1 + zf, 1)
    y_pair(n.yb, z0, lambda k: ysend.at[k])
    send_y(0, ysend.at[zn], zn, 2)
    send_y(0, ysend.at[n.z], n.z, 3)
    heads_in(1)
    split(1)

    def own_y(i, carry):
        y_pair(n.y, i, lambda k: own.at[k, 0])
        return carry

    lax.fori_loop(0, 2, own_y, 0)
    flip[...] = up2[:, 1024:1280].T

    def thin_part(cols):
        four = jnp.dot(flip[...], dy[:, cols], preferred_element_type=F32)
        for xx in range(2):
            a, b = four[128 * xx : 128 * xx + 64], four[128 * xx + 64 : 128 * xx + 128]
            st2[xx, 256:320, cols] = jnp.where(n.c == 0, b, a).astype(BF)
            thin2[64 * xx : 64 * xx + 64, cols] = jnp.where(n.c == 0, a, b).astype(BF)

    chunks(4, 512, thin_part)
    for xx in range(2):
        n.go(remote(st2.at[xx, thin], s1.at[xx, thin], k2s.at[xx, 1], k2r.at[xx, 1], n.to_c))

    def w2_own(xx):
        arrive(s1.at[xx, wide], k2r.at[xx, 0])

        def write(cols, value):
            s1[xx, 0:256, cols] = (s1[xx, 0:256, cols].astype(F32) + value).astype(BF)

        w2_part(2 * xx + n.c, write)
        arrive(s1.at[xx, thin], k2r.at[xx, 1])
        mine = pl.ds(pl.multiple_of(64 * xx, 64), 64)
        s1[xx, 256:320, :] = (s1[xx, 256:320, :].astype(F32) + thin2[mine, :].astype(F32)).astype(BF)

    w2_own(n.xb)
    w2_own(n.x)
    outer = (n.z == 0) | (n.z == 3)
    inner = (n.z == 1) | (n.z == 2)

    def forward(t, j, who):
        k = (3 * zf, 1 + zf, zn)[j]
        up = jnp.where(k > n.z, 1, 0)
        slot = k + up
        block = own.at[k, t]

        @pl.when(who)
        def _():
            arrive(yr.at[k, t], yrs.at[t, k])
            if who is inner:
                arrive(ud.at[slot, t], urs.at[t, slot])
                add_rows(block, [yr.at[k, t], ud.at[slot, t]], 128)
            else:
                add_rows(block, [yr.at[k, t]], 128)

        to = {"ctx": n.ctx, "fsdp": n.z + 2 * up - 1}
        n.go(remote(block, ud.at[slot, t], uss.at[t, j], urs.at[t, slot], to), who)

    forward(0, 0, outer)
    heads_in(2)
    heads_in(3)

    def whole(i, carry):
        sl = pl.ds(pl.multiple_of(64 * i, 64), 64)
        for g in range(4):
            dpr[sl, 128 * g : 128 * g + 128] = rec[g, sl, 0:128]
        return carry

    lax.fori_loop(0, 16, whole, 0)
    loads[3].wait()
    loads[4].wait()

    def staged(k):
        xx = n.xb + (k // 2) * (1 - 2 * n.xb) if isinstance(k, int) else n.xb + lax.div(k, 2) * (1 - 2 * n.xb)
        yy = n.yb + (k % 2) * (1 - 2 * n.yb) if isinstance(k, int) else n.yb + lax.rem(k, 2) * (1 - 2 * n.yb)
        slot = k % 2 if isinstance(k, int) else lax.rem(k, 2)
        return yy, xx, remote(st1.at[slot], r1.at[yy * 2 + xx], k1s.at[k], k1r.at[yy * 2 + xx], n.to_c), slot

    def other_rows(k, carry):
        yy, xx, copy, slot = staged(k)

        @pl.when(k >= 2)
        def _():
            staged(k - 2)[2].wait_send()

        def write(cols, value):
            st1[slot, :, cols] = value.astype(BF)

        w1_part(yy, xx, n.cb, write)
        copy.start()
        return carry

    lax.fori_loop(0, 2, other_rows, 0)

    def w1_own(yy, xx):
        block = r1.at[yy * 2 + xx]
        arrive(block, k1r.at[yy * 2 + xx])

        def write(cols, value):
            block[:, cols] = (block[:, cols].astype(F32) + value).astype(BF)

        w1_part(yy, xx, n.c, write)

    def finish(t):
        k = n.z
        arrive(yr.at[k, t], yrs.at[t, k])

        @pl.when(n.z > 0)
        def _():
            arrive(ud.at[k + 1, t], urs.at[t, k + 1])

        @pl.when(n.z < 3)
        def _():
            arrive(ud.at[k, t], urs.at[t, k])

        @pl.when(n.z == 0)
        def _():
            add_rows(own.at[k, t], [yr.at[k, t], ud.at[k, t]], 128, yo.at[t])

        @pl.when(n.z == 3)
        def _():
            add_rows(own.at[k, t], [yr.at[k, t], ud.at[k + 1, t]], 128, yo.at[t])

        @pl.when(inner)
        def _():
            add_rows(own.at[k, t], [yr.at[k, t], ud.at[k, t], ud.at[k + 1, t]], 128, yo.at[t])

    for yy in (n.yb, n.y):
        w1_own(yy, n.xb)
        n.go(remote(r1.at[yy * 2 + n.xb], r2.at[yy], x1s.at[yy], x1r.at[yy], n.to_x))
    lax.fori_loop(2, 4, other_rows, 0)
    forward(0, 1, outer)
    n.go(remote(s1.at[n.xb], s2, x2s.at[0], x2r.at[0], n.to_x))
    loads[5].wait()

    def spare_at(k):
        return w2.at[pl.ds(pl.multiple_of(128 * k, 128), 128)]

    dn_pair(n.yb, zf, spare_at)
    send_y(1, spare_at(3 * zf), 3 * zf, 0)
    send_y(1, spare_at(1 + zf), 1 + zf, 1)
    forward(0, 0, inner)
    dn_pair(n.yb, z0, spare_at)
    send_y(1, spare_at(zn), zn, 2)
    send_y(1, spare_at(n.z), n.z, 3)
    forward(0, 2, outer)
    forward(0, 1, inner)
    for yy in (n.yb, n.y):
        w1_own(yy, n.x)
    def give(yy, qs):
        arrive(r2.at[yy], x1r.at[yy])
        add_rows(r1.at[yy * 2 + n.x], [r2.at[yy]], 256)
        for q in qs:
            to, _, zz = n.member(q)
            n.go(remote(r1.at[yy * 2 + n.x, pl.ds(pl.multiple_of(zz * 64, 64), 64)], o1.at[n.m], a1s.at[q], a1r.at[q], to))

    give(n.yb, (6, 5, 7, 4))

    def own_dn(i, carry):
        dn_pair(n.y, i, lambda k: own.at[k, 1])
        return carry

    lax.fori_loop(0, 2, own_dn, 0)
    forward(0, 2, inner)
    ones = jnp.ones((8, 1024), BF)
    d1[0] = jnp.dot(ones, dy[...], preferred_element_type=F32)
    tot = sums[0, 0:1, :] + sums[1, 0:1, :] + sums[2, 0:1, :] + sums[3, 0:1, :]
    lo1 = lanes_of((1, 128)) < 64
    zero = jnp.zeros((1, 128), F32)
    vsum = jnp.where(n.c == 0, jnp.where(lo1, tot[:, 128:256], zero), jnp.where(lo1, zero, pltpu.roll(tot[:, 128:256], 64, 1)))
    for g in range(4):
        for mm in range(8):
            e = ev.at[g * 8 + mm]
            for k in range(4):
                e[k : k + 1, :] = jnp.where(n.g == k, tot[:, 0:128], zero)
            for k in range(2):
                e[4 + k : 5 + k, :] = jnp.where(n.x == k, vsum, zero)
            for k in range(8):
                e[6 + k : 7 + k, :] = dsum[0:1, 128 * k : 128 * k + 128]
            tile = 128 * ((mm // 4) * 8 + g * 2 + (mm % 4) // 2)
            e[14:15, :] = acc[0:1, tile : tile + 128]
            e[15:16, :] = acc[1:2, tile : tile + 128]
    for xx in range(2):
        n.go(remote(ev.at[pl.ds((2 * xx + n.cb) * 8, 8)], t1.at[xx], eks.at[xx], ekr.at[xx], n.to_c))
    n.go(remote(d1.at[0], d1.at[1], dbs.at[0], dbr.at[0], n.to_c))
    forward(1, 0, outer)
    for xx in range(2):
        arrive(t1.at[xx], ekr.at[xx])
        sl = pl.ds((2 * xx + n.c) * 8, 8)
        ev[sl] = ev[sl] + t1[xx]
    arrive(d1.at[1], dbr.at[0])
    d1[2] = d1[0] + d1[1]
    n.go(remote(ev.at[pl.ds((2 * n.xb + n.c) * 8, 8)], t2, exs.at[0], exr.at[0], n.to_x))
    n.go(remote(d1.at[2], d1.at[3], dbs.at[1], dbr.at[1], n.to_x))

    forward(1, 1, outer)
    forward(1, 0, inner)
    forward(1, 2, outer)
    forward(1, 1, inner)
    give(n.y, (2, 1, 3))
    mine = pltpu.make_async_copy(r1.at[n.y * 2 + n.x, pl.ds(pl.multiple_of(n.z * 64, 64), 64)], o1.at[n.m], fl.at[0])
    mine.start()
    arrive(t2, exr.at[0])
    final = pl.ds(n.g * 8, 8)
    ev[final] = ev[final] + t2[...]
    for q in range(1, 8):
        to, yy, zz = n.member(q)
        n.go(remote(ev.at[n.g * 8 + yy * 4 + zz], eo.at[n.m], eas.at[q], ear.at[q], to))
    eo[n.m] = ev[n.g * 8 + n.m]
    arrive(d1.at[3], dbr.at[1])
    dbo[...] = d1[2] + d1[3]
    forward(1, 2, inner)
    finish(0)
    arrive(s2, x2r.at[0])
    add_rows(s1.at[n.x], [s2], 320)
    out2 = pltpu.make_async_copy(s1.at[n.x], o2, fl.at[1])
    out2.start()
    finish(1)
    for q in range(1, 8):
        yy, zz = n.source(q)
        arrive(eo.at[yy * 4 + zz], ear.at[q])
        arrive(o1.at[yy * 4 + zz], a1r.at[q])
    mine.wait()
    out2.wait()
    for k in (2, 3):
        staged(k)[2].wait_send()
    n.drain()


def reduce_all(att, normed, dy, x, act, dup, wc, w2, sums, dsum):
    sd = jax.ShapeDtypeStruct
    V = pltpu.VMEM
    return pl.pallas_call(
        reduce_kernel,
        name="reduce_all",
        out_shape=(sd((2, 128, 2048), F32), sd((8, 64, 1792), BF), sd((320, 2048), BF), sd((8, 16, 128), F32),
                   sd((8, 2048), F32)),
        in_specs=[HBM] * 8 + [VM] * 2,
        out_specs=(VM, HBM, HBM, VM, VM),
        scratch_shapes=[
            V((1024, 2048), BF), V((1024, 2048), BF), V((2048, 1792), BF), V((1280, 2048), BF),
            V((1024, 1792), BF), V((1024, 1280), BF), V((4, 1024, 256), BF),
            V((4, 128, 2048), BF), V((4, 2, 128, 2048), BF), V((5, 2, 128, 2048), BF), V((4, 2, 128, 2048), BF),
            V((4, 256, 1792), BF), V((2, 256, 1792), BF), V((2, 256, 1792), BF),
            V((2, 320, 2048), BF), V((2, 320, 2048), BF), V((320, 2048), BF), V((128, 2048), BF), V((256, 1024), BF),
            V((256, 2048), BF), V((256, 128), F32), V((256, 128), F32), V((8, 2048), F32),
            V((32, 16, 128), F32), V((2, 8, 16, 128), F32), V((8, 16, 128), F32), V((4, 8, 2048), F32),
            DMA((4, 3)), DMA((4, 3)), DMA((1,)), DMA((6,)), DMA((1,)),
            DMA((2, 4)), DMA((2, 4)), DMA((2, 3)), DMA((2, 5)),
            DMA((4,)), DMA((4,)), DMA((2,)), DMA((2,)), DMA((8,)), DMA((8,)),
            DMA((2, 2)), DMA((2, 2)), DMA((1,)), DMA((1,)),
            DMA((2,)), DMA((2,)), DMA((1,)), DMA((1,)), DMA((8,)), DMA((8,)), DMA((2,)), DMA((2,)), DMA((2,)),
        ],
        compiler_params=pltpu.CompilerParams(collective_id=3, has_side_effects=True, vmem_limit_bytes=67000000),
    )(att, normed, dy, x, act, dup, wc, w2, sums, dsum)


def finish_kernel(x, dy, yo, o1, o2, cst, y, dx, dqkv, dff, dfc2, ddense):
    low = lanes_of((64, 128)) < 64
    for i in range(16):
        yy, g, zp = i // 8, (i // 2) % 4, i % 2
        a, b = yy * 4 + 2 * zp, yy * 4 + 2 * zp + 1
        cols = slice(128 * i, 128 * i + 128)
        src = slice(128 * g, 128 * g + 128)
        even, odd = o1[a, :, src].astype(F32), o1[b, :, src].astype(F32)
        dqkv[:, cols] = jnp.where(low, even, pltpu.roll(odd, 64, 1))
        dqkv[:, 2048 + 128 * i : 2176 + 128 * i] = jnp.where(low, pltpu.roll(even, 64, 1), odd)
        src = slice(512 + 128 * (g // 2), 640 + 128 * (g // 2))
        even, odd = o1[a, :, src].astype(F32), o1[b, :, src].astype(F32)
        if g % 2 == 0:
            v = jnp.where(low, even, pltpu.roll(odd, 64, 1))
        else:
            v = jnp.where(low, pltpu.roll(even, 64, 1), odd)
        dqkv[:, 4096 + 128 * i : 4224 + 128 * i] = v
    for h in range(32):
        mm, g = (h // 16) * 4 + h % 4, (h // 4) % 4
        dff[:, 256 * h : 256 * h + 256] = o1[mm, :, 768 + 256 * g : 1024 + 256 * g].astype(F32)
    dfc2[...] = o2[0:256, :].astype(F32)
    ddense[...] = o2[256:320, :].astype(F32)

    def body(i, carry):
        sl = pl.ds(pl.multiple_of(16 * i, 16), 16)
        xf = x[sl, :].astype(F32)
        cen = xf - jnp.mean(xf, axis=-1, keepdims=True)
        rstd = lax.rsqrt(jnp.mean(cen * cen, axis=-1, keepdims=True) + EPS)
        xhat = cen * rstd
        y[sl, :] = (xf + yo[0, sl, :] + cst[2:3, :]).astype(BF)
        gr = yo[1, sl, :] * cst[0:1, :]
        dx[sl, :] = dy[sl, :].astype(F32) + rstd * (
            gr - jnp.mean(gr, axis=-1, keepdims=True) - xhat * jnp.mean(gr * xhat, axis=-1, keepdims=True)
        )
        return carry

    lax.fori_loop(0, 8, body, 0)


def finish_all(x, dy, yo, o1, o2, cst):
    sd = jax.ShapeDtypeStruct
    return pl.pallas_call(
        finish_kernel,
        name="finish_all",
        out_shape=(sd((128, 2048), BF), sd((128, 2048), F32), sd((64, 6144), F32), sd((64, 8192), F32),
                   sd((256, 2048), F32), sd((64, 2048), F32)),
        in_specs=[VM] * 6,
        out_specs=(VM,) * 6,
        compiler_params=pltpu.CompilerParams(vmem_limit_bytes=VLIM),
    )(x, dy, yo, o1, o2, cst)


def stored_columns(a):
    rows = a.shape[1]
    qk = a[:, :, :512].reshape(2, 4, rows, 4, 2, 64).transpose(2, 4, 0, 3, 1, 5).reshape(rows, 2, 2048)
    v = a[:, :, 512:768].reshape(2, 4, rows, 4, 64).transpose(2, 0, 3, 1, 4).reshape(rows, 1, 2048)
    f = a[:, :, 768:1792].reshape(2, 4, rows, 4, 256).transpose(2, 0, 3, 1, 4).reshape(rows, 8192)
    return jnp.concatenate([qk, v], axis=1).reshape(rows, 6144), f


def rotary_lanes(pos):
    lane = jnp.arange(128, dtype=jnp.int32) % 64
    freqs = jnp.exp(-(2.0 * (lane % (ROT // 2)).astype(F32) / ROT) * math.log(10000.0))
    angles = pos.astype(F32)[:, None] * freqs[None]
    turns = lane < ROT
    sign = jnp.where(turns, jnp.where(lane < ROT // 2, -1.0, 1.0), 0.0)
    return jnp.where(turns, jnp.cos(angles), 1.0), jnp.sin(angles) * sign


def fast_device(
    block_input, output_grad, segment, slots, ln_gain, ln_bias, qkv_w, qkv_b, dense_w, dense_b, fc1_w, fc1_b, fc2_w, fc2_b
):
    ctx, y, x, c, z = place()
    g, m = x * 2 + c, y * 4 + z
    index = ctx * 4 + z
    xb, dyb = block_input[0], output_grad[0]

    def spread(piece, total):
        count = piece.shape[0]
        own = jnp.arange(total, dtype=jnp.int32) // count == index
        return jnp.where(own, jnp.tile(piece, total // count), jnp.zeros((), BF))

    docs = jnp.broadcast_to(segment.astype(BF), (8, 1024))
    qb = jnp.broadcast_to(spread(qkv_b, 6144)[None], (8, 6144))
    fb = jnp.broadcast_to(spread(fc1_b, 8192)[None], (8, 8192))
    vecs = jnp.stack([spread(v, 2048) for v in (ln_gain, ln_bias, dense_b, fc2_b)])
    rest = jnp.pad(vecs[:, 1792:].reshape(1, 1024), ((0, 0), (0, 768)))
    small = jnp.concatenate([jnp.zeros((1, 1792), BF), vecs[:, :1792], rest, jnp.zeros((2, 1792), BF)], axis=0)
    pairs = lax.dynamic_slice_in_dim(slots.reshape(2, 4, 2), g, 1, 1).reshape(4)
    rows = (pairs[:, None] * 64 + jnp.arange(64, dtype=jnp.int32)[None]).reshape(256)
    cos2, sin2 = rotary_lanes(rows)
    cos, sin = rotary_lanes(jnp.arange(1024, dtype=jnp.int32))
    xg, dg, docg, normed, act, dup, wc, w2g, heads, dsum, cst = gather_all(
        xb, dyb, docs, qkv_w, fc1_w, qb, fb, small, fc2_w, dense_w, cos2, sin2
    )
    slot_of = jnp.sum(jnp.where(slots[None, :] == jnp.arange(16, dtype=jnp.int32)[:, None], jnp.arange(16, dtype=jnp.int32)[None, :], 0), axis=1)
    att, sums = attention(slot_of, heads.reshape(4, 2, 4, 128, 256), docg, cos, sin)
    yo, o1, o2, eo, dbo = reduce_all(att.reshape(4, 1024, 256), normed, dg, xg, act, dup, wc, w2g, sums, dsum)
    out, dx, g_qkv_w, g_fc1_w, g_fc2_w, g_dense_w = finish_all(xb, dyb, yo, o1, o2, cst)
    eo = eo.reshape(8, 2048)
    sq, sf = stored_columns(eo[:, None, :1792])
    g_qkv_b = lax.dynamic_slice_in_dim(sq[0], index * 192, 192, 0)
    g_fc1_b = lax.dynamic_slice_in_dim(sf[0], index * 256, 256, 0)
    tiles = jnp.sum(eo[:, 1792:].reshape(8, 2, 2, 64), axis=0)
    both = lax.dynamic_slice_in_dim(tiles, z % 2, 1, 1)
    g_db = lax.dynamic_slice_in_dim(dbo[0], index * 64, 64, 0)
    return (out[None], dx[None], both[0, 0], both[1, 0], g_qkv_w, g_qkv_b, g_dense_w, g_db, g_fc1_w, g_fc1_b, g_fc2_w, g_db)


def solution(mesh):
    in_specs = (
        P("fsdp", "ctx", None),
        P("fsdp", "ctx", None),
        P("fsdp", None),
        P(),
        P(("ctx", "fsdp")),
        P(("ctx", "fsdp")),
        P(("ctx", "fsdp"), None),
        P(("ctx", "fsdp")),
        P(("ctx", "fsdp"), None),
        P(("ctx", "fsdp")),
        P(("ctx", "fsdp"), None),
        P(("ctx", "fsdp")),
        P(("ctx", "fsdp"), None),
        P(("ctx", "fsdp")),
    )
    out_specs = (
        P("fsdp", "ctx", None),
        P("fsdp", "ctx", None),
        P(("ctx", "fsdp")),
        P(("ctx", "fsdp")),
        P(("ctx", "fsdp"), None),
        P(("ctx", "fsdp")),
        P(("ctx", "fsdp"), None),
        P(("ctx", "fsdp")),
        P(("ctx", "fsdp"), None),
        P(("ctx", "fsdp")),
        P(("ctx", "fsdp"), None),
        P(("ctx", "fsdp")),
    )
    small = mesh.shape["ctx"] == 8 and mesh.shape["fsdp"] == 4
    return jax.shard_map(
        fast_device if small else per_device, mesh=mesh, in_specs=in_specs, out_specs=out_specs, check_vma=False
    )
```

```python
import math

import jax
import jax.numpy as jnp
from jax import lax
from jax.experimental import pallas as pl
from jax.experimental.pallas import tpu as pltpu
from jax.sharding import PartitionSpec as P

HEADS = 32
ROT = 32


EPS = 1e-05
GELU_C = math.sqrt(2.0 / math.pi)
NEG = -1e30


def shifted(block, axis, distance):
    devices = range(lax.axis_size(axis))
    route = [((i - distance) % len(devices), i) for i in devices]
    return lax.ppermute(block, axis, route)


def gelu_pair(upper):
    inner = GELU_C * (upper + 0.044715 * upper * upper * upper)
    tanh_val = jnp.tanh(inner)
    value = 0.5 * upper * (1.0 + tanh_val)
    slope = 0.5 * (1.0 + tanh_val) + 0.5 * upper * (1.0 - tanh_val * tanh_val) * GELU_C * (
        1.0 + 3.0 * 0.044715 * upper * upper
    )
    return (value, slope)


def rotary_tables(positions):
    half = ROT // 2
    freqs = jnp.exp(-(2.0 * jnp.arange(half, dtype=jnp.float32) / ROT) * math.log(10000.0))
    angles = positions.astype(jnp.float32)[:, None] * freqs[None, :]
    return (jnp.cos(angles)[:, None, :], jnp.sin(angles)[:, None, :])


def rotate(tensor, cosine, sine, sign):
    half = ROT // 2
    first = tensor[..., :half]
    second = tensor[..., half:ROT]
    new_first = first * cosine - sign * second * sine
    new_second = second * cosine + sign * first * sine
    return jnp.concatenate([new_first, new_second, tensor[..., ROT:]], axis=-1)


def contract_rows(left, right):
    return lax.dot_general(
        left, right, (((0,), (0,)), ((), ())), preferred_element_type=jnp.float32
    )


def contract_cols(left, right):
    return lax.dot_general(
        left, right, (((1,), (1,)), ((), ())), preferred_element_type=jnp.float32
    )


def own_columns(matrix, cycle_size, shard_count, member):
    count = matrix.shape[0]
    piece_width = matrix.shape[1] // (cycle_size * shard_count)
    parted = matrix.reshape(count, cycle_size, shard_count, piece_width)
    return lax.dynamic_slice_in_dim(parted, member, 1, 2).reshape(count, cycle_size * piece_width)


def per_device(
    block_input,
    output_grad,
    segment,
    slots,
    ln_gain,
    ln_bias,
    qkv_w,
    qkv_b,
    dense_w,
    dense_b,
    fc1_w,
    fc1_b,
    fc2_w,
    fc2_b,
):
    cycle_size = lax.axis_size("ctx")
    index = lax.axis_index("ctx")
    shard_count = lax.axis_size("fsdp")
    member = lax.axis_index("fsdp")
    tokens = block_input.shape[1]
    width = block_input.shape[2]
    stretch = tokens // 2
    heads = HEADS
    head_dim = width // heads
    scale = head_dim ** (-0.5)
    seg_row = segment[0]
    slot_ids = jnp.arange(2 * cycle_size, dtype=jnp.int32)

    def positions(start, count):
        rows = start + jnp.arange(count, dtype=jnp.int32)
        slot = rows // stretch
        owner = jnp.sum(jnp.where(slot[:, None] == slot_ids[None, :], slots[None, :], 0), axis=1)
        return owner * stretch + rows % stretch

    qpos = positions(index * tokens, tokens)
    qdoc = jnp.take(seg_row, qpos)
    cosine, sine = rotary_tables(qpos)
    gain_all, norm_bias_every, w_qkv, b_qkv, w_up, b_up = (
        lax.all_gather(ln_gain, ("ctx", "fsdp"), axis=0, tiled=True),
        lax.all_gather(ln_bias, ("ctx", "fsdp"), axis=0, tiled=True),
        lax.all_gather(qkv_w, ("ctx", "fsdp"), axis=0, tiled=True),
        lax.all_gather(qkv_b, ("ctx", "fsdp"), axis=0, tiled=True),
        lax.all_gather(fc1_w, ("ctx", "fsdp"), axis=0, tiled=True),
        lax.all_gather(fc1_b, ("ctx", "fsdp"), axis=0, tiled=True),
    )
    xf = block_input[0].astype(jnp.float32)
    row_mean = jnp.mean(xf, axis=-1, keepdims=True)
    centered_input = xf - row_mean
    inverse_deviation = lax.rsqrt(
        jnp.mean(centered_input * centered_input, axis=-1, keepdims=True) + EPS
    )
    standardized_input = centered_input * inverse_deviation
    gain_float = gain_all.astype(jnp.float32)
    normed_rows = (standardized_input * gain_float + norm_bias_every.astype(jnp.float32)).astype(
        jnp.bfloat16
    )
    proj = jnp.dot(normed_rows, w_qkv, preferred_element_type=jnp.float32) + b_qkv.astype(
        jnp.float32
    )
    query = rotate(proj[:, :width].reshape(tokens, heads, head_dim), cosine, sine, 1.0).astype(
        jnp.bfloat16
    )
    keys = rotate(
        proj[:, width : 2 * width].reshape(tokens, heads, head_dim), cosine, sine, 1.0
    ).astype(jnp.bfloat16)
    keys_flat = keys.reshape(tokens, width)
    values = proj[:, 2 * width :].astype(jnp.bfloat16)
    acc = jnp.zeros((tokens, heads, head_dim), jnp.float32)
    top = jnp.full((heads, tokens), NEG, jnp.float32)
    key_piece = lax.all_gather(keys_flat, "ctx", axis=0, tiled=True)
    value_piece = lax.all_gather(values, "ctx", axis=0, tiled=True)
    count = key_piece.shape[0]
    kpos = positions(jnp.int32(0), count)
    kdoc = jnp.take(seg_row, kpos)
    mask = ((kpos[None, :] <= qpos[:, None]) & (kdoc[None, :] == qdoc[:, None]))[None]
    scores = (
        jnp.einsum(
            "qhd,khd->hqk",
            query,
            key_piece.reshape(count, heads, head_dim),
            preferred_element_type=jnp.float32,
        )
        * scale
    )
    scores = jnp.where(mask, scores, NEG)
    new_top = jnp.maximum(top, jnp.max(scores, axis=-1))
    factor = jnp.exp(top - new_top)
    expo = jnp.where(mask, jnp.exp(scores - new_top[..., None]), 0.0)
    total = jnp.sum(expo, axis=-1)
    part_sum = jnp.einsum(
        "hqk,khd->qhd",
        expo.astype(jnp.bfloat16),
        value_piece.reshape(count, heads, head_dim),
        preferred_element_type=jnp.float32,
    )
    acc = acc * factor.T[:, :, None] + part_sum
    acc, top, total = (acc, new_top, total)
    attn_heads = (acc / total.T[:, :, None]).astype(jnp.bfloat16)
    lse = top + jnp.log(total)
    attn = attn_heads.reshape(tokens, width)
    w_dense, b_dense, w_down, b_down = (
        lax.all_gather(dense_w, ("ctx", "fsdp"), axis=0, tiled=True),
        lax.all_gather(dense_b, ("ctx", "fsdp"), axis=0, tiled=True),
        lax.all_gather(fc2_w, ("ctx", "fsdp"), axis=0, tiled=True),
        lax.all_gather(fc2_b, ("ctx", "fsdp"), axis=0, tiled=True),
    )
    upper = jnp.dot(normed_rows, w_up, preferred_element_type=jnp.float32) + b_up.astype(
        jnp.float32
    )
    act_f, slope = gelu_pair(upper)
    act = act_f.astype(jnp.bfloat16)
    y_rows = (
        xf
        + jnp.dot(attn, w_dense, preferred_element_type=jnp.float32)
        + b_dense.astype(jnp.float32)
    )
    y_rows = (
        y_rows
        + jnp.dot(act, w_down, preferred_element_type=jnp.float32)
        + b_down.astype(jnp.float32)
    )
    grad_rows = output_grad[0]
    gradient_float = grad_rows.astype(jnp.float32)
    group_attn, group_act, group_grad = (
        lax.all_gather(attn, "fsdp", axis=0, tiled=True),
        lax.all_gather(act, "fsdp", axis=0, tiled=True),
        lax.all_gather(grad_rows, "fsdp", axis=0, tiled=True),
    )
    group_bias = jnp.sum(group_grad.astype(jnp.float32), axis=0)
    own_bias = own_columns(group_bias[None], cycle_size, shard_count, member)[0]
    dense_part = contract_rows(own_columns(group_attn, cycle_size, shard_count, member), group_grad)
    down_part = contract_rows(own_columns(group_act, cycle_size, shard_count, member), group_grad)
    g_dense_w, g_dense_b, g_fc2_w, g_fc2_b = (
        lax.psum_scatter(
            dense_part.astype(jnp.bfloat16), "ctx", scatter_dimension=0, tiled=True
        ).astype(jnp.float32),
        lax.psum_scatter(
            own_bias.astype(jnp.bfloat16), "ctx", scatter_dimension=0, tiled=True
        ).astype(jnp.float32),
        lax.psum_scatter(
            down_part.astype(jnp.bfloat16), "ctx", scatter_dimension=0, tiled=True
        ).astype(jnp.float32),
        lax.psum_scatter(
            own_bias.astype(jnp.bfloat16), "ctx", scatter_dimension=0, tiled=True
        ).astype(jnp.float32),
    )
    dup = contract_cols(grad_rows, w_down) * slope
    up_bias_grad = jnp.sum(dup, axis=0)
    dup_b = dup.astype(jnp.bfloat16)
    dattn = contract_cols(grad_rows, w_dense).astype(jnp.bfloat16).reshape(tokens, heads, head_dim)
    delta = jnp.sum(dattn.astype(jnp.float32) * attn_heads.astype(jnp.float32), axis=-1).T

    def cycle_step(step, carry):
        key_cur, value_cur, dkey_acc, dvalue_acc, dquery_acc = carry
        anchor = (index - step + cycle_size) % cycle_size
        kpos = positions(anchor * tokens, tokens)
        kdoc = jnp.take(seg_row, kpos)
        mask = ((kpos[None, :] <= qpos[:, None]) & (kdoc[None, :] == qdoc[:, None]))[None]
        key_heads = key_cur.reshape(tokens, heads, head_dim)
        scores = (
            jnp.einsum("qhd,khd->hqk", query, key_heads, preferred_element_type=jnp.float32) * scale
        )
        probs = jnp.where(mask, jnp.exp(jnp.where(mask, scores, NEG) - lse[..., None]), 0.0)
        dvalue_acc = dvalue_acc + jnp.einsum(
            "hqk,qhd->khd", probs.astype(jnp.bfloat16), dattn, preferred_element_type=jnp.float32
        ).reshape(tokens, width)
        dprob = jnp.einsum(
            "qhd,khd->hqk",
            dattn,
            value_cur.reshape(tokens, heads, head_dim),
            preferred_element_type=jnp.float32,
        )
        dscore = (probs * (dprob - delta[..., None]) * scale).astype(jnp.bfloat16)
        dquery_acc = dquery_acc + jnp.einsum(
            "hqk,khd->qhd", dscore, key_heads, preferred_element_type=jnp.float32
        )
        dkey_acc = dkey_acc + jnp.einsum(
            "hqk,qhd->khd", dscore, query, preferred_element_type=jnp.float32
        ).reshape(tokens, width)
        key_cur, value_cur = shifted((key_cur, value_cur), "ctx", 1)
        dkey_acc, dvalue_acc = (
            shifted(dkey_acc.astype(jnp.bfloat16), "ctx", 1).astype(dkey_acc.dtype),
            shifted(dvalue_acc.astype(jnp.bfloat16), "ctx", 1).astype(dvalue_acc.dtype),
        )
        return (key_cur, value_cur, dkey_acc, dvalue_acc, dquery_acc)

    flat_zero = jnp.zeros((tokens, width), jnp.float32)
    cycle_init = (
        keys_flat,
        values,
        flat_zero,
        flat_zero,
        jnp.zeros((tokens, heads, head_dim), jnp.float32),
    )
    cycle_out = lax.fori_loop(0, cycle_size, cycle_step, cycle_init)
    dkey_sum, dvalue_sum, dquery_sum = (cycle_out[2], cycle_out[3], cycle_out[4])
    dquery = rotate(dquery_sum, cosine, sine, -1.0).reshape(tokens, width)
    dkey = rotate(dkey_sum.reshape(tokens, heads, head_dim), cosine, sine, -1.0).reshape(
        tokens, width
    )
    dproj = jnp.concatenate([dquery, dkey, dvalue_sum], axis=1)
    qkv_bias_grad = jnp.sum(dproj, axis=0)
    dproj_b = dproj.astype(jnp.bfloat16)
    normed_input_grad = contract_cols(dproj_b, w_qkv) + contract_cols(dup_b, w_up)
    gain_gradient = jnp.sum(normed_input_grad * standardized_input, axis=0)
    lnb_grad = jnp.sum(normed_input_grad, axis=0)
    scaled_rows = normed_input_grad * gain_float
    dx_rows = gradient_float + inverse_deviation * (
        scaled_rows
        - jnp.mean(scaled_rows, axis=-1, keepdims=True)
        - standardized_input * jnp.mean(scaled_rows * standardized_input, axis=-1, keepdims=True)
    )
    group_normed, group_dproj, group_dup = (
        lax.all_gather(normed_rows, "fsdp", axis=0, tiled=True),
        lax.all_gather(dproj_b, "fsdp", axis=0, tiled=True),
        lax.all_gather(dup_b, "fsdp", axis=0, tiled=True),
    )
    own_normed = own_columns(group_normed, cycle_size, shard_count, member)
    g_qkv_w, g_fc1_w = (
        lax.psum_scatter(
            contract_rows(own_normed, group_dproj).astype(jnp.bfloat16),
            "ctx",
            scatter_dimension=0,
            tiled=True,
        ).astype(jnp.float32),
        lax.psum_scatter(
            contract_rows(own_normed, group_dup).astype(jnp.bfloat16),
            "ctx",
            scatter_dimension=0,
            tiled=True,
        ).astype(jnp.float32),
    )
    layer_gain_grad, g_lnb, g_qkv_b, g_fc1_b = (
        lax.psum_scatter(gain_gradient, ("ctx", "fsdp"), scatter_dimension=0, tiled=True),
        lax.psum_scatter(lnb_grad, ("ctx", "fsdp"), scatter_dimension=0, tiled=True),
        lax.psum_scatter(qkv_bias_grad, ("ctx", "fsdp"), scatter_dimension=0, tiled=True),
        lax.psum_scatter(up_bias_grad, ("ctx", "fsdp"), scatter_dimension=0, tiled=True),
    )
    return (
        y_rows.astype(jnp.bfloat16)[None],
        dx_rows[None],
        layer_gain_grad,
        g_lnb,
        g_qkv_w,
        g_qkv_b,
        g_dense_w,
        g_dense_b,
        g_fc1_w,
        g_fc1_b,
        g_fc2_w,
        g_fc2_b,
    )


BF = jnp.bfloat16
F32 = jnp.float32
MESH = pl.DeviceIdType.MESH
HBM = pl.BlockSpec(memory_space=pl.ANY)
VM = pl.BlockSpec(memory_space=pltpu.VMEM)
DMA = pltpu.SemaphoreType.DMA
VLIM = 60 * 1024 * 1024


def place():
    ctx, z = lax.axis_index("ctx"), lax.axis_index("fsdp")
    return ctx, lax.div(ctx, 4), lax.rem(lax.div(ctx, 2), 2), lax.rem(ctx, 2), z


class Net:
    def __init__(self):
        self.ctx, self.y, self.x, self.c, self.z = place()
        self.yb, self.xb, self.cb = 1 - self.y, 1 - self.x, 1 - self.c
        self.m = self.y * 4 + self.z
        self.g = self.x * 2 + self.c
        self.to_y = {"ctx": self.ctx + 4 * (1 - 2 * self.y), "fsdp": self.z}
        self.to_x = {"ctx": self.ctx + 2 * (1 - 2 * self.x), "fsdp": self.z}
        self.to_c = {"ctx": self.ctx + 1 - 2 * self.c, "fsdp": self.z}
        self.up = {"ctx": self.ctx, "fsdp": self.z + 1}
        self.dn = {"ctx": self.ctx, "fsdp": self.z - 1}
        self.sent = []

    def member(self, q):
        flip, step = q // 4, q % 4
        z = lax.rem(self.z + step, 4)
        yy = self.yb if flip else self.y
        return {"ctx": self.ctx + flip * 4 * (1 - 2 * self.y), "fsdp": z}, yy, z

    def source(self, q):
        flip, step = q // 4, q % 4
        return (self.yb if flip else self.y), lax.rem(self.z + 4 - step, 4)

    def barrier(self, more=()):
        sem = pltpu.get_barrier_semaphore()
        peers = [self.member(q)[0] for q in range(1, 8)] + [self.to_x, self.to_c, *more]
        for peer in peers:
            pl.semaphore_signal(sem, inc=1, device_id=peer, device_id_type=MESH)
        pl.semaphore_wait(sem, len(peers))

    def go(self, copy, when=None):
        if when is None:
            copy.start()
        else:
            pl.when(when)(copy.start)
        self.sent.append((copy, when))

    def drain(self):
        for copy, when in self.sent:
            if when is None:
                copy.wait_send()
            else:
                pl.when(when)(copy.wait_send)


def remote(src, dst, send, recv, to):
    return pltpu.make_async_remote_copy(
        src_ref=src, dst_ref=dst, send_sem=send, recv_sem=recv, device_id=to, device_id_type=MESH
    )


def arrive(like, recv):
    pltpu.make_async_copy(like, like, recv).wait()


def head_tiles(src, dst, rows):
    qkv, ff = src
    low = lanes_of((rows, 128)) < 64

    def tile(base, h):
        t = 128 * (h // 2)
        return qkv[:, base + t : base + t + 128].astype(F32)

    def join(a, b, odd):
        if odd:
            return jnp.where(low, pltpu.roll(a, 64, 1), b).astype(BF)
        return jnp.where(low, a, pltpu.roll(b, 64, 1)).astype(BF)

    for mm in range(8):
        first = (mm // 4) * 16 + mm % 4
        odd = first % 2
        for g in range(4):
            h = first + 4 * g
            dst(mm, 128 * g, join(tile(0, h), tile(2048, h), odd))
            if ff is not None:
                dst(mm, 768 + 256 * g, ff[:, 256 * h : 256 * h + 256])
        for k in range(2):
            h = first + 8 * k
            dst(mm, 512 + 128 * k, join(tile(4096, h), tile(4096, h + 4), odd))


def gather_kernel(slots, x, dy, seg, qkv, ff, pack, fc2, dense,
                  xg, dg, docg, normed_o, act_o, dup_o, wc_o, w2_o, heads, dsum, cst, cosp, sinp,
                  docs, qb, cos, sin, xv, dv, wc, w2g, eg, ws, es, nrm, act, dup, hs,
                  loc, us, ur, ds_, dr, ys, yr, as_, ar, es_, er,
                  wxs, wxr, wks, wkr, exs, exr, eks, ekr, fxs, fxr, fks, fkr, hss, hsr, hl, wb):
    n = Net()
    far = {"ctx": n.ctx + 2 * (1 - 2 * n.x) + 1 - 2 * n.c, "fsdp": n.z}
    docs[...] = jnp.broadcast_to(seg[...].astype(F32), (8, 1024)).astype(BF)
    n.barrier(more=(far,))

    def wrow(yy, xx, cc, zz):
        return wc.at[pl.ds(pl.multiple_of((yy * 16 + xx * 8 + cc * 4 + zz) * 64, 64), 64)]

    def wide(gg):
        return w2g.at[pl.ds(pl.multiple_of(gg * 256, 256), 256)]

    def thin(gg):
        return w2g.at[pl.ds(pl.multiple_of(1024 + gg * 64, 64), 64)]

    def shard(yy, zz, p):
        mm = yy * 4 + zz
        if p == 2:
            return docg.at[mm]
        return (xv, dv)[p].at[pl.ds(pl.multiple_of(mm * 128, 128), 128)]

    mine = (x, dy, docs)
    parts = (0, 1, 2)

    def tokens(p):
        n.go(remote(mine[p], shard(n.y, n.z, p), us.at[p, 0], ur.at[p, 0], n.up), n.z < 3)
        n.go(remote(mine[p], shard(n.y, n.z, p), ds_.at[p, 0], dr.at[p, 0], n.dn), n.z > 0)
        n.go(remote(mine[p], shard(n.y, n.z, p), ys.at[p, 0], yr.at[p, n.z], n.to_y))

    tokens(0)
    rows2 = ((fc2, wide), (dense, thin))
    for k, (ref, part) in enumerate(rows2):
        n.go(remote(ref, part(n.g), fxs.at[k], fxr.at[k], n.to_x))
        n.go(remote(ref, part(n.g), fks.at[k], fkr.at[k], n.to_c))

    def put_w(mm, col, value):
        ws[mm, :, col : col + value.shape[1]] = value

    low8 = lanes_of((8, 128)) < 64
    zero8 = jnp.zeros((8, 128), F32)
    index = n.ctx * 4 + n.z
    tile, odd = lax.div(index, 2), lax.rem(index, 2)
    qb[...] = jnp.zeros_like(qb)
    b0 = jnp.broadcast_to(pack[4:5, 0:128].astype(F32), (8, 128))
    b1 = jnp.broadcast_to(pack[4:5, 128:256].astype(F32), (8, 128))
    r0, r1 = pltpu.roll(b0, 64, 1), pltpu.roll(b1, 64, 1)
    first = pl.multiple_of((tile * 3 + odd) * 128, 128)
    qb[:, pl.ds(first, 128)] = jnp.where(odd == 0, b0, jnp.where(low8, zero8, r0)).astype(BF)
    qb[:, pl.ds(pl.multiple_of(first + 128, 128), 128)] = jnp.where(odd == 0, b1, jnp.where(low8, r0, r1)).astype(BF)
    es[...] = jnp.zeros_like(es)

    def put_e(mm, col, value):
        es[mm, 0:1, col : col + value.shape[1]] = value[0:1]

    head_tiles((qkv, ff), put_w, 64)
    head_tiles((qb, None), put_e, 8)
    es[n.m, 0:1, pl.ds(pl.multiple_of(768 + 256 * n.g, 256), 256)] = pack[5:6, :]
    for r in range(4):
        v = pack[r : r + 1, 0:128].astype(F32)
        own64 = jnp.where(odd == 0, v, pltpu.roll(v, 64, 1)).astype(BF)
        for mm in range(8):
            @pl.when(tile < 14)
            def _():
                es[mm, r + 1 : r + 2, pl.ds(pl.multiple_of(128 * tile, 128), 128)] = own64

            @pl.when(tile >= 14)
            def _():
                es[mm, 5:6, pl.ds(pl.multiple_of(256 * r + 128 * (tile - 14), 128), 128)] = own64

    for q in (4, 1, 3, 5, 7, 2, 6):
        to, yy, zz = n.member(q)
        n.go(remote(es.at[yy * 4 + zz], eg.at[n.g * 8 + n.m], es_.at[q], er.at[q], to))
        n.go(remote(ws.at[yy * 4 + zz], wrow(n.y, n.x, n.c, n.z), as_.at[q], ar.at[q], to))
    own = ws.at[n.m]
    n.go(remote(own, wrow(n.y, n.x, n.c, n.z), wxs.at[0], wxr.at[0], n.to_x))
    n.go(remote(own, wrow(n.y, n.x, n.c, n.z), wks.at[0], wkr.at[0], n.to_c))
    tokens(1)
    tokens(2)
    local = [
        pltpu.make_async_copy(x, shard(n.y, n.z, 0), loc.at[0]),
        pltpu.make_async_copy(dy, shard(n.y, n.z, 1), loc.at[1]),
        pltpu.make_async_copy(docs, shard(n.y, n.z, 2), loc.at[2]),
        pltpu.make_async_copy(own, wrow(n.y, n.x, n.c, n.z), loc.at[3]),
        pltpu.make_async_copy(es.at[n.m], eg.at[n.g * 8 + n.m], loc.at[4]),
        pltpu.make_async_copy(fc2, wide(n.g), loc.at[5]),
        pltpu.make_async_copy(dense, thin(n.g), loc.at[6]),
    ]
    for copy in local:
        copy.start()

    lane = lax.rem(lanes_of((64, 128)), 64)
    freqs = jnp.exp(-(2.0 * lax.rem(lane, ROT // 2).astype(F32) / ROT) * math.log(10000.0))
    turns = lane < ROT
    sign = jnp.where(turns, jnp.where(lane < ROT // 2, -1.0, 1.0), 0.0)
    row64 = lax.broadcasted_iota(jnp.int32, (64, 128), 0)

    def turn(start):
        angles = (start + row64).astype(F32) * freqs
        return jnp.where(turns, jnp.cos(angles), 1.0), jnp.sin(angles) * sign

    for k in range(4):
        rows64 = slice(64 * k, 64 * k + 64)
        cos[rows64, :], sin[rows64, :] = turn(slots[(k // 2) * 8 + 2 * n.g + k % 2] * 64)

    def table_rows(i, carry):
        sl = pl.ds(pl.multiple_of(64 * i, 64), 64)
        cosp[sl, :], sinp[sl, :] = turn(64 * i)
        return carry

    lax.fori_loop(0, 16, table_rows, 0)

    def line(d, ps):
        below, above = n.z >= d, n.z + d <= 3
        for p in ps:
            for there, zz, recv, send, nxt, more, to in (
                (below, n.z - d, ur, us, ur, n.z < 3, n.up),
                (above, n.z + d, dr, ds_, dr, n.z > 0, n.dn),
            ):
                block = shard(n.y, zz, p)

                @pl.when(there)
                def _():
                    arrive(block, recv.at[p, d - 1])

                if d < 3:
                    n.go(remote(block, block, send.at[p, d], nxt.at[p, d], to), there & more)
                slot = d if to is n.up else d + 3
                n.go(remote(block, block, ys.at[p, slot], yr.at[p, zz], n.to_y), there)

    def pieces(qs):
        for q in qs:
            yy, zz = n.source(q)
            block = wrow(yy, n.x, n.c, zz)
            arrive(block, ar.at[q])
            n.go(remote(block, block, wxs.at[q], wxr.at[q], n.to_x))
            n.go(remote(block, block, wks.at[q], wkr.at[q], n.to_c))

    def relay(qs):
        for q in qs:
            yy, zz = n.source(q)
            block = wrow(yy, n.xb, n.c, zz)
            arrive(block, wxr.at[q])
            n.go(remote(block, block, wks.at[8 + q], wkr.at[8 + q], n.to_c))

    line(1, (0,))
    pieces((4, 1, 3))
    line(1, (1, 2))
    pieces((5, 7, 2, 6))
    for q in range(1, 8):
        yy, zz = n.source(q)
        arrive(eg.at[n.g * 8 + yy * 4 + zz], er.at[q])
    local[4].wait()
    these = eg.at[pl.ds(n.g * 8, 8)]
    n.go(remote(these, these, exs.at[0], exr.at[0], n.to_x))
    n.go(remote(these, these, eks.at[0], ekr.at[0], n.to_c))
    line(2, parts)
    gx = n.xb * 2 + n.c
    for k, (ref, part) in enumerate(rows2):
        arrive(part(gx), fxr.at[k])
        n.go(remote(part(gx), part(gx), fks.at[2 + k], fkr.at[2 + k], n.to_c))
    theirs = eg.at[pl.ds(gx * 8, 8)]
    relay((0, 4, 1, 3, 5, 7, 2, 6))
    arrive(theirs, exr.at[0])
    n.go(remote(theirs, theirs, eks.at[1], ekr.at[1], n.to_c))
    for q in range(8):
        yy, zz = n.source(q)
        arrive(wrow(yy, n.x, n.cb, zz), wkr.at[q])
        arrive(wrow(yy, n.xb, n.cb, zz), wkr.at[8 + q])
    for k in range(2):
        gg = 2 * (n.xb if k else n.x) + n.cb
        arrive(eg.at[pl.ds(gg * 8, 8)], ekr.at[k])
        for j, (ref, part) in enumerate(rows2):
            arrive(part(gg), fkr.at[2 * k + j])
    for k in (0, 1, 2, 3, 5, 6):
        local[k].wait()
    out_w = [pltpu.make_async_copy(wc, wc_o, wb.at[0]), pltpu.make_async_copy(w2g, w2_o, wb.at[1])]
    for copy in out_w:
        copy.start()

    def add_ext(i, t):
        return t + eg[i].astype(F32)

    ext = lax.fori_loop(0, 32, add_ext, jnp.zeros((8, 1792), F32))
    cst[0:1, 0:1792], cst[0:1, 1792:2048] = ext[1:2], ext[5:6, 0:256]
    cst[1:2, 0:1792], cst[1:2, 1792:2048] = ext[2:3], ext[5:6, 256:512]
    cst[2:3, 0:1792], cst[2:3, 1792:2048] = ext[3:4] + ext[4:5], ext[5:6, 512:768] + ext[5:6, 768:1024]
    cst[3:4, 0:1792], cst[3:4, 1792:2048] = ext[0:1], jnp.zeros((1, 256), F32)
    cst[4:8, :] = jnp.zeros((4, 2048), F32)
    dsum[...] = jnp.zeros_like(dsum)
    z0 = lax.div(n.z, 2)
    half = lanes_of((256, 128)) < 64

    def rows_of(j):
        yy = n.y + lax.rem(j, 2) * (1 - 2 * n.y)
        zp = z0 + lax.div(j, 2) * (1 - 2 * z0)
        return yy, zp, pl.ds(pl.multiple_of((yy * 4 + 2 * zp) * 128, 256), 256)

    def sends(j):
        yy, zp, rows = rows_of(j)
        return [
            remote(hs.at[gg, rows], heads.at[n.g, rows], hss.at[j, k], hsr.at[j, k], to)
            for k, (to, gg) in enumerate(((far, 2 * n.xb + n.cb), (n.to_x, 2 * n.xb + n.c), (n.to_c, 2 * n.x + n.cb)))
        ]

    def keeps(j):
        yy, zp, rows = rows_of(j)
        return [
            pltpu.make_async_copy(hs.at[n.g, rows], heads.at[n.g, rows], hl.at[j, 0]),
            pltpu.make_async_copy(nrm.at[rows], normed_o.at[rows], hl.at[j, 1]),
            pltpu.make_async_copy(act.at[rows], act_o.at[rows], hl.at[j, 2]),
            pltpu.make_async_copy(dup.at[rows], dup_o.at[rows], hl.at[j, 3]),
            pltpu.make_async_copy(xv.at[rows], xg.at[rows], hl.at[j, 4]),
            pltpu.make_async_copy(dv.at[rows], dg.at[rows], hl.at[j, 5]),
        ]

    def pair(j, carry):
        yy, zp, rows = rows_of(j)
        base = (yy * 4 + 2 * zp) * 128

        @pl.when(lax.rem(j, 2) == 1)
        def _():
            for k in range(2):
                for p in parts:
                    arrive(shard(yy, 2 * zp + k, p), yr.at[p, 2 * zp + k])

        def norm(i, c):
            sl = pl.ds(pl.multiple_of(base + 32 * i, 32), 32)
            xf = xv[sl, :].astype(F32)
            cen = xf - jnp.mean(xf, axis=-1, keepdims=True)
            rstd = lax.rsqrt(jnp.mean(cen * cen, axis=-1, keepdims=True) + EPS)
            nrm[sl, :] = (cen * rstd * cst[0:1, :] + cst[1:2, :]).astype(BF)
            return c

        lax.fori_loop(0, 8, norm, 0)
        table = pl.ds(pl.multiple_of(yy * 128, 128), 128)
        cosv = jnp.concatenate([cos[table, :]] * 2, axis=0)
        sinv = jnp.concatenate([sin[table, :]] * 2, axis=0)
        for k in range(2):
            t2 = jnp.dot(nrm[rows, :], wc[:, 256 * k : 256 * k + 256], preferred_element_type=F32)
            t2 = t2 + cst[3:4, 256 * k : 256 * k + 256]
            for i in range(2):
                t = t2[:, 128 * i : 128 * i + 128]
                hs[2 * k + i, rows, 0:128] = (t * cosv + partner(t) * sinv).astype(BF)
        v4 = jnp.dot(nrm[rows, :], wc[:, 512:768], preferred_element_type=F32) + cst[3:4, 512:768]
        d4 = dot_nt(dv[rows, :], w2g[1024:1280, :])
        for g in range(4):
            v, d = (t[:, 128 * (g // 2) : 128 * (g // 2) + 128] for t in (v4, d4))
            if g % 2 == 0:
                vd = jnp.where(half, v, pltpu.roll(d, 64, 1))
            else:
                vd = jnp.where(half, pltpu.roll(v, 64, 1), d)
            hs[g, rows, 128:256] = vd.astype(BF)
        for copy in sends(j):
            copy.start()
        for k in range(4):
            cols, wcols = slice(256 * k, 256 * k + 256), slice(768 + 256 * k, 1024 + 256 * k)
            up = jnp.dot(nrm[rows, :], wc[:, wcols], preferred_element_type=F32) + cst[3:4, wcols]
            a, slope = gelu_pair(up)
            act[rows, cols] = a.astype(BF)
            du = dot_nt(dv[rows, :], w2g[cols, :]) * slope
            dup[rows, cols] = du.astype(BF)
            dsum[:, cols] += jnp.broadcast_to(jnp.sum(du, axis=0, keepdims=True), (8, 256))
        for copy in keeps(j):
            copy.start()
        return carry

    lax.fori_loop(0, 2, pair, 0)
    line(3, parts)
    lax.fori_loop(2, 4, pair, 0)
    for j in range(4):
        for copy in sends(j):
            copy.wait()
        for copy in keeps(j):
            copy.wait()
    for copy in out_w:
        copy.wait()
    n.drain()


def gather_all(slots, x, dy, seg, qkv, ff, pack, fc2, dense):
    sd = jax.ShapeDtypeStruct
    V = pltpu.VMEM
    return pl.pallas_call(
        gather_kernel,
        name="gather_all",
        out_shape=(sd((1024, 2048), BF), sd((1024, 2048), BF), sd((8, 8, 1024), BF), sd((1024, 2048), BF),
                   sd((1024, 1024), BF), sd((1024, 1024), BF), sd((2048, 1792), BF), sd((1280, 2048), BF),
                   sd((4, 1024, 256), BF), sd((8, 1024), F32), sd((8, 2048), F32), sd((1024, 128), F32), sd((1024, 128), F32)),
        in_specs=[pl.BlockSpec(memory_space=pltpu.SMEM)] + [VM] * 8,
        out_specs=(HBM, HBM, VM, HBM, HBM, HBM, HBM, HBM, HBM, VM, VM, VM, VM),
        scratch_shapes=[V((8, 1024), BF), V((8, 6144), BF), V((256, 128), F32), V((256, 128), F32),
                        V((1024, 2048), BF), V((1024, 2048), BF), V((2048, 1792), BF), V((1280, 2048), BF),
                        V((32, 8, 1792), BF), V((8, 64, 1792), BF), V((8, 8, 1792), BF),
                        V((1024, 2048), BF), V((1024, 1024), BF), V((1024, 1024), BF), V((4, 1024, 256), BF),
                        DMA((7,)), DMA((3, 3)), DMA((3, 3)), DMA((3, 3)), DMA((3, 3)), DMA((3, 7)), DMA((3, 4)),
                        DMA((8,)), DMA((8,)), DMA((8,)), DMA((8,)), DMA((8,)), DMA((8,)), DMA((16,)), DMA((16,)),
                        DMA((1,)), DMA((1,)), DMA((2,)), DMA((2,)), DMA((2,)), DMA((2,)), DMA((4,)), DMA((4,)),
                        DMA((4, 3)), DMA((4, 3)), DMA((4, 6)), DMA((2,))],
        compiler_params=pltpu.CompilerParams(collective_id=1, has_side_effects=True, vmem_limit_bytes=VLIM),
    )(slots, x, dy, seg, qkv, ff, pack, fc2, dense)


def lanes_of(shape):
    return lax.broadcasted_iota(jnp.int32, shape, len(shape) - 1)


def partner(t):
    low = lax.rem(lanes_of(t.shape), 64) < 16
    return jnp.where(low, pltpu.roll(t, 112, 1), pltpu.roll(t, 16, 1))


def dot_nt(a, b):
    return lax.dot_general(a, b, (((1,), (1,)), ((), ())), preferred_element_type=F32)


def dot_tn(a, b):
    return lax.dot_general(a, b, (((0,), (0,)), ((), ())), preferred_element_type=F32)


def attention_kernel(slot_of, a, docs, cos, sin, out, sums, seq, flip, doc, both, dk, dv):
    def where_is(p):
        r = slot_of[p]
        ctx = lax.div(r, 2)
        return lax.rem(ctx, 4), lax.div(ctx, 4), pl.ds(pl.multiple_of(lax.rem(r, 2) * 64, 64), 64)

    for p in range(16):
        g, yy, rows = where_is(p)
        seq[64 * p : 64 * p + 64, :] = a[g, yy, 0, rows, :]
    flip[...] = seq[...].T
    doc[...] = jnp.broadcast_to(docs[0, 0:1, :].astype(F32), (128, 1024)).T
    dk[...] = jnp.zeros_like(dk)
    dv[...] = jnp.zeros_like(dv)
    scale = 0.125
    low = lanes_of((256, 128)) < 64
    causal = lax.broadcasted_iota(jnp.int32, (256, 256), 0) <= lanes_of((256, 256))
    for i in range(4):
        k0 = max(0, i - 2) * 256
        kn = 256 * (i + 1) - k0
        rq, rk = slice(256 * i, 256 * i + 256), slice(k0, k0 + kn)
        qk, vd = seq[rq, 0:128], seq[rq, 128:256]
        kk, vv = seq[rk, 0:128], seq[rk, 128:256]
        zero = jnp.zeros((256, 128), F32)
        qs = jnp.where(low, zero, pltpu.roll(qk.astype(F32), 64, 1) * scale).astype(BF)
        ds_lhs = jnp.where(low, pltpu.roll(vd.astype(F32), 64, 1), zero).astype(BF)
        s = dot_nt(kk, qs)
        same = jnp.concatenate([doc[rk, :]] * 2, axis=1) == docs[0, 0:1, rq].astype(F32)
        last = jnp.where(same[kn - 256 :] & causal, s[kn - 256 :], NEG)
        if kn > 256:
            s = jnp.concatenate([jnp.where(same[: kn - 256], s[: kn - 256], NEG), last], axis=0)
        else:
            s = last
        e = jnp.exp(s - jnp.max(s, axis=0, keepdims=True))
        inv = 1.0 / jnp.sum(e, axis=0, keepdims=True)
        o = jnp.dot(flip[128:192, rk], e.astype(BF), preferred_element_type=F32) * inv
        delta = jnp.sum(flip[192:256, rq].astype(F32) * o.astype(BF).astype(F32), axis=0, keepdims=True)
        pr = e * inv
        dv[rk, :] += jnp.dot(pr.astype(BF), vd, preferred_element_type=F32)
        ds = (pr * (dot_nt(vv, ds_lhs) - delta)).astype(BF)
        dk[rk, :] += jnp.dot(ds, qs, preferred_element_type=F32)
        dq = jnp.dot(flip[64:128, rk], ds, preferred_element_type=F32) * scale
        both[rq, :] = jnp.concatenate([dq, o], axis=0).T
    half = lanes_of((64, 128)) < 64
    s1 = jnp.zeros((1, 128), F32)
    s2 = jnp.zeros((1, 128), F32)
    for p in range(16):
        rows = slice(64 * p, 64 * p + 64)
        g, yy, place_rows = where_is(p)
        w = both[rows, :]
        t = jnp.where(half, w, dk[rows, :])
        t = t * cos[rows, :] - partner(t) * sin[rows, :]
        u = jnp.where(half, pltpu.roll(dv[rows, :], 64, 1), w)
        s1 += jnp.sum(t, axis=0, keepdims=True)
        s2 += jnp.sum(u, axis=0, keepdims=True)
        out[g, yy, 0, place_rows, 0:128] = t.astype(BF)
        out[g, yy, 0, place_rows, 128:256] = u.astype(BF)
    sums[0, :, 0:128] = jnp.broadcast_to(s1, (8, 128))
    sums[0, :, 128:256] = jnp.broadcast_to(s2, (8, 128))


def attention(slot_of, a, docs, cos, sin):
    sd = jax.ShapeDtypeStruct
    blk = pl.BlockSpec((4, 2, 1, 128, 256), lambda s, t: (0, 0, s, 0, 0))
    return pl.pallas_call(
        attention_kernel,
        name="attention",
        grid_spec=pltpu.PrefetchScalarGridSpec(
            num_scalar_prefetch=1,
            grid=(4,),
            in_specs=[
                blk,
                pl.BlockSpec((1, 8, 1024), lambda s, t: (s, 0, 0)),
                pl.BlockSpec((1024, 128), lambda s, t: (0, 0)),
                pl.BlockSpec((1024, 128), lambda s, t: (0, 0)),
            ],
            out_specs=(blk, pl.BlockSpec((1, 8, 256), lambda s, t: (s, 0, 0))),
            scratch_shapes=[pltpu.VMEM((1024, 256), BF), pltpu.VMEM((256, 1024), BF)] + [pltpu.VMEM((1024, 128), F32)] * 4,
        ),
        out_shape=(sd((4, 2, 4, 128, 256), BF), sd((4, 8, 256), F32)),
        compiler_params=pltpu.CompilerParams(vmem_limit_bytes=VLIM),
    )(slot_of, a, docs, cos, sin)


def add_rows(dst, srcs, rows, out=None, step=16):
    out = dst if out is None else out

    def body(i, carry):
        sl = pl.ds(pl.multiple_of(i * step, step), step)
        v = dst[sl, :].astype(F32)
        for s in srcs:
            v = v + s[sl, :].astype(F32)
        out[sl, :] = v.astype(out.dtype)
        return carry

    lax.fori_loop(0, rows // step, body, 0)


def reduce_kernel(att, normed_i, dy_i, x_i, act_i, dup_i, wc_i, w2_i, sums, dsum,
                  yo, o1, o2, eo, dbo,
                  nrm, dy, wc, w2, dpr, up2, rec, ysend, yr, ud, own, r1, st1, r2, s1, st2, s2, thin2, flip, xst, mu, rs, acc, ev, t1, t2, d1,
                  hss, hsr, hl, ld, xl, yss, yrs, uss, urs, k1s, k1r, x1s, x1r, a1s, a1r,
                  k2s, k2r, x2s, x2r, eks, ekr, exs, exr, eas, ear, dbs, dbr, fl):
    n = Net()
    far = {"ctx": n.ctx + 2 * (1 - 2 * n.x) + 1 - 2 * n.c, "fsdp": n.z}
    n.barrier(more=(far,))
    z0 = lax.div(n.z, 2)
    zf = 1 - z0

    def halves(k):
        yy = n.y if k % 2 else n.yb
        tile = 0 if k >= 2 else 1
        return pl.ds(pl.multiple_of(yy * 512, 512), 512), pl.ds(128 * tile, 128)

    for k in range(4):
        rows, lanes = halves(k)
        for i, (to, gg) in enumerate(((far, 2 * n.xb + n.cb), (n.to_x, 2 * n.xb + n.c), (n.to_c, 2 * n.x + n.cb))):
            n.go(remote(att.at[gg, rows, lanes], rec.at[n.g, rows, lanes], hss.at[k, i], hsr.at[k, i], to))
    keep = pltpu.make_async_copy(att.at[n.g], rec.at[n.g], hl.at[0])
    loads = [
        pltpu.make_async_copy(dy_i, dy, ld.at[0]),
        pltpu.make_async_copy(act_i, up2.at[:, pl.ds(0, 1024)], ld.at[1]),
        pltpu.make_async_copy(w2_i, w2, ld.at[2]),
        pltpu.make_async_copy(dup_i, dpr.at[:, pl.ds(768, 1024)], ld.at[3]),
        pltpu.make_async_copy(normed_i, nrm, ld.at[4]),
        pltpu.make_async_copy(wc_i, wc, ld.at[5]),
    ]
    for copy in loads[:2] + [keep] + loads[2:]:
        copy.start()

    def heads_in(k):
        rows, lanes = halves(k)
        for i, gg in enumerate((2 * n.xb + n.cb, 2 * n.xb + n.c, 2 * n.x + n.cb)):
            arrive(rec.at[gg, rows, lanes], hsr.at[k, i])

    low = lanes_of((64, 128)) < 64

    def split(k):
        yy = n.y if k % 2 else n.yb

        def body(i, carry):
            sl = pl.ds(pl.multiple_of(yy * 512 + 64 * i, 64), 64)
            for p in range(2):
                a, b = rec[2 * p, sl, 128:256].astype(F32), rec[2 * p + 1, sl, 128:256].astype(F32)
                up2[sl, 1024 + 128 * p : 1152 + 128 * p] = jnp.where(low, pltpu.roll(a, 64, 1), b).astype(BF)
                dpr[sl, 512 + 128 * p : 640 + 128 * p] = jnp.where(low, a, pltpu.roll(b, 64, 1)).astype(BF)
            return carry

        lax.fori_loop(0, 8, body, 0)

    def pair_rows(yy, zp):
        return pl.ds(pl.multiple_of((yy * 4 + 2 * zp) * 128, 256), 256)

    def into(dst, zp, cols, value):
        dst(2 * zp)[:, cols] = value[0:128].astype(BF)
        dst(2 * zp + 1)[:, cols] = value[128:256].astype(BF)

    def chunks(count, width, body):
        def step(i, carry):
            body(pl.ds(pl.multiple_of(i * width, width), width))
            return carry

        lax.fori_loop(0, count, step, 0)

    def y_pair(yy, zp, dst):
        rows = pair_rows(yy, zp)

        def body(cols):
            into(dst, zp, cols, jnp.dot(up2[rows, :], w2[:, cols], preferred_element_type=F32))

        chunks(4, 512, body)

    def dn_pair(yy, zp, dst):
        rows = pair_rows(yy, zp)
        load = pltpu.make_async_copy(x_i.at[rows], xst, xl.at[0])
        load.start()
        load.wait()

        def stats(i, carry):
            sl = pl.ds(pl.multiple_of(32 * i, 32), 32)
            xf = xst[sl, :].astype(F32)
            mean = jnp.mean(xf, axis=-1, keepdims=True)
            cen = xf - mean
            mu[sl, :] = jnp.broadcast_to(mean, (32, 128))
            rs[sl, :] = jnp.broadcast_to(lax.rsqrt(jnp.mean(cen * cen, axis=-1, keepdims=True) + EPS), (32, 128))
            return carry

        lax.fori_loop(0, 8, stats, 0)

        def body(cols):
            d = dot_nt(dpr[rows, :], wc[cols, :])
            xh = (xst[:, cols].astype(F32) - mu[:, 0:1]) * rs[:, 0:1]
            acc[0:1, cols] += jnp.sum(d * xh, axis=0, keepdims=True)
            acc[1:2, cols] += jnp.sum(d, axis=0, keepdims=True)
            into(dst, zp, cols, d)

        chunks(8, 256, body)

    def send_y(t, buf, k, j):
        n.go(remote(buf, yr.at[k, t], yss.at[t, j], yrs.at[t, k], n.to_y))

    def w1_rows(yy, xx, cc):
        return pl.ds(pl.multiple_of((yy * 16 + xx * 8 + cc * 4) * 64, 256), 256)

    def w1_part(yy, xx, cc, write):
        flip[...] = nrm[:, w1_rows(yy, xx, cc)].T
        chunks(7, 256, lambda cols: write(cols, jnp.dot(flip[...], dpr[:, cols], preferred_element_type=F32)))

    def w2_part(gg, write):
        flip[...] = up2[:, pl.ds(pl.multiple_of(gg * 256, 256), 256)].T
        chunks(4, 512, lambda cols: write(cols, jnp.dot(flip[...], dy[:, cols], preferred_element_type=F32)))

    wide, thin = pl.ds(0, 256), pl.ds(256, 64)
    acc[...] = jnp.zeros_like(acc)

    loads[0].wait()
    loads[1].wait()

    def other_wide(xx, carry):
        def write(cols, value):
            st2[xx, 0:256, cols] = value.astype(BF)

        w2_part(2 * xx + n.cb, write)
        return carry

    lax.fori_loop(0, 2, other_wide, 0)
    for xx in range(2):
        n.go(remote(st2.at[xx, wide], s1.at[xx, wide], k2s.at[xx, 0], k2r.at[xx, 0], n.to_c))
    loads[2].wait()
    keep.wait()
    heads_in(0)
    split(0)
    zn = n.z + 1 - 2 * lax.rem(n.z, 2)
    y_pair(n.yb, zf, lambda k: ysend.at[k])
    send_y(0, ysend.at[3 * zf], 3 * zf, 0)
    send_y(0, ysend.at[1 + zf], 1 + zf, 1)
    y_pair(n.yb, z0, lambda k: ysend.at[k])
    send_y(0, ysend.at[zn], zn, 2)
    send_y(0, ysend.at[n.z], n.z, 3)
    heads_in(1)
    split(1)

    def own_y(i, carry):
        y_pair(n.y, i, lambda k: own.at[k, 0])
        return carry

    lax.fori_loop(0, 2, own_y, 0)
    flip[...] = up2[:, 1024:1280].T

    def thin_part(cols):
        four = jnp.dot(flip[...], dy[:, cols], preferred_element_type=F32)
        for xx in range(2):
            a, b = four[128 * xx : 128 * xx + 64], four[128 * xx + 64 : 128 * xx + 128]
            st2[xx, 256:320, cols] = jnp.where(n.c == 0, b, a).astype(BF)
            thin2[64 * xx : 64 * xx + 64, cols] = jnp.where(n.c == 0, a, b).astype(BF)

    chunks(4, 512, thin_part)
    for xx in range(2):
        n.go(remote(st2.at[xx, thin], s1.at[xx, thin], k2s.at[xx, 1], k2r.at[xx, 1], n.to_c))

    def w2_own(xx):
        arrive(s1.at[xx, wide], k2r.at[xx, 0])

        def write(cols, value):
            s1[xx, 0:256, cols] = (s1[xx, 0:256, cols].astype(F32) + value).astype(BF)

        w2_part(2 * xx + n.c, write)
        arrive(s1.at[xx, thin], k2r.at[xx, 1])
        mine = pl.ds(pl.multiple_of(64 * xx, 64), 64)
        s1[xx, 256:320, :] = (s1[xx, 256:320, :].astype(F32) + thin2[mine, :].astype(F32)).astype(BF)

    w2_own(n.xb)
    w2_own(n.x)
    outer = (n.z == 0) | (n.z == 3)
    inner = (n.z == 1) | (n.z == 2)

    def forward(t, j, who):
        k = (3 * zf, 1 + zf, zn)[j]
        up = jnp.where(k > n.z, 1, 0)
        slot = k + up
        block = own.at[k, t]

        @pl.when(who)
        def _():
            arrive(yr.at[k, t], yrs.at[t, k])
            if who is inner:
                arrive(ud.at[slot, t], urs.at[t, slot])
                add_rows(block, [yr.at[k, t], ud.at[slot, t]], 128)
            else:
                add_rows(block, [yr.at[k, t]], 128)

        to = {"ctx": n.ctx, "fsdp": n.z + 2 * up - 1}
        n.go(remote(block, ud.at[slot, t], uss.at[t, j], urs.at[t, slot], to), who)

    forward(0, 0, outer)
    heads_in(2)
    heads_in(3)

    def whole(i, carry):
        sl = pl.ds(pl.multiple_of(64 * i, 64), 64)
        for g in range(4):
            dpr[sl, 128 * g : 128 * g + 128] = rec[g, sl, 0:128]
        return carry

    lax.fori_loop(0, 16, whole, 0)
    loads[3].wait()
    loads[4].wait()

    def staged(k):
        xx = n.xb + (k // 2) * (1 - 2 * n.xb) if isinstance(k, int) else n.xb + lax.div(k, 2) * (1 - 2 * n.xb)
        yy = n.yb + (k % 2) * (1 - 2 * n.yb) if isinstance(k, int) else n.yb + lax.rem(k, 2) * (1 - 2 * n.yb)
        slot = k % 2 if isinstance(k, int) else lax.rem(k, 2)
        return yy, xx, remote(st1.at[slot], r1.at[yy * 2 + xx], k1s.at[k], k1r.at[yy * 2 + xx], n.to_c), slot

    def other_rows(k, carry):
        yy, xx, copy, slot = staged(k)

        @pl.when(k >= 2)
        def _():
            staged(k - 2)[2].wait_send()

        def write(cols, value):
            st1[slot, :, cols] = value.astype(BF)

        w1_part(yy, xx, n.cb, write)
        copy.start()
        return carry

    lax.fori_loop(0, 2, other_rows, 0)

    def w1_own(yy, xx):
        block = r1.at[yy * 2 + xx]
        arrive(block, k1r.at[yy * 2 + xx])

        def write(cols, value):
            block[:, cols] = (block[:, cols].astype(F32) + value).astype(BF)

        w1_part(yy, xx, n.c, write)

    def finish(t):
        k = n.z
        arrive(yr.at[k, t], yrs.at[t, k])

        @pl.when(n.z > 0)
        def _():
            arrive(ud.at[k + 1, t], urs.at[t, k + 1])

        @pl.when(n.z < 3)
        def _():
            arrive(ud.at[k, t], urs.at[t, k])

        @pl.when(n.z == 0)
        def _():
            add_rows(own.at[k, t], [yr.at[k, t], ud.at[k, t]], 128, yo.at[t])

        @pl.when(n.z == 3)
        def _():
            add_rows(own.at[k, t], [yr.at[k, t], ud.at[k + 1, t]], 128, yo.at[t])

        @pl.when(inner)
        def _():
            add_rows(own.at[k, t], [yr.at[k, t], ud.at[k, t], ud.at[k + 1, t]], 128, yo.at[t])

    for yy in (n.yb, n.y):
        w1_own(yy, n.xb)
        n.go(remote(r1.at[yy * 2 + n.xb], r2.at[yy], x1s.at[yy], x1r.at[yy], n.to_x))
    lax.fori_loop(2, 4, other_rows, 0)
    forward(0, 1, outer)
    n.go(remote(s1.at[n.xb], s2, x2s.at[0], x2r.at[0], n.to_x))
    loads[5].wait()

    def spare_at(k):
        return w2.at[pl.ds(pl.multiple_of(128 * k, 128), 128)]

    dn_pair(n.yb, zf, spare_at)
    send_y(1, spare_at(3 * zf), 3 * zf, 0)
    send_y(1, spare_at(1 + zf), 1 + zf, 1)
    forward(0, 0, inner)
    dn_pair(n.yb, z0, spare_at)
    send_y(1, spare_at(zn), zn, 2)
    send_y(1, spare_at(n.z), n.z, 3)
    forward(0, 2, outer)
    forward(0, 1, inner)
    for yy in (n.yb, n.y):
        w1_own(yy, n.x)
    def give(yy, qs):
        arrive(r2.at[yy], x1r.at[yy])
        add_rows(r1.at[yy * 2 + n.x], [r2.at[yy]], 256)
        for q in qs:
            to, _, zz = n.member(q)
            n.go(remote(r1.at[yy * 2 + n.x, pl.ds(pl.multiple_of(zz * 64, 64), 64)], o1.at[n.m], a1s.at[q], a1r.at[q], to))

    give(n.yb, (6, 5, 7, 4))

    def own_dn(i, carry):
        dn_pair(n.y, i, lambda k: own.at[k, 1])
        return carry

    lax.fori_loop(0, 2, own_dn, 0)
    forward(0, 2, inner)
    ones = jnp.ones((8, 1024), BF)
    d1[0] = jnp.dot(ones, dy[...], preferred_element_type=F32)
    tot = sums[0, 0:1, :] + sums[1, 0:1, :] + sums[2, 0:1, :] + sums[3, 0:1, :]
    lo1 = lanes_of((1, 128)) < 64
    zero = jnp.zeros((1, 128), F32)
    vsum = jnp.where(n.c == 0, jnp.where(lo1, tot[:, 128:256], zero), jnp.where(lo1, zero, pltpu.roll(tot[:, 128:256], 64, 1)))
    for g in range(4):
        for mm in range(8):
            e = ev.at[g * 8 + mm]
            for k in range(4):
                e[k : k + 1, :] = jnp.where(n.g == k, tot[:, 0:128], zero)
            for k in range(2):
                e[4 + k : 5 + k, :] = jnp.where(n.x == k, vsum, zero)
            for k in range(8):
                e[6 + k : 7 + k, :] = dsum[0:1, 128 * k : 128 * k + 128]
            tile = 128 * ((mm // 4) * 8 + g * 2 + (mm % 4) // 2)
            e[14:15, :] = acc[0:1, tile : tile + 128]
            e[15:16, :] = acc[1:2, tile : tile + 128]
    for xx in range(2):
        n.go(remote(ev.at[pl.ds((2 * xx + n.cb) * 8, 8)], t1.at[xx], eks.at[xx], ekr.at[xx], n.to_c))
    n.go(remote(d1.at[0], d1.at[1], dbs.at[0], dbr.at[0], n.to_c))
    forward(1, 0, outer)
    for xx in range(2):
        arrive(t1.at[xx], ekr.at[xx])
        sl = pl.ds((2 * xx + n.c) * 8, 8)
        ev[sl] = ev[sl] + t1[xx]
    arrive(d1.at[1], dbr.at[0])
    d1[2] = d1[0] + d1[1]
    n.go(remote(ev.at[pl.ds((2 * n.xb + n.c) * 8, 8)], t2, exs.at[0], exr.at[0], n.to_x))
    n.go(remote(d1.at[2], d1.at[3], dbs.at[1], dbr.at[1], n.to_x))

    forward(1, 1, outer)
    forward(1, 0, inner)
    forward(1, 2, outer)
    forward(1, 1, inner)
    give(n.y, (2, 1, 3))
    mine = pltpu.make_async_copy(r1.at[n.y * 2 + n.x, pl.ds(pl.multiple_of(n.z * 64, 64), 64)], o1.at[n.m], fl.at[0])
    mine.start()
    arrive(t2, exr.at[0])
    final = pl.ds(n.g * 8, 8)
    ev[final] = ev[final] + t2[...]
    for q in range(1, 8):
        to, yy, zz = n.member(q)
        n.go(remote(ev.at[n.g * 8 + yy * 4 + zz], eo.at[n.m], eas.at[q], ear.at[q], to))
    eo[n.m] = ev[n.g * 8 + n.m]
    arrive(d1.at[3], dbr.at[1])
    dbo[...] = d1[2] + d1[3]
    forward(1, 2, inner)
    finish(0)
    arrive(s2, x2r.at[0])
    add_rows(s1.at[n.x], [s2], 320)
    out2 = pltpu.make_async_copy(s1.at[n.x], o2, fl.at[1])
    out2.start()
    finish(1)
    for q in range(1, 8):
        yy, zz = n.source(q)
        arrive(eo.at[yy * 4 + zz], ear.at[q])
        arrive(o1.at[yy * 4 + zz], a1r.at[q])
    mine.wait()
    out2.wait()
    for k in (2, 3):
        staged(k)[2].wait_send()
    n.drain()


def reduce_all(att, normed, dy, x, act, dup, wc, w2, sums, dsum):
    sd = jax.ShapeDtypeStruct
    V = pltpu.VMEM
    return pl.pallas_call(
        reduce_kernel,
        name="reduce_all",
        out_shape=(sd((2, 128, 2048), F32), sd((8, 64, 1792), BF), sd((320, 2048), BF), sd((8, 16, 128), F32),
                   sd((8, 2048), F32)),
        in_specs=[HBM] * 8 + [VM] * 2,
        out_specs=(VM, HBM, HBM, VM, VM),
        scratch_shapes=[
            V((1024, 2048), BF), V((1024, 2048), BF), V((2048, 1792), BF), V((1280, 2048), BF),
            V((1024, 1792), BF), V((1024, 1280), BF), V((4, 1024, 256), BF),
            V((4, 128, 2048), BF), V((4, 2, 128, 2048), BF), V((5, 2, 128, 2048), BF), V((4, 2, 128, 2048), BF),
            V((4, 256, 1792), BF), V((2, 256, 1792), BF), V((2, 256, 1792), BF),
            V((2, 320, 2048), BF), V((2, 320, 2048), BF), V((320, 2048), BF), V((128, 2048), BF), V((256, 1024), BF),
            V((256, 2048), BF), V((256, 128), F32), V((256, 128), F32), V((8, 2048), F32),
            V((32, 16, 128), F32), V((2, 8, 16, 128), F32), V((8, 16, 128), F32), V((4, 8, 2048), F32),
            DMA((4, 3)), DMA((4, 3)), DMA((1,)), DMA((6,)), DMA((1,)),
            DMA((2, 4)), DMA((2, 4)), DMA((2, 3)), DMA((2, 5)),
            DMA((4,)), DMA((4,)), DMA((2,)), DMA((2,)), DMA((8,)), DMA((8,)),
            DMA((2, 2)), DMA((2, 2)), DMA((1,)), DMA((1,)),
            DMA((2,)), DMA((2,)), DMA((1,)), DMA((1,)), DMA((8,)), DMA((8,)), DMA((2,)), DMA((2,)), DMA((2,)),
        ],
        compiler_params=pltpu.CompilerParams(collective_id=3, has_side_effects=True, vmem_limit_bytes=67000000),
    )(att, normed, dy, x, act, dup, wc, w2, sums, dsum)


def finish_kernel(x, dy, yo, o1, o2a, o2b, cst, y, dx, dqkv, dff, dfc2, ddense):
    low = lanes_of((16, 128)) < 64
    for i in range(16):
        yy, g, zp = i // 8, (i // 2) % 4, i % 2
        a, b = yy * 4 + 2 * zp, yy * 4 + 2 * zp + 1
        cols = slice(128 * i, 128 * i + 128)
        src = slice(128 * g, 128 * g + 128)
        even, odd = o1[a, :, src].astype(F32), o1[b, :, src].astype(F32)
        dqkv[:, cols] = jnp.where(low, even, pltpu.roll(odd, 64, 1))
        dqkv[:, 2048 + 128 * i : 2176 + 128 * i] = jnp.where(low, pltpu.roll(even, 64, 1), odd)
        src = slice(512 + 128 * (g // 2), 640 + 128 * (g // 2))
        even, odd = o1[a, :, src].astype(F32), o1[b, :, src].astype(F32)
        if g % 2 == 0:
            v = jnp.where(low, even, pltpu.roll(odd, 64, 1))
        else:
            v = jnp.where(low, pltpu.roll(even, 64, 1), odd)
        dqkv[:, 4096 + 128 * i : 4224 + 128 * i] = v
    for h in range(32):
        mm, g = (h // 16) * 4 + h % 4, (h // 4) % 4
        dff[:, 256 * h : 256 * h + 256] = o1[mm, :, 768 + 256 * g : 1024 + 256 * g].astype(F32)
    dfc2[...] = o2a[...].astype(F32)
    ddense[...] = o2b[...].astype(F32)
    for i in range(2):
        sl = slice(16 * i, 16 * i + 16)
        xf = x[sl, :].astype(F32)
        cen = xf - jnp.mean(xf, axis=-1, keepdims=True)
        rstd = lax.rsqrt(jnp.mean(cen * cen, axis=-1, keepdims=True) + EPS)
        xhat = cen * rstd
        y[sl, :] = (xf + yo[0, sl, :] + cst[2:3, :]).astype(BF)
        gr = yo[1, sl, :] * cst[0:1, :]
        dx[sl, :] = dy[sl, :].astype(F32) + rstd * (
            gr - jnp.mean(gr, axis=-1, keepdims=True) - xhat * jnp.mean(gr * xhat, axis=-1, keepdims=True)
        )


def finish_all(x, dy, yo, o1, o2, cst):
    sd = jax.ShapeDtypeStruct

    def rows(count, width, first=0):
        return pl.BlockSpec((count, width), lambda i: (first + i, 0))

    return pl.pallas_call(
        finish_kernel,
        name="finish_all",
        grid=(4,),
        out_shape=(sd((128, 2048), BF), sd((128, 2048), F32), sd((64, 6144), F32), sd((64, 8192), F32),
                   sd((256, 2048), F32), sd((64, 2048), F32)),
        in_specs=[
            rows(32, 2048),
            rows(32, 2048),
            pl.BlockSpec((2, 32, 2048), lambda i: (0, i, 0)),
            pl.BlockSpec((8, 16, 1792), lambda i: (0, i, 0)),
            rows(64, 2048),
            rows(16, 2048, 16),
            pl.BlockSpec((8, 2048), lambda i: (0, 0)),
        ],
        out_specs=(rows(32, 2048), rows(32, 2048), rows(16, 6144), rows(16, 8192), rows(64, 2048), rows(16, 2048)),
        compiler_params=pltpu.CompilerParams(vmem_limit_bytes=VLIM),
    )(x, dy, yo, o1, o2, o2, cst)


def stored_columns(a):
    rows = a.shape[1]
    qk = a[:, :, :512].reshape(2, 4, rows, 4, 2, 64).transpose(2, 4, 0, 3, 1, 5).reshape(rows, 2, 2048)
    v = a[:, :, 512:768].reshape(2, 4, rows, 4, 64).transpose(2, 0, 3, 1, 4).reshape(rows, 1, 2048)
    f = a[:, :, 768:1792].reshape(2, 4, rows, 4, 256).transpose(2, 0, 3, 1, 4).reshape(rows, 8192)
    return jnp.concatenate([qk, v], axis=1).reshape(rows, 6144), f


def fast_device(
    block_input, output_grad, segment, slots, ln_gain, ln_bias, qkv_w, qkv_b, dense_w, dense_b, fc1_w, fc1_b, fc2_w, fc2_b
):
    ctx, y, x, c, z = place()
    g, m = x * 2 + c, y * 4 + z
    index = ctx * 4 + z
    xb, dyb = block_input[0], output_grad[0]

    vecs = [jnp.pad(v, (0, 256 - v.shape[0])) for v in (ln_gain, ln_bias, dense_b, fc2_b, qkv_b, fc1_b)]
    pack = jnp.stack(vecs + [jnp.zeros_like(fc1_b)] * 2)
    xg, dg, docg, normed, act, dup, wc, w2g, heads, dsum, cst, cos, sin = gather_all(
        slots, xb, dyb, segment, qkv_w, fc1_w, pack, fc2_w, dense_w
    )
    slot_of = jnp.sum(jnp.where(slots[None, :] == jnp.arange(16, dtype=jnp.int32)[:, None], jnp.arange(16, dtype=jnp.int32)[None, :], 0), axis=1)
    att, sums = attention(slot_of, heads.reshape(4, 2, 4, 128, 256), docg, cos, sin)
    yo, o1, o2, eo, dbo = reduce_all(att.reshape(4, 1024, 256), normed, dg, xg, act, dup, wc, w2g, sums, dsum)
    out, dx, g_qkv_w, g_fc1_w, g_fc2_w, g_dense_w = finish_all(xb, dyb, yo, o1, o2, cst)
    eo = eo.reshape(8, 2048)
    sq, sf = stored_columns(eo[:, None, :1792])
    g_qkv_b = lax.dynamic_slice_in_dim(sq[0], index * 192, 192, 0)
    g_fc1_b = lax.dynamic_slice_in_dim(sf[0], index * 256, 256, 0)
    tiles = jnp.sum(eo[:, 1792:].reshape(8, 2, 2, 64), axis=0)
    both = lax.dynamic_slice_in_dim(tiles, z % 2, 1, 1)
    g_db = lax.dynamic_slice_in_dim(dbo[0], index * 64, 64, 0)
    return (out[None], dx[None], both[0, 0], both[1, 0], g_qkv_w, g_qkv_b, g_dense_w, g_db, g_fc1_w, g_fc1_b, g_fc2_w, g_db)


def solution(mesh):
    in_specs = (
        P("fsdp", "ctx", None),
        P("fsdp", "ctx", None),
        P("fsdp", None),
        P(),
        P(("ctx", "fsdp")),
        P(("ctx", "fsdp")),
        P(("ctx", "fsdp"), None),
        P(("ctx", "fsdp")),
        P(("ctx", "fsdp"), None),
        P(("ctx", "fsdp")),
        P(("ctx", "fsdp"), None),
        P(("ctx", "fsdp")),
        P(("ctx", "fsdp"), None),
        P(("ctx", "fsdp")),
    )
    out_specs = (
        P("fsdp", "ctx", None),
        P("fsdp", "ctx", None),
        P(("ctx", "fsdp")),
        P(("ctx", "fsdp")),
        P(("ctx", "fsdp"), None),
        P(("ctx", "fsdp")),
        P(("ctx", "fsdp"), None),
        P(("ctx", "fsdp")),
        P(("ctx", "fsdp"), None),
        P(("ctx", "fsdp")),
        P(("ctx", "fsdp"), None),
        P(("ctx", "fsdp")),
    )
    small = mesh.shape["ctx"] == 8 and mesh.shape["fsdp"] == 4
    return jax.shard_map(
        fast_device if small else per_device, mesh=mesh, in_specs=in_specs, out_specs=out_specs, check_vma=False
    )
```
